128 devices in a mesh: rep: 2 (over core), dp: 64 (over x, y, z).
Axes of the slice: x: 4, y: 4, z: 4, core: 2. Of those that a mesh axis runs over, the one named last changes fastest.
Arguments:
- x: bfloat16 [128, 2048, 1024], P(('rep', 'dp')), parts along dimension 0
- dy: bfloat16 [128, 2048, 1024], P(('rep', 'dp')), parts along dimension 0
- w_gate: bfloat16 [2, 1024, 2560], P(None, 'dp')
- w_up: bfloat16 [2, 1024, 2560], P(None, 'dp')
- w_down: bfloat16 [2, 2560, 1024], P(None, 'dp')
Outputs:
- output 1: bfloat16 [128, 2048, 1024], P(('rep', 'dp')), parts along dimension 0
- output 2: bfloat16 [4, 1024, 2560], P('rep', 'dp'), parts along dimension 0
- output 3: bfloat16 [4, 1024, 2560], P('rep', 'dp'), parts along dimension 0
- output 4: bfloat16 [4, 2560, 1024], P('rep', 'dp'), parts along dimension 0
There are 2 independent parts. The reference program is written for one: setup_inputs(seed, part) draws one part's arguments, and reference() takes and returns one part's arrays. A program takes and returns all parts, laid end to end along the dimension named above; an argument that names none is the same for every part.
All inputs are finite; a program needn't handle non-finite values.
Results may differ from the reference program's by a relative error of at most 0.018.
Values are sent between devices in bfloat16 or wider.
A program may use at most 1.5 GiB of HBM per device.

```python
import jax
import jax.numpy as jnp
from jax import lax

SEQUENCES = 64
TOKENS = 2048
D = 1024
FF = 2560
LAYERS = 2
NAMES = ("w_gate", "w_up", "w_down")
SHAPES = {"w_gate": (LAYERS, D, FF), "w_up": (LAYERS, D, FF), "w_down": (LAYERS, FF, D)}


def bump(key, n, height):
    away = (jnp.arange(n, dtype=jnp.int32) - jax.random.randint(key, (), 0, n, jnp.int32)) % n
    return jnp.where(away < n // 8, height, 1.0)


def together(key, own, strength):
    shared = jax.random.normal(key, own.shape[1:], jnp.float32)
    return (own + strength * shared) * lax.rsqrt(1 + strength * strength)


def setup_inputs(seed: int = 0, part: int = 0) -> dict:
    kx, kdy, ka, kb, kz, kf, kh, kl, *kw = jax.random.split(jax.random.key(seed), 8 + len(NAMES))
    kx, kdy, ka, kb = (jax.random.fold_in(k, part) for k in (kx, kdy, ka, kb))
    shape = (SEQUENCES, TOKENS, D)
    much_x, much_dy = jax.random.uniform(kz, (2,), jnp.float32, 0.0, 1.0)
    layers = 2.0 ** jax.random.uniform(kl, (LAYERS, 1, 1), jnp.float32, -1.0, 1.0)
    x = together(ka, jax.random.normal(kx, shape, jnp.float32), much_x) * bump(kf, D, 4.0)
    dy = together(kb, jax.random.normal(kdy, shape, jnp.float32), much_dy)
    drawn = {"x": x.astype(jnp.bfloat16), "dy": (dy * (SEQUENCES * TOKENS) ** -0.5).astype(jnp.bfloat16)}
    for key, name in zip(kw, NAMES, strict=True):
        w = jax.random.normal(key, SHAPES[name], jnp.float32) * SHAPES[name][1] ** -0.5
        drawn[name] = (w * {"w_gate": 1.0, "w_up": bump(kh, FF, 4.0), "w_down": layers}[name]).astype(jnp.bfloat16)
    return drawn


def matmul(a, w):
    return jnp.dot(a, w, preferred_element_type=jnp.float32).astype(jnp.bfloat16)


def normed(h):
    wide = h.astype(jnp.float32)
    scale = lax.rsqrt(jnp.mean(wide**2, -1, keepdims=True) + 1e-6)
    return (wide * scale).astype(jnp.bfloat16)


def layer(h, w):
    a = normed(h)
    gate = jnp.dot(a, w["w_gate"], preferred_element_type=jnp.float32)
    up = jnp.dot(a, w["w_up"], preferred_element_type=jnp.float32)
    return h + matmul((jax.nn.silu(gate) * up).astype(jnp.bfloat16), w["w_down"])


def stack(weights, h):
    return lax.scan(lambda h, w: (layer(h, w), None), h, weights)[0]


def reference(x, dy, w_gate, w_up, w_down):
    weights = dict(zip(NAMES, (w_gate, w_up, w_down), strict=True))

    def take(so_far, sequence):
        h, by_y = sequence
        _, back = jax.vjp(stack, weights, h)
        by_weights, by_h = back(by_y)
        return jax.tree.map(lambda total, term: total + term.astype(jnp.float32), so_far, by_weights), by_h

    none_yet = {name: jnp.zeros(w.shape, jnp.float32) for name, w in weights.items()}
    by_weights, by_x = lax.scan(take, none_yet, (x, dy))
    return (by_x, *(by_weights[name].astype(jnp.bfloat16) for name in NAMES))
```

```python
import functools

import jax
import jax.numpy as jnp
from jax import lax
from jax.experimental import pallas as pl
from jax.experimental.pallas import tpu as pltpu
from jax.sharding import PartitionSpec as P

NAMES = ("w_gate", "w_up", "w_down")
MESH = pl.DeviceIdType.MESH
BF, F32 = jnp.bfloat16, jnp.float32
ANY = pl.BlockSpec(memory_space=pl.ANY)
VM = pl.BlockSpec(memory_space=pltpu.VMEM)

GATHER_ORDERS = ((2, 1, 0), (0, 2, 1), (1, 0, 2))
SCATTER_ORDERS = ((0, 1, 2), (1, 2, 0), (2, 0, 1))


def thirds(n):
    tiles = n // 128
    cuts = [0, (tiles + 2) // 3, (tiles + 2) // 3 + (tiles + 1) // 3, tiles]
    return [(cuts[i] * 128, cuts[i + 1] * 128) for i in range(3)]


class Place:
    def __init__(self):
        self.core = lax.axis_index("rep")
        me = lax.axis_index("dp")
        self.at = (me // 16, (me // 4) % 4, me % 4)

    def along(self, axis, step):
        return (self.at[axis] + (step + 4)) % 4

    def peer(self, axis, step):
        x, y, z = (self.along(a, step) if a == axis else self.at[a] for a in range(3))
        return {"dp": (x * 4 + y) * 4 + z}

    def other(self):
        return {"rep": 1 - self.core}


def enter(place, steps, other):
    barrier = pltpu.get_barrier_semaphore()
    for axis in range(3):
        for step in steps:
            pl.semaphore_signal(barrier, inc=1, device_id=place.peer(axis, step), device_id_type=MESH)
    if other:
        pl.semaphore_signal(barrier, inc=1, device_id=place.other(), device_id_type=MESH)
    pl.semaphore_wait(barrier, 3 * len(steps) + other)


class Gather:
    def __init__(self, place, full, mine, parts, send, recv):
        self.p, self.full, self.mine, self.parts, self.send, self.recv = place, full, mine, parts, send, recv
        self.copies = {}

    def view(self, color, where):
        at = [where.get(a, self.p.at[a]) for a in range(3)]
        return self.full.at[(*at, *self.parts[color])]

    def go(self, color, slot, src, dst, device):
        copy = pltpu.make_async_remote_copy(
            src_ref=src, dst_ref=dst, send_sem=self.send.at[color, slot], recv_sem=self.recv.at[color, slot], device_id=device, device_id_type=MESH
        )
        copy.start()
        self.copies[color, slot] = copy

    def stage(self, number):
        for color, (a, b, c) in enumerate(GATHER_ORDERS):
            got = lambda *slots: [self.copies[color, s].wait_recv() for s in slots]
            everything = slice(None)
            if number == 0:
                for slot, step in enumerate((1, -1, 2)):
                    self.go(color, slot, self.mine.at[self.parts[color]], self.view(color, {}), self.p.peer(a, step))
            for first, axis, begin, done in ((3, b, 1, {a: everything}), (7, c, 3, {a: everything, b: everything})):
                if number == begin:
                    if first == 3:
                        got(0, 1, 2)
                    else:
                        got(5, 6)
                    block = self.view(color, done)
                    for slot, step in ((first, 1), (first + 1, -1)):
                        self.go(color, slot, block, block, self.p.peer(axis, step))
                    if first == 7:
                        self.go(color, 11, block, block, self.p.other())
                if number == begin + 1:
                    for slot, step, half in ((first, 1, slice(0, 2)), (first + 1, -1, slice(2, 4))):
                        got(slot)
                        whole = self.view(color, {**done, axis: self.p.along(axis, -step)})
                        part = self.view(color, {**done, axis: self.p.along(axis, -step), a if first == 3 else b: half})
                        self.go(color, slot + 2, part, part, self.p.peer(axis, step))
                        if first == 7:
                            self.go(color, slot + 5, whole, whole, self.p.other())
            if number == 5:
                for slot, step, half in ((9, 1, slice(0, 2)), (10, -1, slice(2, 4))):
                    got(slot)
                    part = self.view(color, {a: everything, b: half, c: self.p.along(c, 2)})
                    self.go(color, slot + 5, part, part, self.p.other())
            if number == 6:
                got(11, 12, 13, 14, 15)

    def finish(self):
        for copy in self.copies.values():
            copy.wait_send()


def gather_parts(core, ff, d):
    gu = [(slice(None), slice(*cut)) for cut in thirds(ff)]
    half = pl.ds(pl.multiple_of(core * (d // 2), 128), d // 2)
    down = [(slice(*cut), half) for cut in ((32, 40), (0, 16), (16, 32))]
    return gu, down


def gather_kernel(g_ref, u_ref, d_ref, gu_full, d_full, mine, own_sem, send, recv):
    place = Place()
    layers = g_ref.shape[0]
    for n in range(layers):
        mine[n, 0] = g_ref[n]
        mine[n, 1] = u_ref[n]
    enter(place, (1, -1, 2), 1)
    gu_parts, d_parts = gather_parts(place.core, g_ref.shape[-1], d_ref.shape[-1])
    half = d_parts[0][1]
    x, y, z = place.at
    own = []
    for n in range(layers):
        for k, (src, dst) in enumerate(
            (
                (mine.at[n, place.core], gu_full.at[n, place.core, x, y, z]),
                (d_ref.at[n, :, half], d_full.at[n, x, y, z, :, half]),
            )
        ):
            own.append(pltpu.make_async_copy(src, dst, own_sem.at[2 * n + k]))
            own[-1].start()
    jobs = []
    for n in range(layers):
        jobs.append(Gather(place, gu_full.at[n, place.core], mine.at[n, place.core], gu_parts, send.at[2 * n], recv.at[2 * n]))
        jobs.append(Gather(place, d_full.at[n], d_ref.at[n], d_parts, send.at[2 * n + 1], recv.at[2 * n + 1]))
    for t in range(7 + len(jobs) - 1):
        if t == 1:
            for copy in own:
                copy.wait()
        for k, job in enumerate(jobs):
            if 0 <= t - k < 7:
                job.stage(t - k)
    for job in jobs:
        job.finish()


def gather(wg, wu, wd):
    layers, rows, ff = wg.shape
    drows, d = wd.shape[1:]
    return pl.pallas_call(
        gather_kernel,
        out_shape=(
            jax.ShapeDtypeStruct((layers, 2, 4, 4, 4, rows, ff), BF),
            jax.ShapeDtypeStruct((layers, 4, 4, 4, drows, d), BF),
        ),
        in_specs=[VM] * 3,
        out_specs=(ANY, ANY),
        scratch_shapes=[
            pltpu.VMEM((layers, 2, rows, ff), BF),
            pltpu.SemaphoreType.DMA((2 * layers,)),
            pltpu.SemaphoreType.DMA((2 * layers, 3, 16)),
            pltpu.SemaphoreType.DMA((2 * layers, 3, 16)),
        ],
        compiler_params=pltpu.CompilerParams(collective_id=0, has_side_effects=True),
        name="gather",
    )(wg, wu, wd)


class Scatter:
    def __init__(self, place, mine, out, in_a, in_h, acc_b, send_b, in_b, in_bh, acc_c, send_c, in_c, send, recv):
        self.p, self.mine, self.out = place, mine, out
        self.in_a, self.in_h, self.acc_b, self.send_b, self.in_b, self.in_bh = in_a, in_h, acc_b, send_b, in_b, in_bh
        self.acc_c, self.send_c, self.in_c, self.send, self.recv = acc_c, send_c, in_c, send, recv
        self.cuts = thirds(mine.shape[-1])
        self.copies = {}

    def go(self, color, slot, src, dst, axis, step):
        copy = pltpu.make_async_remote_copy(
            src_ref=src, dst_ref=dst, send_sem=self.send.at[color, slot], recv_sem=self.recv.at[color, slot], device_id=self.p.peer(axis, step),
            device_id_type=MESH,
        )
        copy.start()
        self.copies[color, slot] = copy

    def stage(self, number):
        for color, (a, b, c) in enumerate(SCATTER_ORDERS):
            cut = slice(*self.cuts[color])
            got = lambda *slots: [self.copies[color, s].wait_recv() for s in slots]

            def block(where, i, j):
                at = [None] * 3
                at[a], at[b], at[c] = self.p.along(a, where), i, j
                return (*at, slice(None), cut)

            if number == 0:
                for slot, step in ((0, 1), (1, -1)):
                    at = [slice(None)] * 3
                    at[a], at[b] = self.p.along(a, 2), pl.ds(2 * slot, 2)
                    self.go(color, slot, self.mine.at[(*at, slice(None), cut)], self.in_h[color].at[slot], a, step)
            if number == 1:
                for slot, step in ((0, 1), (1, -1)):
                    got(slot)

                    @pl.loop(0, 8)
                    def _(k):
                        i, j = k // 4, k % 4
                        at = block(step, 2 * slot + i, j)
                        self.mine[at] = (self.mine[at].astype(F32) + self.half(color, a, b, c, slot, i, j)).astype(BF)

                for slot, step in ((0, 1), (1, -1)):
                    at = [slice(None)] * 3
                    at[a] = self.p.along(a, step)
                    self.go(color, 2 + slot, self.mine.at[(*at, slice(None), cut)], self.in_a[color].at[slot], a, step)
            if number == 2:
                got(2, 3)

                @pl.loop(0, 16)
                def _(k):
                    i, j = k // 4, k % 4
                    l, m = (i, j) if b < c else (j, i)
                    term = self.mine[block(0, i, j)].astype(F32)
                    total = term + self.in_a[color][0, l, m].astype(F32) + self.in_a[color][1, l, m].astype(F32)
                    self.acc_b[color][i, j] = total
                    self.send_b[color][i, j] = total.astype(BF)

                for slot, step in ((0, 1), (1, -1)):
                    src = self.send_b[color].at[self.p.along(b, 2), pl.ds(2 * slot, 2)]
                    self.go(color, 4 + slot, src, self.in_bh[color].at[slot], b, step)
            if number == 3:
                for slot, step in ((0, 1), (1, -1)):
                    got(4 + slot)
                    i = self.p.along(b, step)

                    @pl.loop(0, 2)
                    def _(j):
                        total = self.acc_b[color][i, 2 * slot + j] + self.in_bh[color][slot, j].astype(F32)
                        self.send_b[color][i, 2 * slot + j] = total.astype(BF)

                for slot, step in ((0, 1), (1, -1)):
                    self.go(color, 6 + slot, self.send_b[color].at[self.p.along(b, step)], self.in_b[color].at[slot], b, step)
            if number == 4:
                got(6, 7)

                @pl.loop(0, 4)
                def _(j):
                    total = self.acc_b[color][self.p.at[b], j] + self.in_b[color][0, j].astype(F32) + self.in_b[color][1, j].astype(F32)
                    self.acc_c[color][j] = total
                    self.send_c[color][j] = total.astype(BF)

                for slot, step in enumerate((1, -1, 2)):
                    self.go(color, 8 + slot, self.send_c[color].at[self.p.along(c, step)], self.in_c[color].at[slot], c, step)
            if number == 5:
                got(8, 9, 10)
                total = self.acc_c[color][self.p.at[c]]
                for slot in range(3):
                    total = total + self.in_c[color][slot].astype(F32)
                self.out[:, cut] = total.astype(BF)

    def half(self, color, a, b, c, slot, i, j):
        l, m = (i, j) if b < c else (j, i)
        return self.in_h[color][slot, l, m].astype(F32)

    def finish(self):
        for copy in self.copies.values():
            copy.wait_send()


SCATTER_STAGES = 6


def scatter_scratch(rows, columns):
    shapes = {k: [] for k in ("in_a", "in_h", "acc_b", "send_b", "in_b", "in_bh", "acc_c", "send_c", "in_c")}
    for (lo, hi), (a, b, c) in zip(thirds(columns), SCATTER_ORDERS):
        w = hi - lo
        half = (2, 4) if b < c else (4, 2)
        for name, shape, kind in (
            ("in_a", (2, 4, 4), BF), ("in_h", (2, *half), BF), ("acc_b", (4, 4), F32), ("send_b", (4, 4), BF), ("in_b", (2, 4), BF),
            ("in_bh", (2, 2), BF), ("acc_c", (4,), F32), ("send_c", (4,), BF), ("in_c", (3,), BF),
        ):
            shapes[name].append(pltpu.VMEM((*shape, rows, w), kind))
    return list(shapes.values())


def scatter_kernel(n, *refs):
    terms, outs = refs[:n], refs[n : 2 * n]
    mine, scratch, load, send, recv = refs[2 * n : 3 * n], refs[3 * n : 4 * n], *refs[4 * n :]
    place = Place()
    loads = [pltpu.make_async_copy(terms[k], mine[k], load.at[k]) for k in range(n)]
    for copy in loads:
        copy.start()
    enter(place, (1, -1, 2), 0)
    jobs = [Scatter(place, mine[k], outs[k], *scratch[k], send.at[k], recv.at[k]) for k in range(n)]
    skew = 2
    for t in range(SCATTER_STAGES + skew * (n - 1)):
        for k, job in enumerate(jobs):
            if t - skew * k == 0:
                loads[k].wait()
            if 0 <= t - skew * k < SCATTER_STAGES:
                job.stage(t - skew * k)
    for job in jobs:
        job.finish()


def scatter(terms, number):
    n = len(terms)
    return pl.pallas_call(
        functools.partial(scatter_kernel, n),
        out_shape=tuple(jax.ShapeDtypeStruct(t.shape[3:], BF) for t in terms),
        in_specs=[ANY] * n,
        out_specs=(VM,) * n,
        scratch_shapes=[
            *(pltpu.VMEM(t.shape, BF) for t in terms),
            *(scatter_scratch(*t.shape[3:]) for t in terms),
            pltpu.SemaphoreType.DMA((n,)),
            pltpu.SemaphoreType.DMA((n, 3, 11)),
            pltpu.SemaphoreType.DMA((n, 3, 11)),
        ],
        compiler_params=pltpu.CompilerParams(collective_id=number, has_side_effects=True, vmem_limit_bytes=60 * 2**20),
        name=f"scatter{number}",
    )(*terms)


def matmul(a, w):
    return jnp.dot(a, w, preferred_element_type=F32).astype(BF)


def normed(h):
    wide = h.astype(F32)
    scale = lax.rsqrt(jnp.mean(wide**2, -1, keepdims=True) + 1e-6)
    return (wide * scale).astype(BF)


def layer(h, w):
    a = normed(h)
    gate = jnp.dot(a, w["w_gate"], preferred_element_type=F32)
    up = jnp.dot(a, w["w_up"], preferred_element_type=F32)
    return h + matmul((jax.nn.silu(gate) * up).astype(BF), w["w_down"])


def stack(weights, h):
    for w in weights:
        h = layer(h, w)
    return h


def solution(mesh):
    def step(x, dy, wg, wu, wd):
        layers, rows, ff = wg.shape
        drows, d = wd.shape[1:]
        gu, down = gather(wg, wu, wd)
        gu = gu.reshape(layers, 2, d, ff)
        down = down.reshape(layers, ff, d)
        weights = [{"w_gate": gu[n, 0], "w_up": gu[n, 1], "w_down": down[n]} for n in range(layers)]
        _, back = jax.vjp(stack, weights, x[0])
        by_weights, by_x = back(dy[0])
        outs = {name: [] for name in NAMES}
        for n in range(layers):
            shaped = [t.reshape(4, 4, 4, t.shape[0] // 64, t.shape[1]) for t in (by_weights[n][name] for name in NAMES)]
            for name, out in zip(NAMES, scatter(shaped, 1 + n)):
                outs[name].append(out)
        return (by_x[None], *(jnp.stack(outs[name]) for name in NAMES))

    seq, rows = P(("rep", "dp"), None, None), P(None, "dp", None)
    return jax.shard_map(
        step, mesh=mesh, in_specs=(seq, seq, rows, rows, rows), out_specs=(seq, *(P("rep", "dp", None),) * 3), check_vma=False
    )
```

```python
import jax
import jax.numpy as jnp
from jax import lax
from jax.experimental import pallas as pl
from jax.experimental.pallas import tpu as pltpu
from jax.sharding import PartitionSpec as P

MESH = pl.DeviceIdType.MESH
BF, F32 = jnp.bfloat16, jnp.float32
ANY = pl.BlockSpec(memory_space=pl.ANY)
VM = pl.BlockSpec(memory_space=pltpu.VMEM)
T, D, FF = 2048, 1024, 2560
RING, LANES, ROWS, MXU = 4, 128, 8, 256
CUBE = (RING,) * 3
TILES = 40
AXES = range(3)
STEPS = (1, -1, 2)
SIDES = ((0, 1), (1, -1))
EVERY = slice(None)
VMEM = 63 * 2**20

GATHER_ORDERS = ((2, 1, 0), (0, 2, 1), (1, 0, 2))
SCATTER_ORDERS = ((0, 1, 2), (1, 2, 0), (2, 0, 1))
SHARES = ((0, 14), (14, 27), (27, 40))


class Place:
    def __init__(self):
        self.core = lax.axis_index("rep")
        me = lax.axis_index("dp")
        self.at = (me // RING**2, (me // RING) % RING, me % RING)
        self.on = {(a, step): (self.at[a] + (step + RING)) % RING for a in AXES for step in STEPS}

    def along(self, axis, step):
        return self.on[axis, step]

    def peer(self, axis, step):
        x, y, z = (self.along(a, step) if a == axis else self.at[a] for a in AXES)
        return {"dp": (x * RING + y) * RING + z}

    def other(self):
        return {"rep": 1 - self.core}


def enter(place, other):
    barrier = pltpu.get_barrier_semaphore()
    for axis in AXES:
        for step in STEPS:
            pl.semaphore_signal(barrier, inc=1, device_id=place.peer(axis, step), device_id_type=MESH)
    if other:
        pl.semaphore_signal(barrier, inc=1, device_id=place.other(), device_id_type=MESH)
    pl.semaphore_wait(barrier, len(STEPS) * len(AXES) + other)


def remote(src, dst, send, recv, device):
    return pltpu.make_async_remote_copy(src_ref=src, dst_ref=dst, send_sem=send, recv_sem=recv, device_id=device, device_id_type=MESH)


def normed(h):
    wide = h.astype(F32)
    scale = lax.rsqrt(jnp.mean(wide**2, -1, keepdims=True) + 1e-6)
    return (wide * scale).astype(BF)


def dot(a, b, over_a=1, over_b=0):
    return lax.dot_general(a, b, (((over_a,), (over_b,)), ((), ())), preferred_element_type=F32)


def at_step(hooks, step):
    for number, hook in hooks.items():
        pl.when(step == number)(hook)


class Gather:
    def __init__(self, place, full, mine, parts, send, recv):
        self.p, self.full, self.mine, self.parts, self.send, self.recv = place, full, mine, parts, send, recv

    STARTS = (0, 3, 5, 7, 10, 14, 16)
    CROSS = (9, 12, 13, 14, 15)

    def view(self, color, where):
        at = [where.get(a, self.p.at[a]) for a in AXES]
        return self.full.at[(*at, *self.parts[color])]

    def copy(self, color, slot):
        a, b, c = GATHER_ORDERS[color]
        p = self.p
        sems = self.send.at[color, slot], self.recv.at[color, slot]
        stage = sum(slot >= first for first in self.STARTS) - 1
        k = slot - self.STARTS[stage]
        if stage == 0:
            return remote(self.mine.at[self.parts[color]], self.view(color, {}), *sems, p.peer(a, STEPS[k]))
        axis, done, split = (b, {a: EVERY}, a) if stage < 3 else (c, {a: EVERY, b: EVERY}, b)
        side = k % 2
        step, half = STEPS[side], slice(2 * side, 2 * side + 2)
        where = dict(done)
        if stage in (2, 4):
            where[axis] = p.along(axis, -step)
            if slot not in self.CROSS:
                where[split] = half
        if stage == 5:
            where.update({axis: p.along(axis, 2), split: half})
        block = self.view(color, where)
        return remote(block, block, *sems, p.other() if slot in self.CROSS else p.peer(axis, step))

    def stage(self, number):
        last = len(self.STARTS) - 1
        for color in AXES:
            if number == last:
                wait = self.CROSS
            else:
                wait = [k for k in range(self.STARTS[number - 1], self.STARTS[number]) if k not in self.CROSS] if number else ()
            for slot in wait:
                self.copy(color, slot).wait_recv()
            for slot in range(self.STARTS[number], self.STARTS[number + 1]) if number < last else ():
                self.copy(color, slot).start()

    def finish(self):
        for color in AXES:
            for slot in range(self.STARTS[-1]):
                self.copy(color, slot).wait_send()


def thirds(n):
    cuts = [0]
    for left in (3, 2, 1):
        cuts.append(cuts[-1] + -((cuts[-1] - n // LANES) // left))
    return [(lo * LANES, hi * LANES) for lo, hi in zip(cuts, cuts[1:])]


def gather_parts(core):
    gu = [(EVERY, slice(*cut)) for cut in thirds(FF)]
    half = pl.ds(pl.multiple_of(core * (D // 2), D // 2), D // 2)
    down = [(slice(*cut), EVERY, half) for cut in ((4, 5), (0, 2), (2, 4))]
    return gu, down


def slots(*groups):
    def hook():
        for job, stage in groups:
            job.stage(stage)

    return hook


class Scatter:
    def __init__(self, place, mine, out, number, bufs, send, recv):
        self.p, self.mine, self.out, self.number, self.send, self.recv = place, mine, out, number, send, recv
        self.in_a, self.in_h, self.acc_b, self.send_b, self.in_b, self.in_bh, self.acc_c, self.send_c, self.in_c = bufs

    def term(self, color, where):
        at = dict(zip(SCATTER_ORDERS[color], where))
        return (*(at[axis] for axis in AXES), slice(*SHARES[color]))

    STARTS = (0, 2, 4, 6, 8, 11)

    def copy(self, color, slot):
        a, b, c = SCATTER_ORDERS[color]
        p = self.p
        sems = self.send.at[color, slot], self.recv.at[color, slot]
        twin = self.number % 2
        stage = sum(slot >= first for first in self.STARTS) - 1
        k = slot - self.STARTS[stage]
        step, half = STEPS[k], pl.ds(2 * k, 2)
        if stage == 0:
            src, dst, axis = self.mine.at[self.term(color, (p.along(a, 2), half, EVERY))], self.in_h[color].at[k], a
        elif stage == 1:
            src, dst, axis = self.mine.at[self.term(color, (p.along(a, step), EVERY, EVERY))], self.in_a[color].at[k], a
        elif stage == 2:
            src, dst, axis = self.send_b[color].at[twin, p.along(b, 2), half], self.in_bh[color].at[k], b
        elif stage == 3:
            src, dst, axis = self.send_b[color].at[twin, p.along(b, step)], self.in_b[color].at[k], b
        else:
            src, dst, axis = self.send_c[color].at[twin, p.along(c, step)], self.in_c[color].at[self.number, k], c
        return remote(src, dst, *sems, p.peer(axis, step))

    def stage(self, number):
        last = len(self.STARTS) - 1
        for color, axes in enumerate(SCATTER_ORDERS):
            for slot in range(self.STARTS[number - 1], self.STARTS[number]) if number else ():
                self.copy(color, slot).wait_recv()
            self.sum(number, color, *axes)
            for slot in range(self.STARTS[number], self.STARTS[number + 1]) if number < last else ():
                self.copy(color, slot).start()
            for slot in range(self.STARTS[2], self.STARTS[last]) if number == last else ():
                self.copy(color, slot).wait_send()

    def sum(self, number, color, a, b, c):
        p, mine, twin = self.p, self.mine, self.number % 2
        in_a, in_h, acc_b, send_b, in_b, in_bh = (
            t[color] for t in (self.in_a, self.in_h, self.acc_b, self.send_b, self.in_b, self.in_bh)
        )
        acc_c, send_c, in_c = (t[color] for t in (self.acc_c, self.send_c, self.in_c))
        flip = (lambda i, j: (i, j)) if b < c else (lambda i, j: (j, i))
        if number == 1:
            for slot, step in SIDES:

                @pl.loop(0, 2 * RING)
                def _(k):
                    i, j = k // RING, k % RING
                    at = self.term(color, (p.along(a, step), 2 * slot + i, j))
                    mine[at] = (mine[at].astype(F32) + in_h[(slot, *flip(i, j))].astype(F32)).astype(BF)

        if number == 2:

            @pl.loop(0, RING**2)
            def _(k):
                i, j = k // RING, k % RING
                total = mine[self.term(color, (p.at[a], i, j))].astype(F32)
                total = total + in_a[(0, *flip(i, j))].astype(F32) + in_a[(1, *flip(i, j))].astype(F32)
                acc_b[i, j] = total
                send_b[twin, i, j] = total.astype(BF)

        if number == 3:
            for slot, step in SIDES:
                i = p.along(b, step)

                @pl.loop(0, 2)
                def _(j):
                    send_b[twin, i, 2 * slot + j] = (acc_b[i, 2 * slot + j] + in_bh[slot, j].astype(F32)).astype(BF)

        if number == 4:

            @pl.loop(0, RING)
            def _(j):
                total = acc_b[p.at[b], j] + in_b[0, j].astype(F32) + in_b[1, j].astype(F32)
                acc_c[j] = total
                send_c[twin, j] = total.astype(BF)

        if number == 5:
            total = acc_c[p.at[c]]
            for slot in AXES:
                total = total + in_c[self.number, slot].astype(F32)
            lo, hi = SHARES[color]
            high = self.out.shape[0] // ROWS
            for k in range(lo, hi):
                col, row = k // high, k % high
                self.out[pl.ds(ROWS * row, ROWS), pl.ds(LANES * col, LANES)] = total[k - lo].astype(BF)

    def finish(self):
        for color in AXES:
            for slot in range(self.STARTS[2]):
                self.copy(color, slot).wait_send()


def scatter_scratch(jobs):
    two, ring = (2,), (RING,)
    groups = []
    for (lo, hi), (a, b, c) in zip(SHARES, SCATTER_ORDERS):
        half = two + ring if b < c else ring + two
        shapes = (
            (two + ring + ring, BF), (two + half, BF), (ring + ring, F32), (two + ring + ring, BF), (two + ring, BF), (two + two, BF), (ring, F32),
            (two + ring, BF), ((jobs, len(STEPS)), BF),
        )
        groups.append([pltpu.VMEM((*shape, hi - lo, ROWS, LANES), kind) for shape, kind in shapes])
    return zip(*groups)


def store_tiles(val, store, high):
    for k in range(val.shape[1] // LANES):
        store(k, val[:, LANES * k : LANES * (k + 1)].reshape(-1, high, ROWS, LANES).astype(BF))


def part(k, size):
    return pl.ds(pl.multiple_of(k * size, size), size)


def blocks(shape, places, **mode):
    return pl.BlockSpec(shape, lambda *at: tuple(at[places[k]] if k in places else 0 for k in range(len(shape))), **mode)


def silu_parts(gate):
    s = jax.nn.sigmoid(gate)
    silu = gate * s
    return silu, s + silu * (1 - s)


def forward_kernel(
    g_ref, u_ref, d_ref, x_ref, dy_ref, gu_full, d_full, aT0, gate_up, act1, h1, aT1, act2, dgu2, mine, mine_d, a_v, h_v, t_v, dy_v, sem, send, recv
):
    place = Place()
    core = place.core
    layers = g_ref.shape[0]
    for n in range(layers):
        for k, ref in enumerate((g_ref, u_ref)):
            mine[n, k] = ref[n]
        mine_d[n] = d_ref[n]
    sems = [sem.at[k] for k in range(sem.shape[0])]
    load = pltpu.make_async_copy(x_ref, h_v, sems.pop())
    load_dy = pltpu.make_async_copy(dy_ref, dy_v, sems.pop())
    load.start()
    load_dy.start()
    enter(place, 1)
    gu_parts, d_parts = gather_parts(core)
    half = d_parts[0][-1]
    own, jobs = [], []
    for n in range(layers):
        own.append(pltpu.make_async_copy(mine.at[n, core], gu_full.at[(n, core, *place.at)], sems.pop()))
        own.append(pltpu.make_async_copy(mine_d.at[n, :, :, half], d_full.at[(n, *place.at, EVERY, EVERY, half)], sems.pop()))
        for args in ((gu_full.at[n, core], mine.at[n, core], gu_parts), (d_full.at[n], mine_d.at[n], d_parts)):
            jobs.append(Gather(place, *args, send.at[len(jobs)], recv.at[len(jobs)]))
    j0, *later = jobs
    j1, j2, j3 = later
    j0.stage(0)
    for copy in own:
        copy.start()
    load.wait()

    def norm_rows(k):
        rows = part(k, MXU)
        a = normed(h_v[rows])
        a_v[rows] = a
        t_v[:, rows] = a.T

    pl.loop(0, RING)(norm_rows)
    for copy in own:
        copy.wait()
    j0.stage(1)
    pl.loop(RING, 2 * RING)(norm_rows)
    put = pltpu.make_async_copy(t_v, aT0, sems[0])
    put.start()
    for stage in range(2, 7):
        j0.stage(stage)
        if stage > 2:
            for job in later if stage < 6 else ():
                job.stage(stage - 3)

    hooks = {0: slots((j1, 3), (j2, 3)), 3: slots((j1, 4)), 6: slots((j1, 5), (j2, 4), (j3, 3))}
    wide, tall = 512, 1024

    def gate_up_body(w, out_gu, out_act):
        row, step = pl.program_id(1), pl.program_id(0) * (T // tall) + pl.program_id(1)
        at_step(hooks, step)
        a = a_v[part(row, tall)]
        for k in range(wide // MXU):
            cols = slice(MXU * k, MXU * (k + 1))
            gate, up = (dot(a, w[m, :, :, :, :, cols].reshape(D, MXU)) for m in range(2))
            for m, val in enumerate((gate, up)):
                out_gu[m, :, cols] = val
            out_act[:, cols] = (silu_parts(gate)[0] * up).astype(BF)

    pltpu.emit_pipeline(
        gate_up_body,
        grid=(FF // wide, T // tall),
        in_specs=[blocks((2, *CUBE, 16, wide), {5: 0})],
        out_specs=[blocks((2, tall, wide), {1: 1, 2: 0}), blocks((tall, wide), {0: 1, 1: 0})],
    )(gu_full.at[0], gate_up, act1)
    put.wait()
    j1.stage(6)

    hooks_down = {0: slots((j2, 5), (j3, 4)), 2: slots((j2, 6), (j3, 5))}

    def down_body(act, w, out_h):
        step = pl.program_id(0)
        at_step(hooks_down, step)
        for k in range(wide // MXU):
            rows = slice(MXU * k, MXU * (k + 1))
            there = part(step * (wide // MXU) + k, MXU)
            out = dot(act[rows], w[...].reshape(FF, D)).astype(BF)
            h = (h_v[there].astype(F32) + out.astype(F32)).astype(BF)
            out_h[rows] = h
            a = normed(h)
            a_v[there] = a
            t_v[:, there] = a.T

    pltpu.emit_pipeline(
        down_body,
        grid=(T // wide,),
        in_specs=[blocks((wide, FF), {0: 0}), blocks(d_full.shape[1:], {}, pipeline_mode=pl.Buffered(1))],
        out_specs=[blocks((wide, D), {0: 0})],
    )(act1, d_full.at[0], h1)
    put = pltpu.make_async_copy(t_v, aT1, sems[0])
    put.start()
    load_dy.wait()
    j3.stage(6)

    def second_body(w, wd_block, out_act, out_dgu):
        wd = wd_block[...].reshape(FF // 2 // ROWS, ROWS, D)
        rows = part(pl.program_id(1), wide)
        a, dy = a_v[rows], dy_v[rows]
        for k in range(FF // 2 // MXU):
            cols = slice(MXU * k, MXU * (k + 1))
            gate, up = (dot(a, w[m, :, :, :, :, cols].reshape(D, MXU)) for m in range(2))
            by_act = dot(dy, wd[MXU // ROWS * k : MXU // ROWS * (k + 1)].reshape(MXU, D), 1, 1).astype(BF).astype(F32)
            silu, slope = silu_parts(gate)
            out_act[:, cols] = (silu * up).astype(BF)
            for m, val in enumerate((by_act * up * slope, by_act * silu)):
                out_dgu[m, :, cols] = val.astype(BF)

    pltpu.emit_pipeline(
        second_body,
        grid=(2, T // wide),
        in_specs=[blocks((2, *CUBE, 16, FF // 2), {5: 0}), blocks((2, *d_full.shape[2:]), {0: 0})],
        out_specs=[blocks((wide, FF // 2), {0: 1, 1: 0}), blocks((2, wide, FF // 2), {1: 1, 2: 0})],
    )(gu_full.at[1], d_full.at[1], act2, dgu2)
    put.wait()
    for job in jobs:
        job.finish()


def shaped(*shape, kind=BF):
    return jax.ShapeDtypeStruct(shape, kind)


def calls(kernel, number, ins, outs, scratch):
    return pl.pallas_call(
        kernel,
        out_shape=tuple(shape for shape, _ in outs),
        in_specs=ins,
        out_specs=tuple(spec for _, spec in outs),
        scratch_shapes=scratch,
        compiler_params=pltpu.CompilerParams(collective_id=number, has_side_effects=True, vmem_limit_bytes=VMEM),
        name=kernel.__name__,
    )


def forward(wg, wu, wd, x, dy):
    layers, rows = wg.shape[:-1]
    high = TILES * LANES // D
    outs = [
        shaped(layers, 2, *CUBE, rows, FF), shaped(layers, *CUBE, high, ROWS, D), shaped(D, T), shaped(2, T, FF, kind=F32), shaped(T, FF),
        shaped(T, D), shaped(D, T), shaped(T, FF), shaped(2, T, FF),
    ]
    scratch = [shaped(layers, 2, rows, FF), shaped(layers, high, ROWS, D), shaped(T, D), shaped(T, D), shaped(D, T), shaped(T, D)]
    sems = [(7,), (2 * layers, 3, 16), (2 * layers, 3, 16)]
    scratch = [pltpu.VMEM(t.shape, t.dtype) for t in scratch] + [pltpu.SemaphoreType.DMA(t) for t in sems]
    call = calls(forward_kernel, 0, [VM] * 3 + [ANY] * 2, [(t, ANY) for t in outs], scratch)
    return call(wg, wu, wd.reshape(layers, high, ROWS, D), x, dy)


def down_grad(act, by_out, sink, hooks, outs=(), out_specs=()):
    high = TILES * LANES // D

    def body(act_cols, *refs):
        k = pl.program_id(0)
        at_step(hooks, k)

        def store(c, val):
            sink(k, slice(high * c, high * (c + 1)), val.reshape(RING, RING, high, ROWS, LANES), *refs)

        store_tiles(dot(act_cols[...], by_out[...], 0, 0), store, high)

    pltpu.emit_pipeline(body, grid=(RING,), in_specs=[blocks((T, FF // RING), {1: 0})], out_specs=list(out_specs))(act, *outs)


def gate_up_grads(a_t, dgu, mine, hooks):
    high = TILES * LANES // FF
    wide = 512
    each = FF // wide

    def body(cols):
        k = pl.program_id(0)
        at_step(hooks, k)

        def store(c, val):
            tiles = pl.ds((k % each) * (high * wide // LANES) + high * c, high)
            mine[1 + k // each, :, :, :, tiles] = val.reshape(*CUBE, high, ROWS, LANES)

        store_tiles(dot(a_t[...], cols[...]), store, high)

    pltpu.emit_pipeline(body, grid=(2 * each,), in_specs=[pl.BlockSpec((None, T, wide), lambda k: (k // each, 0, k % each))])(dgu)


def state_grad(dgu, w, h, by_out, out, keep, hooks):
    def body(d, h, out):
        k = pl.program_id(0)
        at_step(hooks, k)
        rows = part(k, MXU)
        by_gate, by_up = (dot(d[m], w[m], 1, 1).astype(BF).astype(F32) for m in range(2))
        by_a = (by_gate + by_up).astype(BF).astype(F32)
        wide = h[...].astype(F32)
        scale = lax.rsqrt(jnp.mean(wide**2, -1, keepdims=True) + 1e-6)
        inner = jnp.mean(by_a * wide, -1, keepdims=True)
        by_norm = (by_a * scale - wide * (inner * scale * scale * scale)).astype(BF)
        total = (by_out[rows].astype(F32) + by_norm.astype(F32)).astype(BF)
        out[...] = total
        if keep is not None:
            keep[rows] = total

    rows = blocks((MXU, D), {0: 0})
    pltpu.emit_pipeline(body, grid=(T // MXU,), in_specs=[blocks((2, MXU, FF), {1: 0}), rows], out_specs=[rows])(dgu, h, out)


def scatter_jobs(place, mine, outs, bufs, send, recv):
    groups = [bufs[k : k + len(SHARES)] for k in range(0, len(bufs), len(SHARES))]
    return [Scatter(place, mine.at[k], out, k, groups, send.at[k], recv.at[k]) for k, out in enumerate(outs)]


def at_slot(jobs, t):
    return slots(*((job, t - 2 * k) for k, job in enumerate(jobs) if 0 <= t - 2 * k < len(Scatter.STARTS)))


def rest_of(jobs, first):
    for t in range(first, len(Scatter.STARTS) + 2 * (len(jobs) - 1)):
        at_slot(jobs, t)()
    for job in jobs:
        job.finish()


def second_kernel(act2, dy, aT1, dgu2, w2, h1, act1, dh1, down1, d_out, g_out, u_out, dy_v, t_v, dh_v, w_v, mine, *more):
    *bufs, sem, send, recv = more
    place = Place()
    loads = [pltpu.make_async_copy(*pair, sem.at[k]) for k, pair in enumerate(((dy, dy_v), (aT1, t_v), (w2.at[1], w_v)))]
    for copy in loads:
        copy.start()
    enter(place, 0)
    jobs = scatter_jobs(place, mine, (d_out, g_out, u_out), bufs, send, recv)
    load_dy, load_t, load_w = loads
    load_dy.wait()

    def keep_down(k, tiles, val):
        mine[0, k, :, :, tiles] = val

    down_grad(act2, dy_v, keep_down, {})
    load_t.wait()
    gate_up_grads(t_v, dgu2, mine, {0: at_slot(jobs, 0), 4: at_slot(jobs, 1), 9: at_slot(jobs, 2)})
    load_w.wait()
    state_grad(dgu2, w_v, h1, dy_v, dh1, dh_v, {2: at_slot(jobs, 3), 6: at_slot(jobs, 4)})

    def put_down(k, tiles, val, out):
        out[:, :, tiles] = val

    down_grad(act1, dh_v, put_down, {1: at_slot(jobs, 5)}, [down1], [blocks((None, *down1.shape[1:]), {0: 0})])
    rest_of(jobs, 6)


SUMS = [((TILES * LANES // D * ROWS, D), VM), ((TILES * LANES // FF * ROWS, FF), VM), ((TILES * LANES // FF * ROWS, FF), VM)]


def scatter_scratch_all():
    return [
        pltpu.VMEM((len(SUMS), *CUBE, TILES, ROWS, LANES), BF),
        *(buf for group in scatter_scratch(len(SUMS)) for buf in group),
        pltpu.SemaphoreType.DMA((4,)),
        *[pltpu.SemaphoreType.DMA((len(SUMS), len(SHARES), Scatter.STARTS[-1]))] * 2,
    ]


def backward(kernel, number, outs, vmem, args):
    outs = [(t, ANY) for t in outs] + [(shaped(*shape), spec) for shape, spec in SUMS]
    return calls(kernel, number, [ANY] * len(args), outs, [pltpu.VMEM(t, BF) for t in vmem] + scatter_scratch_all())(*args)


def second(*args):
    outs = [shaped(T, D), shaped(*CUBE, TILES, ROWS, LANES)]
    return backward(second_kernel, 1, outs, [(T, D), (D, T), (T, D), (2, D, FF)], args)


def first_kernel(dh1, gate_up, wd1, aT0, w1, x, down1, dx, dgu1, d_out, g_out, u_out, dh_v, t_v, wd_v, w_v, mine, *more):
    *bufs, sem, send, recv = more
    place = Place()
    pairs = ((down1, mine.at[0]), (dh1, dh_v), (wd1.at[0], wd_v), (aT0, t_v))
    loads = [pltpu.make_async_copy(*pair, sem.at[k]) for k, pair in enumerate(pairs)]
    for copy in loads:
        copy.start()
    enter(place, 0)
    jobs = scatter_jobs(place, mine, (d_out, g_out, u_out), bufs, send, recv)
    for copy in loads:
        copy.wait()
    load_w = pltpu.make_async_copy(w1.at[0], w_v, sem.at[0])
    load_w.start()
    at_slot(jobs, 0)()
    hooks = {10: at_slot(jobs, 1)}
    wide = 512

    def act_body(gu, out):
        col, row = pl.program_id(0), pl.program_id(1)
        at_step(hooks, col * (T // wide) + row)
        by_act = dot(dh_v[part(row, wide)], wd_v[part(col, wide)], 1, 1).astype(BF).astype(F32)
        silu, slope = silu_parts(gu[0])
        for m, val in enumerate((by_act * gu[1] * slope, by_act * silu)):
            out[m] = val.astype(BF)

    block = blocks((2, wide, wide), {1: 1, 2: 0})
    pltpu.emit_pipeline(act_body, grid=(FF // wide, T // wide), in_specs=[block], out_specs=[block])(gate_up, dgu1)
    gate_up_grads(t_v, dgu1, mine, {5: at_slot(jobs, 2), 9: at_slot(jobs, 3)})
    load_w.wait()
    state_grad(dgu1, w_v, x, dh_v, dx, None, {2: at_slot(jobs, 4), 5: at_slot(jobs, 5)})
    rest_of(jobs, 6)


def first(*args):
    return backward(first_kernel, 2, [shaped(T, D), shaped(2, T, FF)], [(T, D), (D, T), (FF, D), (2, D, FF)], args)


def solution(mesh):
    def step(x, dy, wg, wu, wd):
        x, dy = x[0], dy[0]
        gu, down, aT0, gate_up, act1, h1, aT1, act2, dgu2 = forward(wg, wu, wd, x, dy)
        gu, down = gu.reshape(-1, 2, D, FF), down.reshape(-1, FF, D)
        dh1, down1, d2, g2, u2 = second(act2, dy, aT1, dgu2, gu, h1, act1)
        dx, _, d1, g1, u1 = first(dh1, gate_up, down, aT0, gu, x, down1)
        return dx[None], jnp.stack([g1, g2]), jnp.stack([u1, u2]), jnp.stack([d1, d2])

    seq, rows = P(("rep", "dp"), None, None), P(None, "dp", None)
    return jax.shard_map(
        step, mesh=mesh, in_specs=(seq, seq, rows, rows, rows), out_specs=(seq, *[P("rep", "dp", None)] * 3), check_vma=False
    )
```

```python
import jax
import jax.numpy as jnp
from jax import lax
from jax.experimental import pallas as pl
from jax.experimental.pallas import tpu as pltpu
from jax.sharding import PartitionSpec as P

MESH = pl.DeviceIdType.MESH
BF, F32 = jnp.bfloat16, jnp.float32
ANY = pl.BlockSpec(memory_space=pl.ANY)
VM = pl.BlockSpec(memory_space=pltpu.VMEM)
T, D, FF = 2048, 1024, 2560
RING, LANES, ROWS, MXU = 4, 128, 8, 256
PAIR = 2 * ROWS
CUBE = (RING,) * 3
UNITS = 20
HIGH = UNITS * PAIR * LANES // D // ROWS
AXES = range(3)
STEPS = (1, -1, 2)
SIDES = ((0, 1), (1, -1))
EVERY = slice(None)
VMEM = 63 * 2**20

GATHER_ORDERS = ((2, 1, 0), (0, 2, 1), (1, 0, 2))
SCATTER_ORDERS = ((0, 1, 2), (1, 2, 0), (2, 0, 1))
SHARES = ((0, 7), (7, 14), (14, 20))


class Place:
    def __init__(self):
        self.core = lax.axis_index("rep")
        me = lax.axis_index("dp")
        self.at = (me // RING**2, (me // RING) % RING, me % RING)
        self.on = {(a, step): (self.at[a] + (step + RING)) % RING for a in AXES for step in STEPS}

    def along(self, axis, step):
        return self.on[axis, step]

    def peer(self, axis, step):
        x, y, z = (self.along(a, step) if a == axis else self.at[a] for a in AXES)
        return {"dp": (x * RING + y) * RING + z}

    def other(self):
        return {"rep": 1 - self.core}


def enter(place, other):
    barrier = pltpu.get_barrier_semaphore()
    for axis in AXES:
        for step in STEPS:
            pl.semaphore_signal(barrier, inc=1, device_id=place.peer(axis, step), device_id_type=MESH)
    if other:
        pl.semaphore_signal(barrier, inc=1, device_id=place.other(), device_id_type=MESH)
    pl.semaphore_wait(barrier, len(STEPS) * len(AXES) + other)


def remote(src, dst, send, recv, device):
    return pltpu.make_async_remote_copy(src_ref=src, dst_ref=dst, send_sem=send, recv_sem=recv, device_id=device, device_id_type=MESH)


def normed(h):
    wide = h.astype(F32)
    scale = lax.rsqrt(jnp.mean(wide**2, -1, keepdims=True) + 1e-6)
    return (wide * scale).astype(BF)


def dot(a, b, over_a=1, over_b=0):
    return lax.dot_general(a, b, (((over_a,), (over_b,)), ((), ())), preferred_element_type=F32)


def at_step(hooks, step):
    for number, hook in hooks.items():
        pl.when(step == number)(hook)


class Gather:
    def __init__(self, place, full, mine, parts, send, recv):
        self.p, self.full, self.mine, self.parts, self.send, self.recv = place, full, mine, parts, send, recv

    STARTS = (0, 3, 5, 7, 10, 14, 16)
    CROSS = (9, 12, 13, 14, 15)

    def view(self, color, where):
        at = [where.get(a, self.p.at[a]) for a in AXES]
        return self.full.at[(*at, *self.parts[color])]

    def copy(self, color, slot):
        a, b, c = GATHER_ORDERS[color]
        p = self.p
        sems = self.send.at[color, slot], self.recv.at[color, slot]
        stage = sum(slot >= first for first in self.STARTS) - 1
        k = slot - self.STARTS[stage]
        if stage == 0:
            return remote(self.mine.at[self.parts[color]], self.view(color, {}), *sems, p.peer(a, STEPS[k]))
        axis, done, split = (b, {a: EVERY}, a) if stage < 3 else (c, {a: EVERY, b: EVERY}, b)
        side = k % 2
        step, half = STEPS[side], slice(2 * side, 2 * side + 2)
        where = dict(done)
        if stage in (2, 4):
            where[axis] = p.along(axis, -step)
            if slot not in self.CROSS:
                where[split] = half
        if stage == 5:
            where.update({axis: p.along(axis, 2), split: half})
        block = self.view(color, where)
        return remote(block, block, *sems, p.other() if slot in self.CROSS else p.peer(axis, step))

    def stage(self, number):
        last = len(self.STARTS) - 1
        for color in AXES:
            if number == last:
                wait = self.CROSS
            else:
                wait = [k for k in range(self.STARTS[number - 1], self.STARTS[number]) if k not in self.CROSS] if number else ()
            for slot in wait:
                self.copy(color, slot).wait_recv()
            for slot in range(self.STARTS[number], self.STARTS[number + 1]) if number < last else ():
                self.copy(color, slot).start()

    def finish(self):
        for color in AXES:
            for slot in range(self.STARTS[-1]):
                self.copy(color, slot).wait_send()


def thirds(n):
    cuts = [0]
    for left in (3, 2, 1):
        cuts.append(cuts[-1] + -((cuts[-1] - n // LANES) // left))
    return [(lo * LANES, hi * LANES) for lo, hi in zip(cuts, cuts[1:])]


def gather_parts(core):
    gu = [(EVERY, slice(*cut)) for cut in thirds(FF)]
    half = pl.ds(pl.multiple_of(core * (D // 2), D // 2), D // 2)
    down = [(slice(*cut), EVERY, half) for cut in ((4, 5), (0, 2), (2, 4))]
    return gu, down


def slots(*groups):
    def hook():
        for job, stage in groups:
            job.stage(stage)

    return hook


class Scatter:
    STARTS = (0, 2, 4, 6, 8, 11)

    def __init__(self, place, mine, put, number, bufs, send, recv):
        self.p, self.mine, self.put, self.number, self.send, self.recv = place, mine, put, number, send, recv
        self.in_a, self.in_h, self.acc_b, self.send_b, self.in_b, self.in_bh, self.acc_c, self.send_c, self.in_c = bufs

    def term(self, color, where):
        at = dict(zip(SCATTER_ORDERS[color], where))
        return (*(at[axis] for axis in AXES), slice(*SHARES[color]))

    def copy(self, color, slot):
        a, b, c = SCATTER_ORDERS[color]
        p = self.p
        sems = self.send.at[color, slot], self.recv.at[color, slot]
        twin = self.number % 2
        stage = sum(slot >= first for first in self.STARTS) - 1
        k = slot - self.STARTS[stage]
        step, half = STEPS[k], pl.ds(2 * k, 2)
        if stage == 0:
            src, dst, axis = self.mine.at[self.term(color, (p.along(a, 2), half, EVERY))], self.in_h[color].at[twin, k], a
        elif stage == 1:
            src, dst, axis = self.mine.at[self.term(color, (p.along(a, step), EVERY, EVERY))], self.in_a[color].at[twin, k], a
        elif stage == 2:
            src, dst, axis = self.send_b[color].at[p.along(b, 2), half], self.in_bh[color].at[k], b
        elif stage == 3:
            src, dst, axis = self.send_b[color].at[p.along(b, step)], self.in_b[color].at[k], b
        else:
            src, dst, axis = self.send_c[color].at[p.along(c, step)], self.in_c[color].at[self.number, k], c
        return remote(src, dst, *sems, p.peer(axis, step))

    def stage(self, number):
        last = len(self.STARTS) - 1
        for color, axes in enumerate(SCATTER_ORDERS):
            for slot in range(self.STARTS[number - 1], self.STARTS[number]) if number else ():
                self.copy(color, slot).wait_recv()
            self.sum(number, color, *axes)
            for slot in range(self.STARTS[number], self.STARTS[number + 1]) if number < last else ():
                self.copy(color, slot).start()
            done = {3: self.STARTS[:3:2], last: self.STARTS[2::3]}.get(number)
            for slot in range(*done) if done else ():
                self.copy(color, slot).wait_send()

    def sum(self, number, color, a, b, c):
        p, mine, twin = self.p, self.mine, self.number % 2
        in_a, in_h, acc_b, send_b, in_b, in_bh = (
            t[color] for t in (self.in_a, self.in_h, self.acc_b, self.send_b, self.in_b, self.in_bh)
        )
        acc_c, send_c, in_c = (t[color] for t in (self.acc_c, self.send_c, self.in_c))
        flip = (lambda i, j: (i, j)) if b < c else (lambda i, j: (j, i))
        if number == 1:
            for slot, step in SIDES:

                @pl.loop(0, 2 * RING)
                def _(k):
                    i, j = k // RING, k % RING
                    at = self.term(color, (p.along(a, step), 2 * slot + i, j))
                    mine[at] = (mine[at].astype(F32) + in_h[(twin, slot, *flip(i, j))].astype(F32)).astype(BF)

        if number == 2:

            @pl.loop(0, RING**2)
            def _(k):
                i, j = k // RING, k % RING
                total = mine[self.term(color, (p.at[a], i, j))].astype(F32)
                for slot, _ in SIDES:
                    total = total + in_a[(twin, slot, *flip(i, j))].astype(F32)
                acc_b[i, j] = total
                send_b[i, j] = total.astype(BF)

        if number == 3:
            for slot, step in SIDES:
                i = p.along(b, step)

                @pl.loop(0, 2)
                def _(j):
                    send_b[i, 2 * slot + j] = (acc_b[i, 2 * slot + j] + in_bh[slot, j].astype(F32)).astype(BF)

        if number == 4:

            @pl.loop(0, RING)
            def _(j):
                total = acc_b[p.at[b], j]
                for slot, _ in SIDES:
                    total = total + in_b[slot, j].astype(F32)
                acc_c[j] = total
                send_c[j] = total.astype(BF)

        if number == 5:
            total = acc_c[p.at[c]]
            for slot in AXES:
                total = total + in_c[self.number, slot].astype(F32)
            lo, hi = SHARES[color]
            for k in range(lo, hi):
                self.put(k, total[k - lo])


def scatter_scratch(jobs):
    two, ring = (2,), (RING,)
    groups = []
    for (lo, hi), (a, b, c) in zip(SHARES, SCATTER_ORDERS):
        half = two + ring if b < c else ring + two
        shapes = (
            (two + two + ring + ring, BF), (two + two + half, BF), (ring + ring, F32), (ring + ring, BF), (two + ring, BF), (two + two, BF),
            (ring, F32), (ring, BF), ((jobs, len(STEPS)), BF),
        )
        groups.append([pltpu.VMEM((*shape, hi - lo, PAIR, LANES), kind) for shape, kind in shapes])
    return zip(*groups)


def put_gate_up(out):
    def put(k, unit):
        out[:, part(k, LANES)] = unit.astype(BF)

    return put


def put_down(out):
    def put(k, unit):
        extra = k - D // LANES * 2
        if extra < 0:
            out[part(k % 2, PAIR), part(k // 2, LANES)] = unit.astype(BF)
        else:
            for n in range(2):
                out[part(HIGH - 1, ROWS), part(2 * extra + n, LANES)] = unit[ROWS * n : ROWS * (n + 1)].astype(BF)

    return put


def part(k, size):
    return slice(k * size, (k + 1) * size) if isinstance(k, int) else pl.ds(pl.multiple_of(k * size, size), size)


def blocks(shape, places, **mode):
    return pl.BlockSpec(shape, lambda *at: tuple(at[places[k]] if k in places else 0 for k in range(len(shape))), **mode)


def silu_parts(gate):
    s = jax.nn.sigmoid(gate)
    silu = gate * s
    return silu, s + silu * (1 - s)


def forward_kernel(
    g_ref, u_ref, d_ref, x_ref, dy_ref, gu_full, d_full, aT0, gate_up, act1, h1, aT1, act2, dgu2, mine, mine_d, a_v, h_v, t_v, dy_v, sem, send, recv
):
    place = Place()
    core = place.core
    layers = g_ref.shape[0]
    for n in range(layers):
        for k, ref in enumerate((g_ref, u_ref)):
            mine[n, k] = ref[n]
        mine_d[n] = d_ref[n]
    sems = [sem.at[k] for k in range(sem.shape[0])]
    load = pltpu.make_async_copy(x_ref, h_v, sems.pop())
    load_dy = pltpu.make_async_copy(dy_ref, dy_v, sems.pop())
    load.start()
    load_dy.start()
    enter(place, 1)
    gu_parts, d_parts = gather_parts(core)
    half = d_parts[0][-1]
    own, jobs = [], []
    for n in range(layers):
        own.append(pltpu.make_async_copy(mine.at[n, core], gu_full.at[(n, core, *place.at)], sems.pop()))
        own.append(pltpu.make_async_copy(mine_d.at[n, :, :, half], d_full.at[(n, *place.at, EVERY, EVERY, half)], sems.pop()))
        for args in ((gu_full.at[n, core], mine.at[n, core], gu_parts), (d_full.at[n], mine_d.at[n], d_parts)):
            jobs.append(Gather(place, *args, send.at[len(jobs)], recv.at[len(jobs)]))
    j0, *later = jobs
    j1, j2, j3 = later
    j0.stage(0)
    for copy in own:
        copy.start()
    load.wait()

    def norm_rows(k):
        rows = part(k, MXU)
        a = normed(h_v[rows])
        a_v[rows] = a
        t_v[:, rows] = a.T

    pl.loop(0, RING)(norm_rows)
    for copy in own:
        copy.wait()
    j0.stage(1)
    pl.loop(RING, 2 * RING)(norm_rows)
    put = pltpu.make_async_copy(t_v, aT0, sems[0])
    put.start()
    for stage in range(2, 7):
        j0.stage(stage)
        if stage > 2:
            for job in later if stage < 6 else ():
                job.stage(stage - 3)

    hooks = {0: slots((j1, 3), (j2, 3)), 3: slots((j1, 4)), 6: slots((j1, 5), (j2, 4), (j3, 3))}
    wide, tall = 512, 1024

    def gate_up_body(w, out_gu, out_act):
        row, step = pl.program_id(1), pl.program_id(0) * (T // tall) + pl.program_id(1)
        at_step(hooks, step)
        a = a_v[part(row, tall)]
        for k in range(wide // MXU):
            cols = slice(MXU * k, MXU * (k + 1))
            gate, up = (dot(a, w[m, :, :, :, :, cols].reshape(D, MXU)) for m in range(2))
            for m, val in enumerate((gate, up)):
                out_gu[m, :, cols] = val
            out_act[:, cols] = (silu_parts(gate)[0] * up).astype(BF)

    pltpu.emit_pipeline(
        gate_up_body,
        grid=(FF // wide, T // tall),
        in_specs=[blocks((2, *CUBE, 16, wide), {5: 0})],
        out_specs=[blocks((2, tall, wide), {1: 1, 2: 0}), blocks((tall, wide), {0: 1, 1: 0})],
    )(gu_full.at[0], gate_up, act1)
    put.wait()
    j1.stage(6)

    hooks_down = {0: slots((j2, 5), (j3, 4)), 2: slots((j2, 6), (j3, 5))}

    def down_body(act, w, out_h):
        step = pl.program_id(0)
        at_step(hooks_down, step)
        for k in range(wide // MXU):
            rows = slice(MXU * k, MXU * (k + 1))
            there = part(step * (wide // MXU) + k, MXU)
            out = dot(act[rows], w[...].reshape(FF, D)).astype(BF)
            h = (h_v[there].astype(F32) + out.astype(F32)).astype(BF)
            out_h[rows] = h
            a = normed(h)
            a_v[there] = a
            t_v[:, there] = a.T

    pltpu.emit_pipeline(
        down_body,
        grid=(T // wide,),
        in_specs=[blocks((wide, FF), {0: 0}), blocks(d_full.shape[1:], {}, pipeline_mode=pl.Buffered(1))],
        out_specs=[blocks((wide, D), {0: 0})],
    )(act1, d_full.at[0], h1)
    put = pltpu.make_async_copy(t_v, aT1, sems[0])
    put.start()
    load_dy.wait()
    j3.stage(6)

    def second_body(w, wd_block, out_act, out_dgu):
        wd = wd_block[...].reshape(FF // 2 // ROWS, ROWS, D)
        rows = part(pl.program_id(1), wide)
        a, dy = a_v[rows], dy_v[rows]
        for k in range(FF // 2 // MXU):
            cols = slice(MXU * k, MXU * (k + 1))
            gate, up = (dot(a, w[m, :, :, :, :, cols].reshape(D, MXU)) for m in range(2))
            by_act = dot(dy, wd[MXU // ROWS * k : MXU // ROWS * (k + 1)].reshape(MXU, D), 1, 1).astype(BF).astype(F32)
            silu, slope = silu_parts(gate)
            out_act[:, cols] = (silu * up).astype(BF)
            for m, val in enumerate((by_act * up * slope, by_act * silu)):
                out_dgu[m, :, cols] = val.astype(BF)

    pltpu.emit_pipeline(
        second_body,
        grid=(2, T // wide),
        in_specs=[blocks((2, *CUBE, 16, FF // 2), {5: 0}), blocks((2, *d_full.shape[2:]), {0: 0})],
        out_specs=[blocks((wide, FF // 2), {0: 1, 1: 0}), blocks((2, wide, FF // 2), {1: 1, 2: 0})],
    )(gu_full.at[1], d_full.at[1], act2, dgu2)
    put.wait()
    for job in jobs:
        job.finish()


def shaped(*shape, kind=BF):
    return jax.ShapeDtypeStruct(shape, kind)


def calls(kernel, number, ins, outs, scratch):
    return pl.pallas_call(
        kernel,
        out_shape=tuple(shape for shape, _ in outs),
        in_specs=ins,
        out_specs=tuple(spec for _, spec in outs),
        scratch_shapes=scratch,
        compiler_params=pltpu.CompilerParams(collective_id=number, has_side_effects=True, vmem_limit_bytes=VMEM),
        name=kernel.__name__,
    )


def forward(wg, wu, wd, x, dy):
    layers, rows = wg.shape[:-1]
    high = HIGH
    outs = [
        shaped(layers, 2, *CUBE, rows, FF), shaped(layers, *CUBE, high, ROWS, D), shaped(D, T), shaped(2, T, FF, kind=F32), shaped(T, FF),
        shaped(T, D), shaped(D, T), shaped(T, FF), shaped(2, T, FF),
    ]
    scratch = [shaped(layers, 2, rows, FF), shaped(layers, high, ROWS, D), shaped(T, D), shaped(T, D), shaped(D, T), shaped(T, D)]
    sems = [(7,), (2 * layers, 3, 16), (2 * layers, 3, 16)]
    scratch = [pltpu.VMEM(t.shape, t.dtype) for t in scratch] + [pltpu.SemaphoreType.DMA(t) for t in sems]
    call = calls(forward_kernel, 0, [VM] * 3 + [ANY] * 2, [(t, ANY) for t in outs], scratch)
    return call(wg, wu, wd.reshape(layers, high, ROWS, D), x, dy)


def down_grad(act, by_out, mine, hooks):
    def body(act_cols):
        k = pl.program_id(0)
        at_step(hooks, k)
        val = dot(act_cols[...], by_out[...], 0, 0)
        tiles = D // LANES
        left = None
        for c in range(tiles):
            col = val[:, part(c, LANES)].reshape(RING**2, HIGH, ROWS, LANES)
            mine[k, :, :, 2 * c : 2 * c + 2] = col[:, : HIGH - 1].reshape(RING, RING, 2, PAIR, LANES).astype(BF)
            last = col[:, HIGH - 1 :]
            if c % 2:
                both = jnp.concatenate([left, last], 1).reshape(RING, RING, PAIR, LANES)
                mine[k, :, :, 2 * tiles + c // 2] = both.astype(BF)
            left = last

    pltpu.emit_pipeline(body, grid=(RING,), in_specs=[blocks((T, FF // RING), {1: 0})])(act)


def gate_up_grads(a_t, dgu, mine, hooks):
    wide = 512
    each = FF // wide

    def body(cols):
        k = pl.program_id(0)
        at_step(hooks, k)
        val = dot(a_t[...], cols[...])
        for c in range(wide // LANES):
            col = val[:, part(c, LANES)].reshape(*CUBE, PAIR, LANES).astype(BF)
            mine[1 + k // each, :, :, :, (k % each) * (wide // LANES) + c] = col

    pltpu.emit_pipeline(body, grid=(2 * each,), in_specs=[pl.BlockSpec((None, T, wide), lambda k: (k // each, 0, k % each))])(dgu)


def state_grad(dgu, w, h, by_out, held, out, keep, hooks):
    steps = T // MXU

    def project(d, k):
        by_gate, by_up = (dot(d[m], w[m], 1, 1).astype(BF).astype(F32) for m in range(2))
        held[k % 2] = (by_gate + by_up).astype(BF)

    def finish(h, outs, k):
        rows = part(jnp.maximum(k - 1, 0), MXU)
        by_a = held[(k + 1) % 2].astype(F32)
        wide = h[...].astype(F32)
        scale = lax.rsqrt(jnp.mean(wide**2, -1, keepdims=True) + 1e-6)
        inner = jnp.mean(by_a * wide, -1, keepdims=True)
        by_norm = (by_a * scale - wide * (inner * scale * scale * scale)).astype(BF)
        total = (by_out[rows].astype(F32) + by_norm.astype(F32)).astype(BF)
        if keep is None:
            outs[0][...] = total
        else:
            keep[rows] = total

    def body(d, h, *outs):
        k = pl.program_id(0)
        at_step(hooks, k)

        @pl.when(k < steps)
        def _():
            finish(h, outs, k)
            project(d, k)

        pl.when(k == steps)(lambda: finish(h, outs, k))

    behind = pl.BlockSpec((MXU, D), lambda k: (jnp.maximum(k - 1, 0), 0))
    pltpu.emit_pipeline(
        body,
        grid=(steps + 1,),
        in_specs=[pl.BlockSpec((2, MXU, FF), lambda k: (0, jnp.minimum(k, steps - 1), 0)), behind],
        out_specs=[behind] if keep is None else [],
    )(dgu, h, *([out] if keep is None else []))


def act_grads(gate_up, by_out, w, out, hooks):
    wide = 512

    def body(gu, out):
        col, row = pl.program_id(0), pl.program_id(1)
        at_step(hooks, col * (T // wide) + row)
        by_act = dot(by_out[part(row, wide)], w[part(col, wide)], 1, 1).astype(BF).astype(F32)
        silu, slope = silu_parts(gu[0])
        for m, val in enumerate((by_act * gu[1] * slope, by_act * silu)):
            out[m] = val.astype(BF)

    block = blocks((2, wide, wide), {1: 1, 2: 0})
    pltpu.emit_pipeline(body, grid=(FF // wide, T // wide), in_specs=[block], out_specs=[block])(gate_up, out)


PHASES = (
    {},
    {0: [(0, 0)], 3: [(0, 1)], 5: [(1, 0)], 7: [(0, 2)], 9: [(0, 3)]},
    {0: [(1, 1), (2, 0)], 1: [(0, 4)], 3: [(0, 5)], 4: [(1, 2)], 6: [(1, 3)], 7: [(2, 1)]},
    {0: [(1, 4)], 1: [(1, 5)], 3: [(2, 2)]},
    {0: [(2, 3), (3, 0)], 5: [(2, 4)], 9: [(2, 5), (3, 1)]},
    {0: [(3, 2)], 1: [(3, 3)], 3: [(3, 4)], 4: [(3, 5)], 5: [(4, 0)], 8: [(4, 1)]},
    {0: [(5, 0)], 2: [(4, 2)], 3: [(4, 3)], 4: [(5, 1)], 5: [(4, 4)], 6: [(4, 5)]},
)
ENDING = ((5, 2), (5, 3), (5, 4), (5, 5))


def backward_kernel(
    act2, dy, aT1, dgu2, gu_w, h1, act1, gate_up, d_w, aT0, x, dx, dgu1, d_out, g_out, u_out, dy_w_v, t_v, dh_v, w_v, held, mine, *more
):
    *bufs, sem, send, recv = more
    place = Place()
    sems = [sem.at[k] for k in range(sem.shape[0])]

    def load(src, dst):
        copy = pltpu.make_async_copy(src, dst, sems.pop())
        copy.start()
        return copy

    dy_v = dy_w_v.at[:T]
    load_dy, load_t, load_w = load(dy, dy_v), load(aT1, t_v), load(gu_w.at[1], w_v)
    enter(place, 0)
    groups = [bufs[k : k + len(SHARES)] for k in range(0, len(bufs), len(SHARES))]
    jobs = []
    for layer in (1, 0):
        for k, put in enumerate((put_down(d_out.at[layer]), put_gate_up(g_out.at[layer]), put_gate_up(u_out.at[layer]))):
            n = len(jobs)
            jobs.append(Scatter(place, mine.at[k], put, n, groups, send.at[n], recv.at[n]))
    hooks = [{step: slots(*((jobs[n], stage) for n, stage in pairs)) for step, pairs in phase.items()} for phase in PHASES]
    load_dy.wait()
    down_grad(act2, dy_v, mine.at[0], hooks[0])
    load_t.wait()
    gate_up_grads(t_v, dgu2, mine, hooks[1])
    load_t = load(aT0, t_v)
    load_w.wait()
    state_grad(dgu2, w_v, h1, dy_v, held, None, dh_v, hooks[2])
    load_w = load(gu_w.at[0], w_v)
    load_d = load(d_w.at[0], dy_w_v)
    down_grad(act1, dh_v, mine.at[0], hooks[3])
    load_d.wait()
    act_grads(gate_up, dh_v, dy_w_v, dgu1, hooks[4])
    load_t.wait()
    gate_up_grads(t_v, dgu1, mine, hooks[5])
    load_w.wait()
    state_grad(dgu1, w_v, x, dh_v, held, dx, None, hooks[6])
    slots(*((jobs[n], stage) for n, stage in ENDING))()


def backward(*args):
    n = 6
    sums = [shaped(2, HIGH * ROWS, D), shaped(2, PAIR, FF), shaped(2, PAIR, FF)]
    outs = [(shaped(T, D), ANY), (shaped(2, T, FF), ANY)] + [(t, VM) for t in sums]
    vmem = [(FF, D), (D, T), (T, D), (2, D, FF), (2, MXU, D), (len(sums), *CUBE, UNITS, PAIR, LANES)]
    scratch = [
        *(pltpu.VMEM(t, BF) for t in vmem),
        *(buf for group in scatter_scratch(n) for buf in group),
        pltpu.SemaphoreType.DMA((n,)),
        *[pltpu.SemaphoreType.DMA((n, len(SHARES), Scatter.STARTS[-1]))] * 2,
    ]
    return calls(backward_kernel, 1, [ANY] * len(args), outs, scratch)(*args)


def solution(mesh):
    def step(x, dy, wg, wu, wd):
        x, dy = x[0], dy[0]
        gu, down, aT0, gate_up, act1, h1, aT1, act2, dgu2 = forward(wg, wu, wd, x, dy)
        gu, down = gu.reshape(-1, 2, D, FF), down.reshape(-1, FF, D)
        dx, _, by_d, by_g, by_u = backward(act2, dy, aT1, dgu2, gu, h1, act1, gate_up, down, aT0, x)
        return dx[None], by_g, by_u, by_d

    seq, rows = P(("rep", "dp"), None, None), P(None, "dp", None)
    return jax.shard_map(
        step, mesh=mesh, in_specs=(seq, seq, rows, rows, rows), out_specs=(seq, *[P("rep", "dp", None)] * 3), check_vma=False
    )
```

```python
import jax
import jax.numpy as jnp
from jax import lax
from jax.experimental import pallas as pl
from jax.experimental.pallas import tpu as pltpu
from jax.sharding import PartitionSpec as P

MESH = pl.DeviceIdType.MESH
BF, F32 = jnp.bfloat16, jnp.float32
ANY = pl.BlockSpec(memory_space=pl.ANY)
VM = pl.BlockSpec(memory_space=pltpu.VMEM)
T, D, FF = 2048, 1024, 2560
RING, LANES, ROWS, MXU = 4, 128, 8, 256
PAIR = 2 * ROWS
CUBE = (RING,) * 3
UNITS = 20
HIGH = UNITS * PAIR * LANES // D // ROWS
AXES = range(3)
STEPS = (1, -1, 2)
SIDES = ((0, 1), (1, -1))
EVERY = slice(None)
VMEM = 63 * 2**20

GATHER_ORDERS = ((2, 1, 0), (0, 2, 1), (1, 0, 2))
SCATTER_ORDERS = ((0, 1, 2), (1, 2, 0), (2, 0, 1))
SHARES = ((0, 7), (7, 14), (14, 20))


class Place:
    def __init__(self):
        self.core = lax.axis_index("rep")
        me = lax.axis_index("dp")
        self.at = (me // RING**2, (me // RING) % RING, me % RING)
        self.on = {(a, step): (self.at[a] + (step + RING)) % RING for a in AXES for step in STEPS}

    def along(self, axis, step):
        return self.on[axis, step]

    def peer(self, axis, step):
        x, y, z = (self.along(a, step) if a == axis else self.at[a] for a in AXES)
        return {"dp": (x * RING + y) * RING + z}

    def other(self):
        return {"rep": 1 - self.core}


def enter(place, other):
    barrier = pltpu.get_barrier_semaphore()
    for axis in AXES:
        for step in STEPS:
            pl.semaphore_signal(barrier, inc=1, device_id=place.peer(axis, step), device_id_type=MESH)
    if other:
        pl.semaphore_signal(barrier, inc=1, device_id=place.other(), device_id_type=MESH)
    return lambda: pl.semaphore_wait(barrier, len(STEPS) * len(AXES) + other)


def remote(src, dst, send, recv, device):
    return pltpu.make_async_remote_copy(src_ref=src, dst_ref=dst, send_sem=send, recv_sem=recv, device_id=device, device_id_type=MESH)


def normed(h):
    wide = h.astype(F32)
    scale = lax.rsqrt(jnp.mean(wide**2, -1, keepdims=True) + 1e-6)
    return (wide * scale).astype(BF)


def dot(a, b, over_a=1, over_b=0):
    return lax.dot_general(a, b, (((over_a,), (over_b,)), ((), ())), preferred_element_type=F32)


def at_step(hooks, step):
    for number, hook in hooks.items():
        pl.when(step == number)(hook)


class Gather:
    def __init__(self, name, place, full, parts, send, recv):
        self.name, self.p, self.full, self.parts, self.send, self.recv = name, place, full, parts, send, recv

    STARTS = (0, 3, 5, 7, 10, 14, 16)
    CROSS = (9, 12, 13, 14, 15)

    def view(self, color, where):
        at = [where.get(a, self.p.at[a]) for a in AXES]
        return self.full.at[(*at, *self.parts[color])]

    def copy(self, color, slot):
        a, b, c = GATHER_ORDERS[color]
        p = self.p
        sems = self.send.at[color, slot], self.recv.at[color, slot]
        stage = sum(slot >= first for first in self.STARTS) - 1
        k = slot - self.STARTS[stage]
        if stage == 0:
            block = self.view(color, {})
            return remote(block, block, *sems, p.peer(a, STEPS[k]))
        axis, done, split = (b, {a: EVERY}, a) if stage < 3 else (c, {a: EVERY, b: EVERY}, b)
        side = k % 2
        step, half = STEPS[side], slice(2 * side, 2 * side + 2)
        where = dict(done)
        if stage in (2, 4):
            where[axis] = p.along(axis, -step)
            if slot not in self.CROSS:
                where[split] = half
        if stage == 5:
            where.update({axis: p.along(axis, 2), split: half})
        block = self.view(color, where)
        return remote(block, block, *sems, p.other() if slot in self.CROSS else p.peer(axis, step))

    def stage(self, number):
        last = len(self.STARTS) - 1
        for color in AXES:
            if number == last:
                wait = self.CROSS
            else:
                wait = [k for k in range(self.STARTS[number - 1], self.STARTS[number]) if k not in self.CROSS] if number else ()
            for slot in wait:
                self.copy(color, slot).wait_recv()
            for slot in range(self.STARTS[number], self.STARTS[number + 1]) if number < last else ():
                self.copy(color, slot).start()

    def finish(self):
        for color in AXES:
            for slot in range(self.STARTS[-1]):
                self.copy(color, slot).wait_send()


def gather_parts(core):
    pieces = []
    for widths in ((3, 3, 2), (2, 2, 2), (2, 2, 2)):
        pieces.append([])
        for width in widths:
            first = sum(sum(w for _, w in piece) for piece in pieces)
            pieces[-1].append((first, width))
    whole = [(7 * k, w) for k, w in enumerate((7, 7, 6))]
    columns = [[(EVERY, slice(first * LANES, (first + w) * LANES)) for first, w in piece] for piece in (*pieces, whole)]
    half = part(core, D // 2)
    return columns, [(slice(*cut), EVERY, half) for cut in ((4, 5), (0, 2), (2, 4))]


def slots(*groups):
    def hook():
        for job, stage in groups:
            with jax.named_scope(f"{job.name}_{stage}"):
                job.stage(stage)

    return hook


def spread(jobs, table, sizes):
    plan = {}
    for n, (job, steps) in enumerate(zip(jobs, table, strict=True)):
        for stage, step in enumerate(steps):
            plan.setdefault(step, []).append((-stage, n, job))
    hooks, first = [], 0
    for size in sizes:
        steps = [step for step in sorted(plan) if first <= step < first + size]
        hooks.append({step - first: slots(*((job, -late) for late, _, job in sorted(plan[step], key=lambda t: t[:2]))) for step in steps})
        first += size
    return hooks


class Scatter:
    STARTS = (0, 2, 4, 6, 8, 11)

    def __init__(self, place, mine, put, number, bufs, send, recv):
        self.name = f"rs{number}"
        self.p, self.mine, self.put, self.number, self.send, self.recv = place, mine, put, number, send, recv
        self.in_a, self.in_h, self.acc_b, self.send_b, self.in_b, self.in_bh, self.acc_c, self.send_c, self.in_c = bufs

    def term(self, color, where):
        at = dict(zip(SCATTER_ORDERS[color], where))
        return (*(at[axis] for axis in AXES), slice(*SHARES[color]))

    def copy(self, color, slot):
        a, b, c = SCATTER_ORDERS[color]
        p = self.p
        sems = self.send.at[color, slot], self.recv.at[color, slot]
        twin = self.number % 2
        stage = sum(slot >= first for first in self.STARTS) - 1
        k = slot - self.STARTS[stage]
        step, half = STEPS[k], pl.ds(2 * k, 2)
        if stage == 0:
            src, dst, axis = self.mine.at[self.term(color, (p.along(a, 2), half, EVERY))], self.in_h[color].at[twin, k], a
        elif stage == 1:
            src, dst, axis = self.mine.at[self.term(color, (p.along(a, step), EVERY, EVERY))], self.in_a[color].at[twin, k], a
        elif stage == 2:
            src, dst, axis = self.send_b[color].at[p.along(b, 2), half], self.in_bh[color].at[k], b
        elif stage == 3:
            src, dst, axis = self.send_b[color].at[p.along(b, step)], self.in_b[color].at[k], b
        else:
            src, dst, axis = self.send_c[color].at[p.along(c, step)], self.in_c[color].at[self.number, k], c
        return remote(src, dst, *sems, p.peer(axis, step))

    def stage(self, number):
        last = len(self.STARTS) - 1
        for color, axes in enumerate(SCATTER_ORDERS):
            for slot in range(self.STARTS[number - 1], self.STARTS[number]) if number else ():
                self.copy(color, slot).wait_recv()
            self.sum(number, color, *axes)
            for slot in range(self.STARTS[number], self.STARTS[number + 1]) if number < last else ():
                self.copy(color, slot).start()
            done = {3: self.STARTS[:3:2], 4: self.STARTS[2:5:2], last: self.STARTS[4:]}.get(number)
            for slot in range(*done) if done else ():
                self.copy(color, slot).wait_send()

    def sum(self, number, color, a, b, c):
        p, mine, twin = self.p, self.mine, self.number % 2
        in_a, in_h, acc_b, send_b, in_b, in_bh = (
            t[color] for t in (self.in_a, self.in_h, self.acc_b, self.send_b, self.in_b, self.in_bh)
        )
        acc_c, send_c, in_c = (t[color] for t in (self.acc_c, self.send_c, self.in_c))
        flip = (lambda i, j: (i, j)) if b < c else (lambda i, j: (j, i))
        if number == 1:
            for slot, step in SIDES:

                @pl.loop(0, 2 * RING)
                def _(k):
                    i, j = k // RING, k % RING
                    at = self.term(color, (p.along(a, step), 2 * slot + i, j))
                    mine[at] = (mine[at].astype(F32) + in_h[(twin, slot, *flip(i, j))].astype(F32)).astype(BF)

        if number == 2:

            @pl.loop(0, RING**2)
            def _(k):
                i, j = k // RING, k % RING
                total = mine[self.term(color, (p.at[a], i, j))].astype(F32)
                for slot, _ in SIDES:
                    total = total + in_a[(twin, slot, *flip(i, j))].astype(F32)
                acc_b[i, j] = total
                send_b[i, j] = total.astype(BF)

        if number == 3:
            for slot, step in SIDES:
                i = p.along(b, step)

                @pl.loop(0, 2)
                def _(j):
                    send_b[i, 2 * slot + j] = (acc_b[i, 2 * slot + j] + in_bh[slot, j].astype(F32)).astype(BF)

        if number == 4:

            @pl.loop(0, RING)
            def _(j):
                total = acc_b[p.at[b], j]
                for slot, _ in SIDES:
                    total = total + in_b[slot, j].astype(F32)
                acc_c[j] = total
                send_c[j] = total.astype(BF)

        if number == 5:
            total = acc_c[p.at[c]]
            for slot in AXES:
                total = total + in_c[self.number, slot].astype(F32)
            lo, hi = SHARES[color]
            for k in range(lo, hi):
                self.put(k, total[k - lo])


def scatter_scratch(jobs):
    two, ring = (2,), (RING,)
    groups = []
    for (lo, hi), (a, b, c) in zip(SHARES, SCATTER_ORDERS):
        half = two + ring if b < c else ring + two
        shapes = (
            (two + two + ring + ring, BF), (two + two + half, BF), (ring + ring, F32), (ring + ring, BF), (two + ring, BF), (two + two, BF),
            (ring, F32), (ring, BF), ((jobs, len(STEPS)), BF),
        )
        groups.append([pltpu.VMEM((*shape, hi - lo, PAIR, LANES), kind) for shape, kind in shapes])
    return zip(*groups)


def put_gate_up(out):
    def put(k, unit):
        out[:, part(k, LANES)] = unit.astype(BF)

    return put


def put_down(out):
    def put(k, unit):
        extra = k - D // LANES * 2
        if extra < 0:
            out[part(k % 2, PAIR), part(k // 2, LANES)] = unit.astype(BF)
        else:
            for n in range(2):
                out[part(HIGH - 1, ROWS), part(2 * extra + n, LANES)] = unit[ROWS * n : ROWS * (n + 1)].astype(BF)

    return put


def part(k, size):
    return slice(k * size, (k + 1) * size) if isinstance(k, int) else pl.ds(pl.multiple_of(k * size, size), size)


def blocks(shape, places, **mode):
    return pl.BlockSpec(shape, lambda *at: tuple(at[places[k]] if k in places else 0 for k in range(len(shape))), **mode)


def silu_parts(gate):
    s = jax.nn.sigmoid(gate)
    silu = gate * s
    return silu, s + silu * (1 - s)


FORWARD_STEPS = (8, FF // MXU, 4, 8)
GATHERS = (
    (0, 1, 2, 3, 4, 5, 7),
    (0, 1, 2, 3, 5, 10, 11),
    (0, 1, 2, 4, 10, 12, 13),
    (6, 9, 10, 11, 15, 17, 18),
    (6, 9, 11, 12, 18, 21, 22),
    (6, 9, 11, 15, 19, 21, 22),
)


def forward_kernel(
    g_ref, u_ref, d_ref, x_ref, dy_ref, gu_out, d_out, aT0, gate_up, act1, h1, aT1, act2, dgu2, gu_v, d_v, a_v, h_v, t_v, dy_v, sem, send, recv
):
    place = Place()
    core = place.core
    sems = [sem.at[k] for k in range(sem.shape[0])]

    def copy(src, dst):
        at = sems.pop()
        made = lambda: pltpu.make_async_copy(src, dst, at)
        return lambda: made().start(), lambda: made().wait()

    fetch_x, fetch_dy = copy(x_ref, h_v), copy(dy_ref, dy_v)
    puts = [copy(t_v, aT0), copy(t_v, aT1), copy(gu_v.at[0], gu_out.at[0]), copy(gu_v.at[1], gu_out.at[1]), copy(d_v.at[0], d_out)]
    put_t0, put_t1, *put_w = puts
    fetch_x[0]()
    columns, rows_of_down = gather_parts(core)
    half = rows_of_down[0][-1]
    for n in range(g_ref.shape[0]):
        gu_v[(n, core, *place.at)] = jnp.where(core == 0, g_ref[n], u_ref[n])
        d_v[(n, *place.at, EVERY, EVERY, half)] = d_ref[n, :, :, half]
    entered = enter(place, 1)
    fetch_dy[0]()
    plan = [(gu_v.at[0, core], piece) for piece in columns[:-1]]
    plan += [(d_v.at[0], rows_of_down), (gu_v.at[1, core], columns[-1]), (d_v.at[1], rows_of_down)]
    jobs = [Gather(f"ag{n}", place, *what, send.at[n], recv.at[n]) for n, what in enumerate(plan)]
    prelude, *hooks = spread(jobs, GATHERS, FORWARD_STEPS)
    with jax.named_scope("enter"):
        entered()

    def norm_rows(k):
        rows = part(k, MXU)
        a = normed(h_v[rows])
        a_v[rows] = a
        t_v[:, rows] = a.T

    for step in sorted(prelude):
        prelude[step]()
        if step == 0:
            fetch_x[1]()
        if step < 2:
            with jax.named_scope("norm"):
                pl.loop(RING * step, RING * (step + 1))(norm_rows)
    put_t0[0]()

    def gate_up_body(out_gu, out_act):
        step = pl.program_id(0)
        at_step(hooks[0], step)
        w = [gu_v[0, m, :, :, :, :, part(step, MXU)].reshape(D, MXU) for m in range(2)]
        tall = T // RING
        for k in range(RING):
            rows = part(k, tall)
            gate, up = (dot(a_v[rows], w[m]) for m in range(2))
            for m, val in enumerate((gate, up)):
                out_gu[m, rows] = val
            out_act[rows] = (silu_parts(gate)[0] * up).astype(BF)

    with jax.named_scope("P1"):
        outs = [blocks((2, T, MXU), {2: 0}), blocks((T, MXU), {1: 0})]
        pltpu.emit_pipeline(gate_up_body, grid=(FF // MXU,), out_specs=outs)(gate_up, act1)
    put_t0[1]()

    wide = 512

    def down_body(act, out_h):
        step = pl.program_id(0)
        at_step(hooks[1], step)
        for k in range(wide // MXU):
            rows = part(k, MXU)
            there = part(step * (wide // MXU) + k, MXU)
            out = dot(act[rows], d_v[0].reshape(FF, D)).astype(BF)
            h = (h_v[there].astype(F32) + out.astype(F32)).astype(BF)
            out_h[rows] = h
            a = normed(h)
            a_v[there] = a
            t_v[:, there] = a.T

    with jax.named_scope("P2"):
        pltpu.emit_pipeline(
            down_body, grid=(T // wide,), in_specs=[blocks((wide, FF), {0: 0})], out_specs=[blocks((wide, D), {0: 0})]
        )(act1, h1)
    put_t1[0]()
    fetch_dy[1]()

    for step, put in enumerate(put_w):
        hooks[2][step + 1] = put[0]

    def second_body(out_act, out_dgu):
        col, row = pl.program_id(0), pl.program_id(1)
        at_step(hooks[2], col * (T // wide) + row)
        rows = part(row, wide)
        a, dy = a_v[rows], dy_v[rows]
        wd = d_v[1, pl.ds(2 * col, 2)].reshape(FF // 2 // ROWS, ROWS, D)
        for k in range(FF // 2 // MXU):
            cols = part(k, MXU)
            there = part(col * (FF // 2 // MXU) + k, MXU)
            gate, up = (dot(a, gu_v[1, m, :, :, :, :, there].reshape(D, MXU)) for m in range(2))
            by_act = dot(dy, wd[part(k, MXU // ROWS)].reshape(MXU, D), 1, 1).astype(BF).astype(F32)
            silu, slope = silu_parts(gate)
            out_act[:, cols] = (silu * up).astype(BF)
            for m, val in enumerate((by_act * up * slope, by_act * silu)):
                out_dgu[m, :, cols] = val.astype(BF)

    with jax.named_scope("P3"):
        outs = [blocks((wide, FF // 2), {0: 1, 1: 0}), blocks((2, wide, FF // 2), {1: 1, 2: 0})]
        pltpu.emit_pipeline(second_body, grid=(2, T // wide), out_specs=outs)(act2, dgu2)
    for put in (put_t1, *put_w):
        put[1]()
    for job in jobs:
        job.finish()


def shaped(*shape, kind=BF):
    return jax.ShapeDtypeStruct(shape, kind)


def calls(kernel, number, ins, outs, scratch):
    return pl.pallas_call(
        kernel,
        out_shape=tuple(shape for shape, _ in outs),
        in_specs=ins,
        out_specs=tuple(spec for _, spec in outs),
        scratch_shapes=scratch,
        compiler_params=pltpu.CompilerParams(collective_id=number, has_side_effects=True, vmem_limit_bytes=VMEM),
        name=kernel.__name__,
    )


def forward(wg, wu, wd, x, dy):
    layers, rows = wg.shape[:-1]
    outs = [
        shaped(layers, 2, *CUBE, rows, FF), shaped(*CUBE, HIGH, ROWS, D), shaped(D, T), shaped(2, T, FF, kind=F32), shaped(T, FF),
        shaped(T, D), shaped(D, T), shaped(T, FF), shaped(2, T, FF),
    ]
    scratch = [(layers, 2, *CUBE, rows, FF), (layers, *CUBE, HIGH, ROWS, D), (T, D), (T, D), (D, T), (T, D)]
    sems = [(7,), (6, 3, 16), (6, 3, 16)]
    scratch = [pltpu.VMEM(t, BF) for t in scratch] + [pltpu.SemaphoreType.DMA(t) for t in sems]
    call = calls(forward_kernel, 0, [VM] * 3 + [ANY] * 2, [(t, ANY) for t in outs], scratch)
    return call(wg, wu, wd.reshape(layers, HIGH, ROWS, D), x, dy)


def down_grad(act, by_out, mine, hooks):
    def body(act_cols):
        k = pl.program_id(0)
        at_step(hooks, k)
        val = dot(act_cols[...], by_out[...], 0, 0)
        tiles = D // LANES
        left = None
        for c in range(tiles):
            col = val[:, part(c, LANES)].reshape(RING**2, HIGH, ROWS, LANES)
            mine[k, :, :, 2 * c : 2 * c + 2] = col[:, : HIGH - 1].reshape(RING, RING, 2, PAIR, LANES).astype(BF)
            last = col[:, HIGH - 1 :]
            if c % 2:
                both = jnp.concatenate([left, last], 1).reshape(RING, RING, PAIR, LANES)
                mine[k, :, :, 2 * tiles + c // 2] = both.astype(BF)
            left = last

    pltpu.emit_pipeline(body, grid=(RING,), in_specs=[blocks((T, FF // RING), {1: 0})])(act)


def gate_up_grads(a_t, dgu, mine, hooks):
    wide = 512
    each = FF // wide

    def body(cols):
        k = pl.program_id(0)
        at_step(hooks, k)
        for n in range(wide // MXU):
            val = dot(a_t[...], cols[:, part(n, MXU)])
            for c in range(MXU // LANES):
                col = val[:, part(c, LANES)].reshape(*CUBE, PAIR, LANES).astype(BF)
                mine[1 + k // each, :, :, :, (k % each) * (wide // LANES) + n * (MXU // LANES) + c] = col

    pltpu.emit_pipeline(body, grid=(2 * each,), in_specs=[pl.BlockSpec((None, T, wide), lambda k: (k // each, 0, k % each))])(dgu)


def state_grad(dgu, w, h, by_out, held, out, keep, hooks):
    steps = T // MXU

    def project(d, k, n):
        cols = part(n, MXU)
        by_gate, by_up = (dot(d[m], w[m, cols], 1, 1).astype(BF).astype(F32) for m in range(2))
        held[k % 2, :, cols] = (by_gate + by_up).astype(BF)

    def finish(h, outs, k, n):
        rows = part(n, MXU // RING)
        there = part(jnp.maximum(k - 1, 0) * RING + n, MXU // RING)
        by_a = held[(k + 1) % 2, rows].astype(F32)
        wide = h[rows].astype(F32)
        scale = lax.rsqrt(jnp.mean(wide**2, -1, keepdims=True) + 1e-6)
        inner = jnp.mean(by_a * wide, -1, keepdims=True)
        by_norm = (by_a * scale - wide * (inner * scale * scale * scale)).astype(BF)
        total = (by_out[there].astype(F32) + by_norm.astype(F32)).astype(BF)
        if keep is None:
            outs[0][rows] = total
        else:
            keep[there] = total

    def body(d, h, *outs):
        k = pl.program_id(0)
        at_step(hooks, k)

        @pl.when(k < steps)
        def _():
            for n in range(RING):
                finish(h, outs, k, n)
                project(d, k, n)

        @pl.when(k == steps)
        def _():
            for n in range(RING):
                finish(h, outs, k, n)

    behind = pl.BlockSpec((MXU, D), lambda k: (jnp.maximum(k - 1, 0), 0))
    pltpu.emit_pipeline(
        body,
        grid=(steps + 1,),
        in_specs=[pl.BlockSpec((2, MXU, FF), lambda k: (0, jnp.minimum(k, steps - 1), 0)), behind],
        out_specs=[behind] if keep is None else [],
    )(dgu, h, *([out] if keep is None else []))


def act_grads(gate_up, by_out, w, out, hooks):
    wide = 512

    def body(gu, out):
        col, row = pl.program_id(0), pl.program_id(1)
        at_step(hooks, col * (T // wide) + row)
        by_act = dot(by_out[part(row, wide)], w[part(col, wide)], 1, 1).astype(BF).astype(F32)
        silu, slope = silu_parts(gu[0])
        for m, val in enumerate((by_act * gu[1] * slope, by_act * silu)):
            out[m] = val.astype(BF)

    block = blocks((2, wide, wide), {1: 1, 2: 0})
    ahead = blocks((2, wide, wide), {1: 1, 2: 0}, pipeline_mode=pl.Buffered(3))
    pltpu.emit_pipeline(body, grid=(FF // wide, T // wide), in_specs=[ahead], out_specs=[block])(gate_up, out)


BACKWARD_STEPS = (4, 10, 9, 4, 20, 10, 9, 5)
SCATTERS = (
    (4, 8, 14, 16, 18, 24),
    (9, 16, 21, 24, 26, 31),
    (16, 24, 31, 36, 42, 48),
    (27, 36, 47, 49, 51, 54),
    (52, 55, 60, 62, 64, 67),
    (57, 62, 66, 68, 69, 70),
)


def backward_kernel(
    act2, dy, aT1, dgu2, gu_w, h1, act1, gate_up, d_w, aT0, x, dx, dgu1, d_out, g_out, u_out, dy_w_v, t_v, dh_v, w_v, held, mine, *more
):
    *bufs, sem, send, recv = more
    place = Place()
    sems = [sem.at[k] for k in range(sem.shape[0])]

    def load(src, dst):
        at = sems.pop()
        copy = lambda: pltpu.make_async_copy(src, dst, at)
        return lambda: copy().start(), lambda: copy().wait()

    dy_v = dy_w_v.at[:T]
    loads = (dy, dy_v), (aT1, t_v), (gu_w.at[1], w_v), (aT0, t_v), (d_w, dy_w_v), (gu_w.at[0], w_v)
    fetch_dy, fetch_t, fetch_w, fetch_t0, fetch_d, fetch_w0 = (load(*pair) for pair in loads)
    fetch_dy[0]()
    entered = enter(place, 0)
    groups = [bufs[k : k + len(SHARES)] for k in range(0, len(bufs), len(SHARES))]
    jobs = []
    for layer in (1, 0):
        for k, put in enumerate((put_down(d_out.at[layer]), put_gate_up(g_out.at[layer]), put_gate_up(u_out.at[layer]))):
            n = len(jobs)
            jobs.append(Scatter(place, mine.at[k], put, n, groups, send.at[n], recv.at[n]))
    hooks = spread(jobs, SCATTERS, BACKWARD_STEPS)
    for phase, step, fetch in ((0, 1, fetch_t), (1, 2, fetch_w), (2, 1, fetch_t0), (3, 0, fetch_d), (5, 3, fetch_w0)):
        hooks[phase][step] = fetch[0]
    fetch_dy[1]()
    with jax.named_scope("P4"):
        down_grad(act2, dy_v, mine.at[0], hooks[0])
    entered()
    fetch_t[1]()
    with jax.named_scope("P5"):
        gate_up_grads(t_v, dgu2, mine, hooks[1])
    fetch_w[1]()
    with jax.named_scope("P6"):
        state_grad(dgu2, w_v, h1, dy_v, held, None, dh_v, hooks[2])
    with jax.named_scope("P7"):
        down_grad(act1, dh_v, mine.at[0], hooks[3])
    fetch_d[1]()
    with jax.named_scope("P8"):
        act_grads(gate_up, dh_v, dy_w_v, dgu1, hooks[4])
    fetch_t0[1]()
    with jax.named_scope("P9"):
        gate_up_grads(t_v, dgu1, mine, hooks[5])
    fetch_w0[1]()
    with jax.named_scope("P10"):
        state_grad(dgu1, w_v, x, dh_v, held, dx, None, hooks[6])
    with jax.named_scope("ending"):
        for step in sorted(hooks[7]):
            hooks[7][step]()


def backward(*args):
    n = 6
    sums = [shaped(2, HIGH * ROWS, D), shaped(2, PAIR, FF), shaped(2, PAIR, FF)]
    outs = [(shaped(T, D), ANY), (shaped(2, T, FF), ANY)] + [(t, VM) for t in sums]
    vmem = [(FF, D), (D, T), (T, D), (2, D, FF), (2, MXU, D), (len(sums), *CUBE, UNITS, PAIR, LANES)]
    scratch = [
        *(pltpu.VMEM(t, BF) for t in vmem),
        *(buf for group in scatter_scratch(n) for buf in group),
        pltpu.SemaphoreType.DMA((n,)),
        *[pltpu.SemaphoreType.DMA((n, len(SHARES), Scatter.STARTS[-1]))] * 2,
    ]
    return calls(backward_kernel, 1, [ANY] * len(args), outs, scratch)(*args)


def solution(mesh):
    def step(x, dy, wg, wu, wd):
        x, dy = x[0], dy[0]
        gu, down, aT0, gate_up, act1, h1, aT1, act2, dgu2 = forward(wg, wu, wd, x, dy)
        gu, down = gu.reshape(-1, 2, D, FF), down.reshape(FF, D)
        dx, _, by_d, by_g, by_u = backward(act2, dy, aT1, dgu2, gu, h1, act1, gate_up, down, aT0, x)
        return dx[None], by_g, by_u, by_d

    seq, rows = P(("rep", "dp"), None, None), P(None, "dp", None)
    return jax.shard_map(
        step, mesh=mesh, in_specs=(seq, seq, rows, rows, rows), out_specs=(seq, *[P("rep", "dp", None)] * 3), check_vma=False
    )
```

```python
import jax
import jax.numpy as jnp
from jax import lax
from jax.experimental import pallas as pl
from jax.experimental.pallas import tpu as pltpu
from jax.sharding import PartitionSpec as P

MESH = pl.DeviceIdType.MESH
BF, F32 = jnp.bfloat16, jnp.float32
ANY = pl.BlockSpec(memory_space=pl.ANY)
VM = pl.BlockSpec(memory_space=pltpu.VMEM)
T, D, FF = 2048, 1024, 2560
RING, LANES, ROWS, MXU = 4, 128, 8, 256
PAIR = 2 * ROWS
CUBE = (RING,) * 3
UNITS = 20
HIGH = UNITS * PAIR * LANES // D // ROWS
AXES = range(3)
STEPS = (1, -1, 2)
SIDES = ((0, 1), (1, -1))
EVERY = slice(None)
VMEM = 63 * 2**20

GATHER_ORDERS = ((2, 1, 0), (0, 2, 1), (1, 0, 2))
SCATTER_ORDERS = ((0, 1, 2), (1, 2, 0), (2, 0, 1))
SHARES = ((0, 7), (7, 14), (14, 20))


class Place:
    def __init__(self):
        self.core = lax.axis_index("rep")
        me = lax.axis_index("dp")
        self.at = (me // RING**2, (me // RING) % RING, me % RING)
        self.on = {(a, step): (self.at[a] + (step + RING)) % RING for a in AXES for step in STEPS}

    def along(self, axis, step):
        return self.on[axis, step]

    def peer(self, axis, step):
        x, y, z = (self.along(a, step) if a == axis else self.at[a] for a in AXES)
        return {"dp": (x * RING + y) * RING + z}

    def other(self):
        return {"rep": 1 - self.core}


def enter(place, other):
    barrier = pltpu.get_barrier_semaphore()
    for axis in AXES:
        for step in STEPS:
            pl.semaphore_signal(barrier, inc=1, device_id=place.peer(axis, step), device_id_type=MESH)
    if other:
        pl.semaphore_signal(barrier, inc=1, device_id=place.other(), device_id_type=MESH)
    return lambda: pl.semaphore_wait(barrier, len(STEPS) * len(AXES) + other)


def remote(src, dst, send, recv, device):
    return pltpu.make_async_remote_copy(src_ref=src, dst_ref=dst, send_sem=send, recv_sem=recv, device_id=device, device_id_type=MESH)


def normed(h):
    wide = h.astype(F32)
    scale = lax.rsqrt(jnp.mean(wide**2, -1, keepdims=True) + 1e-6)
    return (wide * scale).astype(BF)


def dot(a, b, over_a=1, over_b=0):
    return lax.dot_general(a, b, (((over_a,), (over_b,)), ((), ())), preferred_element_type=F32)


def at_step(hooks, step):
    for number, hook in hooks.items():
        pl.when(step == number)(hook)


class Gather:
    def __init__(self, name, place, full, parts, send, recv):
        self.name, self.p, self.full, self.parts, self.send, self.recv = name, place, full, parts, send, recv

    STARTS = (0, 3, 5, 7, 10, 14, 16)
    CROSS = (9, 12, 13, 14, 15)

    def view(self, color, where):
        at = [where.get(a, self.p.at[a]) for a in AXES]
        return self.full.at[(*at, *self.parts[color])]

    def copy(self, color, slot):
        a, b, c = GATHER_ORDERS[color]
        p = self.p
        sems = self.send.at[color, slot], self.recv.at[color, slot]
        stage = sum(slot >= first for first in self.STARTS) - 1
        k = slot - self.STARTS[stage]
        if stage == 0:
            block = self.view(color, {})
            return remote(block, block, *sems, p.peer(a, STEPS[k]))
        axis, done, split = (b, {a: EVERY}, a) if stage < 3 else (c, {a: EVERY, b: EVERY}, b)
        side = k % 2
        step, half = STEPS[side], slice(2 * side, 2 * side + 2)
        where = dict(done)
        if stage in (2, 4):
            where[axis] = p.along(axis, -step)
            if slot not in self.CROSS:
                where[split] = half
        if stage == 5:
            where.update({axis: p.along(axis, 2), split: half})
        block = self.view(color, where)
        return remote(block, block, *sems, p.other() if slot in self.CROSS else p.peer(axis, step))

    def stage(self, number):
        last = len(self.STARTS) - 1
        for color in AXES:
            if number == last:
                wait = self.CROSS
            else:
                wait = [k for k in range(self.STARTS[number - 1], self.STARTS[number]) if k not in self.CROSS] if number else ()
            for slot in wait:
                self.copy(color, slot).wait_recv()
            for slot in range(self.STARTS[number], self.STARTS[number + 1]) if number < last else ():
                self.copy(color, slot).start()

    def finish(self):
        for color in AXES:
            for slot in range(self.STARTS[-1]):
                self.copy(color, slot).wait_send()


def gather_parts(core):
    pieces = []
    for widths in ((3, 3, 2), (2, 2, 2), (2, 2, 2)):
        pieces.append([])
        for width in widths:
            first = sum(sum(w for _, w in piece) for piece in pieces)
            pieces[-1].append((first, width))
    whole = [(7 * k, w) for k, w in enumerate((7, 7, 6))]
    columns = [[(EVERY, slice(first * LANES, (first + w) * LANES)) for first, w in piece] for piece in (*pieces, whole)]
    half = part(core, D // 2)
    return columns, [(slice(*cut), EVERY, half) for cut in ((4, 5), (0, 2), (2, 4))]


def slots(*groups):
    def hook():
        for job, stage in groups:
            with jax.named_scope(f"{job.name}_{stage}"):
                job.stage(stage)

    return hook


def spread(jobs, table, sizes):
    plan = {}
    for n, (job, steps) in enumerate(zip(jobs, table, strict=True)):
        for stage, step in enumerate(steps):
            plan.setdefault(step, []).append((-stage, n, job))
    hooks, first = [], 0
    for size in sizes:
        steps = [step for step in sorted(plan) if first <= step < first + size]
        hooks.append({step - first: slots(*((job, -late) for late, _, job in sorted(plan[step], key=lambda t: t[:2]))) for step in steps})
        first += size
    return hooks


class Scatter:
    STARTS = (0, 2, 4, 6, 8, 11)

    def __init__(self, place, mine, put, number, bufs, send, recv, recv_c):
        self.name = f"rs{number}"
        self.p, self.mine, self.put, self.number, self.send, self.recv, self.recv_c = place, mine, put, number, send, recv, recv_c
        self.in_a, self.in_h, self.acc_b, self.send_b, self.in_b, self.in_bh, self.acc_c, self.send_c, self.in_c = bufs

    def term(self, color, where):
        at = dict(zip(SCATTER_ORDERS[color], where))
        return (*(at[axis] for axis in AXES), slice(*SHARES[color]))

    def copy(self, color, slot):
        a, b, c = SCATTER_ORDERS[color]
        p = self.p
        twin = self.number % 2
        stage = sum(slot >= first for first in self.STARTS) - 1
        k = slot - self.STARTS[stage]
        sems = self.send.at[twin, color, slot], self.recv.at[twin, color, slot] if stage < 4 else self.recv_c.at[self.number, color, k]
        step, half = STEPS[k], pl.ds(2 * k, 2)
        if stage == 0:
            src, dst, axis = self.mine.at[self.term(color, (p.along(a, 2), half, EVERY))], self.in_h[color].at[twin, k], a
        elif stage == 1:
            src, dst, axis = self.mine.at[self.term(color, (p.along(a, step), EVERY, EVERY))], self.in_a[color].at[twin, k], a
        elif stage == 2:
            src, dst, axis = self.send_b[color].at[p.along(b, 2), half], self.in_bh[color].at[k], b
        elif stage == 3:
            src, dst, axis = self.send_b[color].at[p.along(b, step)], self.in_b[color].at[k], b
        else:
            src, dst, axis = self.send_c[color].at[p.along(c, step)], self.in_c[color].at[self.number, k], c
        return remote(src, dst, *sems, p.peer(axis, step))

    def stage(self, number):
        last = len(self.STARTS) - 1
        for color, axes in enumerate(SCATTER_ORDERS):
            for slot in range(self.STARTS[number - 1], self.STARTS[number]) if number else ():
                self.copy(color, slot).wait_recv()
            self.sum(number, color, *axes)
            for slot in range(self.STARTS[number], self.STARTS[number + 1]) if number < last else ():
                self.copy(color, slot).start()
            done = {3: self.STARTS[:3:2], 4: self.STARTS[2:5:2], last: self.STARTS[4:]}.get(number)
            for slot in range(*done) if done else ():
                self.copy(color, slot).wait_send()

    def sum(self, number, color, a, b, c):
        p, mine, twin = self.p, self.mine, self.number % 2
        in_a, in_h, acc_b, send_b, in_b, in_bh = (
            t[color] for t in (self.in_a, self.in_h, self.acc_b, self.send_b, self.in_b, self.in_bh)
        )
        acc_c, send_c, in_c = (t[color] for t in (self.acc_c, self.send_c, self.in_c))
        flip = (lambda i, j: (i, j)) if b < c else (lambda i, j: (j, i))
        if number == 1:
            for slot, step in SIDES:

                @pl.loop(0, 2 * RING)
                def _(k):
                    i, j = k // RING, k % RING
                    at = self.term(color, (p.along(a, step), 2 * slot + i, j))
                    mine[at] = (mine[at].astype(F32) + in_h[(twin, slot, *flip(i, j))].astype(F32)).astype(BF)

        if number == 2:

            @pl.loop(0, RING**2)
            def _(k):
                i, j = k // RING, k % RING
                total = mine[self.term(color, (p.at[a], i, j))].astype(F32)
                for slot, _ in SIDES:
                    total = total + in_a[(twin, slot, *flip(i, j))].astype(F32)
                acc_b[i, j] = total
                send_b[i, j] = total.astype(BF)

        if number == 3:
            for slot, step in SIDES:
                i = p.along(b, step)

                @pl.loop(0, 2)
                def _(j):
                    send_b[i, 2 * slot + j] = (acc_b[i, 2 * slot + j] + in_bh[slot, j].astype(F32)).astype(BF)

        if number == 4:

            @pl.loop(0, RING)
            def _(j):
                total = acc_b[p.at[b], j]
                for slot, _ in SIDES:
                    total = total + in_b[slot, j].astype(F32)
                acc_c[j] = total
                send_c[j] = total.astype(BF)

        if number == 5:
            total = acc_c[p.at[c]]
            for slot in AXES:
                total = total + in_c[self.number, slot].astype(F32)
            lo, hi = SHARES[color]
            for k in range(lo, hi):
                self.put(k, total[k - lo])


def scatter_scratch(jobs):
    two, ring = (2,), (RING,)
    groups = []
    for (lo, hi), (a, b, c) in zip(SHARES, SCATTER_ORDERS):
        half = two + ring if b < c else ring + two
        shapes = (
            (two + two + ring + ring, BF), (two + two + half, BF), (ring + ring, F32), (ring + ring, BF), (two + ring, BF), (two + two, BF),
            (ring, F32), (ring, BF), ((jobs, len(STEPS)), BF),
        )
        groups.append([pltpu.VMEM((*shape, hi - lo, PAIR, LANES), kind) for shape, kind in shapes])
    return zip(*groups)


def put_gate_up(out):
    def put(k, unit):
        out[:, part(k, LANES)] = unit.astype(BF)

    return put


def put_down(out):
    def put(k, unit):
        extra = k - D // LANES * 2
        if extra < 0:
            out[part(k % 2, PAIR), part(k // 2, LANES)] = unit.astype(BF)
        else:
            for n in range(2):
                out[part(HIGH - 1, ROWS), part(2 * extra + n, LANES)] = unit[ROWS * n : ROWS * (n + 1)].astype(BF)

    return put


def part(k, size):
    return slice(k * size, (k + 1) * size) if isinstance(k, int) else pl.ds(pl.multiple_of(k * size, size), size)


def blocks(shape, places, **mode):
    return pl.BlockSpec(shape, lambda *at: tuple(at[places[k]] if k in places else 0 for k in range(len(shape))), **mode)


def silu_parts(gate):
    s = jax.nn.sigmoid(gate)
    silu = gate * s
    return silu, s + silu * (1 - s)


FORWARD_STEPS = (9, FF // MXU, 4, 1, 8)
GATHERS = (
    (0, 1, 2, 3, 5, 7, 8),
    (0, 1, 2, 5, 10, 12, 13),
    (0, 1, 2, 7, 12, 15, 16),
    (0, 4, 6, 11, 15, 18, 19),
    (0, 4, 6, 15, 21, 23, 24),
    (0, 4, 6, 13, 17, 22, 24),
)


def forward_kernel(
    g_ref, u_ref, d_ref, x_ref, dy_ref, gu_out, d_out, aT0, gate_up, act1, h1, aT1, act2, dgu2, gu_v, d_v, a_v, h_v, t_v, dy_v, sem, send, recv
):
    place = Place()
    core = place.core
    sems = [sem.at[k] for k in range(sem.shape[0])]

    def copy(src, dst):
        at = sems.pop()
        made = lambda: pltpu.make_async_copy(src, dst, at)
        return lambda: made().start(), lambda: made().wait()

    fetch_x, fetch_dy = copy(x_ref, h_v), copy(dy_ref, dy_v)
    puts = [copy(t_v, aT0), copy(t_v, aT1), copy(gu_v.at[0], gu_out.at[0]), copy(gu_v.at[1], gu_out.at[1]), copy(d_v.at[0], d_out)]
    put_t0, put_t1, *put_w = puts
    fetch_x[0]()
    columns, rows_of_down = gather_parts(core)
    half = rows_of_down[0][-1]
    for n in range(g_ref.shape[0]):
        gu_v[(n, core, *place.at)] = jnp.where(core == 0, g_ref[n], u_ref[n])
        d_v[(n, *place.at, EVERY, EVERY, half)] = d_ref[n, :, :, half]
    entered = enter(place, 1)
    fetch_dy[0]()
    plan = [(gu_v.at[0, core], piece) for piece in columns[:-1]]
    plan += [(d_v.at[0], rows_of_down), (gu_v.at[1, core], columns[-1]), (d_v.at[1], rows_of_down)]
    jobs = [Gather(f"ag{n}", place, *what, send.at[n], recv.at[n]) for n, what in enumerate(plan)]
    prelude, *hooks = spread(jobs, GATHERS, FORWARD_STEPS)
    with jax.named_scope("enter"):
        entered()

    def norm_rows(k):
        rows = part(k, MXU)
        a = normed(h_v[rows])
        a_v[rows] = a
        t_v[:, rows] = a.T

    for step in sorted(prelude):
        prelude[step]()
        if step == 0:
            fetch_x[1]()
        if step < 2:
            with jax.named_scope("norm"):
                pl.loop(RING * step, RING * (step + 1))(norm_rows)
    put_t0[0]()

    def gate_up_body(out_gu, out_act):
        step = pl.program_id(0)
        at_step(hooks[0], step)
        w = [gu_v[0, m, :, :, :, :, part(step, MXU)].reshape(D, MXU) for m in range(2)]
        tall = T // RING
        for k in range(RING):
            rows = part(k, tall)
            gate, up = (dot(a_v[rows], w[m]) for m in range(2))
            for m, val in enumerate((gate, up)):
                out_gu[m, rows] = val
            out_act[rows] = (silu_parts(gate)[0] * up).astype(BF)

    with jax.named_scope("P1"):
        outs = [blocks((2, T, MXU), {2: 0}), blocks((T, MXU), {1: 0})]
        pltpu.emit_pipeline(gate_up_body, grid=(FF // MXU,), out_specs=outs)(gate_up, act1)
    put_t0[1]()

    wide = 512

    def down_body(act, out_h):
        step = pl.program_id(0)
        at_step(hooks[1], step)
        for k in range(wide // MXU):
            rows = part(k, MXU)
            there = part(step * (wide // MXU) + k, MXU)
            out = dot(act[rows], d_v[0].reshape(FF, D)).astype(BF)
            h = (h_v[there].astype(F32) + out.astype(F32)).astype(BF)
            out_h[rows] = h
            a = normed(h)
            a_v[there] = a
            t_v[:, there] = a.T

    with jax.named_scope("P2"):
        pltpu.emit_pipeline(
            down_body, grid=(T // wide,), in_specs=[blocks((wide, FF), {0: 0})], out_specs=[blocks((wide, D), {0: 0})]
        )(act1, h1)
    put_t1[0]()
    fetch_dy[1]()

    for step in sorted(hooks[2]):
        hooks[2][step]()

    for step, put in enumerate(put_w):
        hooks[3][step + 1] = put[0]

    def second_body(out_act, out_dgu):
        col, row = pl.program_id(0), pl.program_id(1)
        at_step(hooks[3], col * (T // wide) + row)
        rows = part(row, wide)
        a, dy = a_v[rows], dy_v[rows]
        wd = d_v[1, pl.ds(2 * col, 2)].reshape(FF // 2 // ROWS, ROWS, D)
        for k in range(FF // 2 // MXU):
            cols = part(k, MXU)
            there = part(col * (FF // 2 // MXU) + k, MXU)
            gate, up = (dot(a, gu_v[1, m, :, :, :, :, there].reshape(D, MXU)) for m in range(2))
            by_act = dot(dy, wd[part(k, MXU // ROWS)].reshape(MXU, D), 1, 1).astype(BF).astype(F32)
            silu, slope = silu_parts(gate)
            out_act[:, cols] = (silu * up).astype(BF)
            for m, val in enumerate((by_act * up * slope, by_act * silu)):
                out_dgu[m, :, cols] = val.astype(BF)

    with jax.named_scope("P3"):
        outs = [blocks((wide, FF // 2), {0: 1, 1: 0}), blocks((2, wide, FF // 2), {1: 1, 2: 0})]
        pltpu.emit_pipeline(second_body, grid=(2, T // wide), out_specs=outs)(act2, dgu2)
    for put in (put_t1, *put_w):
        put[1]()
    for job in jobs:
        job.finish()


def shaped(*shape, kind=BF):
    return jax.ShapeDtypeStruct(shape, kind)


def calls(kernel, number, ins, outs, scratch):
    return pl.pallas_call(
        kernel,
        out_shape=tuple(shape for shape, _ in outs),
        in_specs=ins,
        out_specs=tuple(spec for _, spec in outs),
        scratch_shapes=scratch,
        compiler_params=pltpu.CompilerParams(collective_id=number, has_side_effects=True, vmem_limit_bytes=VMEM),
        name=kernel.__name__,
    )


def forward(wg, wu, wd, x, dy):
    layers, rows = wg.shape[:-1]
    outs = [
        shaped(layers, 2, *CUBE, rows, FF), shaped(*CUBE, HIGH, ROWS, D), shaped(D, T), shaped(2, T, FF, kind=F32), shaped(T, FF),
        shaped(T, D), shaped(D, T), shaped(T, FF), shaped(2, T, FF),
    ]
    scratch = [(layers, 2, *CUBE, rows, FF), (layers, *CUBE, HIGH, ROWS, D), (T, D), (T, D), (D, T), (T, D)]
    sems = [(7,), (6, 3, 16), (6, 3, 16)]
    scratch = [pltpu.VMEM(t, BF) for t in scratch] + [pltpu.SemaphoreType.DMA(t) for t in sems]
    call = calls(forward_kernel, 0, [VM] * 3 + [ANY] * 2, [(t, ANY) for t in outs], scratch)
    return call(wg, wu, wd.reshape(layers, HIGH, ROWS, D), x, dy)


def down_grad(act, by_out, mine, hooks):
    def body(act_cols):
        k = pl.program_id(0)
        at_step(hooks, k)
        val = dot(act_cols[...], by_out[...], 0, 0)
        tiles = D // LANES
        left = None
        for c in range(tiles):
            col = val[:, part(c, LANES)].reshape(RING**2, HIGH, ROWS, LANES)
            mine[k, :, :, 2 * c : 2 * c + 2] = col[:, : HIGH - 1].reshape(RING, RING, 2, PAIR, LANES).astype(BF)
            last = col[:, HIGH - 1 :]
            if c % 2:
                both = jnp.concatenate([left, last], 1).reshape(RING, RING, PAIR, LANES)
                mine[k, :, :, 2 * tiles + c // 2] = both.astype(BF)
            left = last

    pltpu.emit_pipeline(body, grid=(RING,), in_specs=[blocks((T, FF // RING), {1: 0})])(act)


def gate_up_grads(a_t, dgu, mine, hooks):
    wide = 512
    each = FF // wide

    def body(cols):
        k = pl.program_id(0)
        at_step(hooks, k)
        for n in range(wide // MXU):
            val = dot(a_t[...], cols[:, part(n, MXU)])
            for c in range(MXU // LANES):
                col = val[:, part(c, LANES)].reshape(*CUBE, PAIR, LANES).astype(BF)
                mine[1 + k // each, :, :, :, (k % each) * (wide // LANES) + n * (MXU // LANES) + c] = col

    pltpu.emit_pipeline(body, grid=(2 * each,), in_specs=[pl.BlockSpec((None, T, wide), lambda k: (k // each, 0, k % each))])(dgu)


def state_grad(dgu, w, h, by_out, held, out, keep, hooks):
    steps = T // MXU

    def project(d, k, n):
        cols = part(n, MXU)
        by_gate, by_up = (dot(d[m], w[m, cols], 1, 1).astype(BF).astype(F32) for m in range(2))
        held[k % 2, :, cols] = (by_gate + by_up).astype(BF)

    def finish(h, outs, k, n):
        rows = part(n, MXU // RING)
        there = part(jnp.maximum(k - 1, 0) * RING + n, MXU // RING)
        by_a = held[(k + 1) % 2, rows].astype(F32)
        wide = h[rows].astype(F32)
        scale = lax.rsqrt(jnp.mean(wide**2, -1, keepdims=True) + 1e-6)
        inner = jnp.mean(by_a * wide, -1, keepdims=True)
        by_norm = (by_a * scale - wide * (inner * scale * scale * scale)).astype(BF)
        total = (by_out[there].astype(F32) + by_norm.astype(F32)).astype(BF)
        if keep is None:
            outs[0][rows] = total
        else:
            keep[there] = total

    def body(d, h, *outs):
        k = pl.program_id(0)
        at_step(hooks, k)

        @pl.when(k < steps)
        def _():
            for n in range(RING):
                finish(h, outs, k, n)
                project(d, k, n)

        @pl.when(k == steps)
        def _():
            for n in range(RING):
                finish(h, outs, k, n)

    behind = pl.BlockSpec((MXU, D), lambda k: (jnp.maximum(k - 1, 0), 0))
    pltpu.emit_pipeline(
        body,
        grid=(steps + 1,),
        in_specs=[pl.BlockSpec((2, MXU, FF), lambda k: (0, jnp.minimum(k, steps - 1), 0)), behind],
        out_specs=[behind] if keep is None else [],
    )(dgu, h, *([out] if keep is None else []))


def act_grads(gate_up, by_out, w, out, hooks):
    wide = 512

    def body(gu, out):
        col, row = pl.program_id(0), pl.program_id(1)
        at_step(hooks, col * (T // wide) + row)
        for n in range(wide // MXU):
            cols = part(n, MXU)
            by_act = dot(by_out[part(row, wide)], w[part(col * (wide // MXU) + n, MXU)], 1, 1).astype(BF).astype(F32)
            silu, slope = silu_parts(gu[0, :, cols])
            for m, val in enumerate((by_act * gu[1, :, cols] * slope, by_act * silu)):
                out[m, :, cols] = val.astype(BF)

    block = blocks((2, wide, wide), {1: 1, 2: 0})
    ahead = blocks((2, wide, wide), {1: 1, 2: 0}, pipeline_mode=pl.Buffered(3))
    pltpu.emit_pipeline(body, grid=(FF // wide, T // wide), in_specs=[ahead], out_specs=[block])(gate_up, out)


BACKWARD_STEPS = (4, 10, 9, 4, 20, 10, 9, 5)
SCATTERS = (
    (4, 8, 14, 16, 18, 24),
    (9, 16, 21, 24, 26, 31),
    (16, 24, 32, 36, 42, 48),
    (27, 36, 47, 49, 51, 54),
    (52, 55, 59, 61, 63, 67),
    (57, 61, 65, 68, 69, 70),
)


def backward_kernel(
    act2, dy, aT1, dgu2, gu_w, h1, act1, gate_up, d_w, aT0, x, dx, dgu1, d_out, g_out, u_out, dy_w_v, t_v, dh_v, w_v, held, mine, *more
):
    *bufs, sem, send, recv, recv_c = more
    place = Place()
    sems = [sem.at[k] for k in range(sem.shape[0])]

    def load(src, dst):
        at = sems.pop()
        copy = lambda: pltpu.make_async_copy(src, dst, at)
        return lambda: copy().start(), lambda: copy().wait()

    dy_v = dy_w_v.at[:T]
    loads = (dy, dy_v), (aT1, t_v), (gu_w.at[1], w_v), (aT0, t_v), (d_w, dy_w_v), (gu_w.at[0], w_v)
    fetch_dy, fetch_t, fetch_w, fetch_t0, fetch_d, fetch_w0 = (load(*pair) for pair in loads)
    fetch_dy[0]()
    entered = enter(place, 0)
    groups = [bufs[k : k + len(SHARES)] for k in range(0, len(bufs), len(SHARES))]
    jobs = []
    for layer in (1, 0):
        for k, put in enumerate((put_down(d_out.at[layer]), put_gate_up(g_out.at[layer]), put_gate_up(u_out.at[layer]))):
            n = len(jobs)
            jobs.append(Scatter(place, mine.at[k], put, n, groups, send, recv, recv_c))
    hooks = spread(jobs, SCATTERS, BACKWARD_STEPS)
    for phase, step, fetch in ((0, 1, fetch_t), (1, 2, fetch_w), (2, 1, fetch_t0), (3, 0, fetch_d), (5, 3, fetch_w0)):
        hooks[phase][step] = fetch[0]
    fetch_dy[1]()
    with jax.named_scope("P4"):
        down_grad(act2, dy_v, mine.at[0], hooks[0])
    entered()
    fetch_t[1]()
    with jax.named_scope("P5"):
        gate_up_grads(t_v, dgu2, mine, hooks[1])
    fetch_w[1]()
    with jax.named_scope("P6"):
        state_grad(dgu2, w_v, h1, dy_v, held, None, dh_v, hooks[2])
    with jax.named_scope("P7"):
        down_grad(act1, dh_v, mine.at[0], hooks[3])
    fetch_d[1]()
    with jax.named_scope("P8"):
        act_grads(gate_up, dh_v, dy_w_v, dgu1, hooks[4])
    fetch_t0[1]()
    with jax.named_scope("P9"):
        gate_up_grads(t_v, dgu1, mine, hooks[5])
    fetch_w0[1]()
    with jax.named_scope("P10"):
        state_grad(dgu1, w_v, x, dh_v, held, dx, None, hooks[6])
    with jax.named_scope("ending"):
        for step in sorted(hooks[7]):
            hooks[7][step]()


def backward(*args):
    n = 6
    sums = [shaped(2, HIGH * ROWS, D), shaped(2, PAIR, FF), shaped(2, PAIR, FF)]
    outs = [(shaped(T, D), ANY), (shaped(2, T, FF), ANY)] + [(t, VM) for t in sums]
    vmem = [(FF, D), (D, T), (T, D), (2, D, FF), (2, MXU, D), (len(sums), *CUBE, UNITS, PAIR, LANES)]
    scratch = [
        *(pltpu.VMEM(t, BF) for t in vmem),
        *(buf for group in scatter_scratch(n) for buf in group),
        pltpu.SemaphoreType.DMA((n,)),
        pltpu.SemaphoreType.DMA((2, len(SHARES), Scatter.STARTS[-1])),
        pltpu.SemaphoreType.DMA((2, len(SHARES), Scatter.STARTS[4])),
        pltpu.SemaphoreType.DMA((n, len(SHARES), len(STEPS))),
    ]
    return calls(backward_kernel, 1, [ANY] * len(args), outs, scratch)(*args)


def solution(mesh):
    def step(x, dy, wg, wu, wd):
        x, dy = x[0], dy[0]
        gu, down, aT0, gate_up, act1, h1, aT1, act2, dgu2 = forward(wg, wu, wd, x, dy)
        gu, down = gu.reshape(-1, 2, D, FF), down.reshape(FF, D)
        dx, _, by_d, by_g, by_u = backward(act2, dy, aT1, dgu2, gu, h1, act1, gate_up, down, aT0, x)
        return dx[None], by_g, by_u, by_d

    seq, rows = P(("rep", "dp"), None, None), P(None, "dp", None)
    return jax.shard_map(
        step, mesh=mesh, in_specs=(seq, seq, rows, rows, rows), out_specs=(seq, *[P("rep", "dp", None)] * 3), check_vma=False
    )
```

```python
import jax
import jax.numpy as jnp
from jax import lax
from jax.experimental import pallas as pl
from jax.experimental.pallas import tpu as pltpu
from jax.sharding import PartitionSpec as P

MESH = pl.DeviceIdType.MESH
BF, F32 = jnp.bfloat16, jnp.float32
ANY = pl.BlockSpec(memory_space=pl.ANY)
VM = pl.BlockSpec(memory_space=pltpu.VMEM)
T, D, FF = 2048, 1024, 2560
RING, LANES, ROWS, MXU = 4, 128, 8, 256
PAIR = 2 * ROWS
CUBE = (RING,) * 3
UNITS = 20
HIGH = UNITS * PAIR * LANES // D // ROWS
AXES = range(3)
BOTH = range(2)
STEPS = (1, -1, 2)
SIDES = ((0, 1), (1, -1))
EVERY = slice(None)
VMEM = 67_043_328

GATHER_ORDERS = ((2, 1, 0), (0, 2, 1), (1, 0, 2))
SCATTER_ORDERS = ((0, 1, 2), (1, 2, 0), (2, 0, 1))
SHARES = ((0, 7), (7, 14), (14, 20))


class Place:
    def __init__(self):
        self.core = lax.axis_index("rep")
        me = lax.axis_index("dp")
        self.at = (me // RING**2, (me // RING) % RING, me % RING)
        self.on = {(a, step): (self.at[a] + (step + RING)) % RING for a in AXES for step in STEPS}

    def along(self, axis, step):
        return self.on[axis, step]

    def peer(self, axis, step):
        x, y, z = (self.along(a, step) if a == axis else self.at[a] for a in AXES)
        return {"dp": (x * RING + y) * RING + z}

    def other(self):
        return {"rep": 1 - self.core}


def enter(place, other):
    barrier = pltpu.get_barrier_semaphore()
    for axis in AXES:
        for step in STEPS:
            pl.semaphore_signal(barrier, inc=1, device_id=place.peer(axis, step), device_id_type=MESH)
    if other:
        pl.semaphore_signal(barrier, inc=1, device_id=place.other(), device_id_type=MESH)
    return lambda: pl.semaphore_wait(barrier, len(STEPS) * len(AXES) + other)


def remote(src, dst, send, recv, device):
    return pltpu.make_async_remote_copy(src_ref=src, dst_ref=dst, send_sem=send, recv_sem=recv, device_id=device, device_id_type=MESH)


def normed(h):
    wide = h.astype(F32)
    scale = lax.rsqrt(jnp.mean(wide**2, -1, keepdims=True) + 1e-6)
    return (wide * scale).astype(BF)


def dot(a, b, over_a=1, over_b=0):
    return lax.dot_general(a, b, (((over_a,), (over_b,)), ((), ())), preferred_element_type=F32)


def at_step(hooks, step):
    for number, hook in hooks.items():
        pl.when(step == number)(hook)


class Gather:
    def __init__(self, name, place, full, parts, send, recv):
        self.name, self.p, self.full, self.parts, self.send, self.recv = name, place, full, parts, send, recv

    STARTS = (0, 3, 5, 7, 10, 14, 16)
    CROSS = (9, 12, 13, 14, 15)

    def view(self, color, where):
        at = [where.get(a, self.p.at[a]) for a in AXES]
        return self.full.at[(*at, *self.parts[color])]

    def copy(self, color, slot):
        a, b, c = GATHER_ORDERS[color]
        p = self.p
        sems = self.send.at[color, slot], self.recv.at[color, slot]
        stage = sum(slot >= first for first in self.STARTS) - 1
        k = slot - self.STARTS[stage]
        if stage == 0:
            block = self.view(color, {})
            return remote(block, block, *sems, p.peer(a, STEPS[k]))
        axis, done, split = (b, {a: EVERY}, a) if stage < 3 else (c, {a: EVERY, b: EVERY}, b)
        side = k % 2
        step, half = STEPS[side], slice(2 * side, 2 * side + 2)
        where = dict(done)
        if stage in (2, 4):
            where[axis] = p.along(axis, -step)
            if slot not in self.CROSS:
                where[split] = half
        if stage == 5:
            where.update({axis: p.along(axis, 2), split: half})
        block = self.view(color, where)
        return remote(block, block, *sems, p.other() if slot in self.CROSS else p.peer(axis, step))

    def stage(self, number):
        last = len(self.STARTS) - 1
        for color in AXES:
            if number == last:
                wait = self.CROSS
            else:
                wait = [k for k in range(self.STARTS[number - 1], self.STARTS[number]) if k not in self.CROSS] if number else ()
            for slot in wait:
                self.copy(color, slot).wait_recv()
            for slot in range(self.STARTS[number], self.STARTS[number + 1]) if number < last else ():
                self.copy(color, slot).start()

    def finish(self):
        for color in AXES:
            for slot in range(self.STARTS[-1]):
                self.copy(color, slot).wait_send()


def gather_parts(core):
    pieces = []
    for widths in ((3, 3, 2), (2, 2, 2), (2, 2, 2)):
        pieces.append([])
        for width in widths:
            first = sum(sum(w for _, w in piece) for piece in pieces)
            pieces[-1].append((first, width))
    whole = [(lo, hi - lo) for lo, hi in SHARES]
    columns = [[(EVERY, slice(first * LANES, (first + w) * LANES)) for first, w in piece] for piece in (*pieces, whole)]
    half = part(core, D // 2)
    return columns, [(slice(*cut), EVERY, half) for cut in ((4, 5), (0, 2), (2, 4))]


def slots(*groups):
    def hook():
        for job, stage in groups:
            with jax.named_scope(f"{job.name}_{stage}"):
                job.stage(stage)

    return hook


def spread(jobs, table, sizes):
    plan = {}
    for n, (job, steps) in enumerate(zip(jobs, table, strict=True)):
        for stage, step in enumerate(steps):
            plan.setdefault(step, []).append((-stage, n, job))
    hooks, first = [], 0
    for size in sizes:
        steps = [step for step in sorted(plan) if first <= step < first + size]
        hooks.append({step - first: slots(*((job, -late) for late, _, job in sorted(plan[step], key=lambda t: t[:2]))) for step in steps})
        first += size
    return hooks


class Scatter:
    STARTS = (0, 2, 4, 6, 8, 11)

    def __init__(self, place, mine, put, number, bufs, send, recv, recv_c):
        self.name = f"rs{number}"
        self.p, self.mine, self.put, self.number, self.send, self.recv, self.recv_c = place, mine, put, number, send, recv, recv_c
        self.in_a, self.in_h, self.acc_b, self.send_b, self.in_b, self.in_bh, self.acc_c, self.send_c, self.in_c = bufs

    def term(self, color, where):
        at = dict(zip(SCATTER_ORDERS[color], where))
        return (*(at[axis] for axis in AXES), slice(*SHARES[color]))

    def copy(self, color, slot):
        a, b, c = SCATTER_ORDERS[color]
        p = self.p
        twin = self.number % 2
        stage = sum(slot >= first for first in self.STARTS) - 1
        k = slot - self.STARTS[stage]
        sems = self.send.at[twin, color, slot], self.recv.at[twin, color, slot] if stage < 4 else self.recv_c.at[self.number, color, k]
        step, half = STEPS[k], pl.ds(2 * k, 2)
        if stage == 0:
            src, dst, axis = self.mine.at[self.term(color, (p.along(a, 2), half, EVERY))], self.in_h[color].at[twin, k], a
        elif stage == 1:
            src, dst, axis = self.mine.at[self.term(color, (p.along(a, step), EVERY, EVERY))], self.in_a[color].at[twin, k], a
        elif stage == 2:
            src, dst, axis = self.send_b[color].at[p.along(b, 2), half], self.in_bh[color].at[k], b
        elif stage == 3:
            src, dst, axis = self.send_b[color].at[p.along(b, step)], self.in_b[color].at[k], b
        else:
            src, dst, axis = self.send_c[color].at[p.along(c, step)], self.in_c[color].at[self.number, k], c
        return remote(src, dst, *sems, p.peer(axis, step))

    def stage(self, number):
        last = len(self.STARTS) - 1
        for color, axes in enumerate(SCATTER_ORDERS):
            for slot in range(self.STARTS[number - 1], self.STARTS[number]) if number else ():
                self.copy(color, slot).wait_recv()
            self.sum(number, color, *axes)
            for slot in range(self.STARTS[number], self.STARTS[number + 1]) if number < last else ():
                self.copy(color, slot).start()
            done = {3: self.STARTS[:3:2], 4: self.STARTS[2:5:2], last: self.STARTS[4:]}.get(number)
            for slot in range(*done) if done else ():
                self.copy(color, slot).wait_send()

    def sum(self, number, color, a, b, c):
        p, mine, twin = self.p, self.mine, self.number % 2
        in_a, in_h, acc_b, send_b, in_b, in_bh = (
            t[color] for t in (self.in_a, self.in_h, self.acc_b, self.send_b, self.in_b, self.in_bh)
        )
        acc_c, send_c, in_c = (t[color] for t in (self.acc_c, self.send_c, self.in_c))
        flip = (lambda i, j: (i, j)) if b < c else (lambda i, j: (j, i))
        if number == 1:
            for slot, step in SIDES:

                @pl.loop(0, 2 * RING)
                def _(k):
                    i, j = k // RING, k % RING
                    at = self.term(color, (p.along(a, step), 2 * slot + i, j))
                    mine[at] = (mine[at].astype(F32) + in_h[(twin, slot, *flip(i, j))].astype(F32)).astype(BF)

        if number == 2:

            @pl.loop(0, RING**2)
            def _(k):
                i, j = k // RING, k % RING
                total = mine[self.term(color, (p.at[a], i, j))].astype(F32)
                for slot, _ in SIDES:
                    total = total + in_a[(twin, slot, *flip(i, j))].astype(F32)
                acc_b[i, j] = total
                send_b[i, j] = total.astype(BF)

        if number == 3:
            for slot, step in SIDES:
                i = p.along(b, step)

                @pl.loop(0, 2)
                def _(j):
                    send_b[i, 2 * slot + j] = (acc_b[i, 2 * slot + j] + in_bh[slot, j].astype(F32)).astype(BF)

        if number == 4:

            @pl.loop(0, RING)
            def _(j):
                total = acc_b[p.at[b], j]
                for slot, _ in SIDES:
                    total = total + in_b[slot, j].astype(F32)
                acc_c[j] = total
                send_c[j] = total.astype(BF)

        if number == 5:
            total = acc_c[p.at[c]]
            for slot in AXES:
                total = total + in_c[self.number, slot].astype(F32)
            lo, hi = SHARES[color]
            for k in range(lo, hi):
                self.put(k, total[k - lo])


def scatter_scratch(jobs):
    two, ring = (2,), (RING,)
    groups = []
    for (lo, hi), (a, b, c) in zip(SHARES, SCATTER_ORDERS):
        half = two + ring if b < c else ring + two
        shapes = (
            (two + two + ring + ring, BF), (two + two + half, BF), (ring + ring, F32), (ring + ring, BF), (two + ring, BF), (two + two, BF),
            (ring, F32), (ring, BF), ((jobs, len(STEPS)), BF),
        )
        groups.append([pltpu.VMEM((*shape, hi - lo, PAIR, LANES), kind) for shape, kind in shapes])
    return zip(*groups)


def put_gate_up(out):
    def put(k, unit):
        out[:, part(k, LANES)] = unit.astype(BF)

    return put


def put_half(outs, half):
    def put(k, unit):
        which, col = k // (UNITS // 2), k % (UNITS // 2) + half * (UNITS // 2)
        outs[which][:, part(col, LANES)] = unit.astype(BF)

    return put


def put_down(out):
    def put(k, unit):
        extra = k - D // LANES * 2
        if extra < 0:
            out[part(k % 2, PAIR), part(k // 2, LANES)] = unit.astype(BF)
        else:
            for n in BOTH:
                out[part(HIGH - 1, ROWS), part(2 * extra + n, LANES)] = unit[ROWS * n : ROWS * (n + 1)].astype(BF)

    return put


def part(k, size):
    return slice(k * size, (k + 1) * size) if isinstance(k, int) else pl.ds(pl.multiple_of(k * size, size), size)


def blocks(shape, places, **mode):
    return pl.BlockSpec(shape, lambda *at: tuple(at[places[k]] if k in places else 0 for k in range(len(shape))), **mode)


def silu_parts(gate):
    s = jax.nn.sigmoid(gate)
    silu = gate * s
    return silu, s + silu * (1 - s)


FORWARD_STEPS = (9, FF // MXU, 4, 1, 8)
GATHERS = (
    (0, 1, 2, 3, 5, 7, 8),
    (0, 1, 2, 5, 10, 12, 13),
    (0, 1, 2, 7, 12, 15, 16),
    (0, 4, 6, 11, 15, 18, 19),
    (0, 4, 6, 15, 21, 23, 24),
    (0, 4, 6, 13, 17, 22, 24),
)


def forward_kernel(
    g_ref, u_ref, d_ref, x_ref, dy_ref, gu_out, d_out, aT0, gate_up, act1, h1, aT1, act2, dgu2, gu_v, d_v, a_v, h_v, t_v, dy_v, sem, send, recv
):
    place = Place()
    core = place.core
    sems = [sem.at[k] for k in range(sem.shape[0])]

    def copy(src, dst):
        at = sems.pop()
        made = lambda: pltpu.make_async_copy(src, dst, at)
        return lambda: made().start(), lambda: made().wait()

    fetch_x, fetch_dy = copy(x_ref, h_v), copy(dy_ref, dy_v)
    puts = [copy(t_v, aT0), copy(t_v, aT1), copy(gu_v.at[0], gu_out.at[0]), copy(gu_v.at[1], gu_out.at[1]), copy(d_v.at[0], d_out)]
    put_t0, put_t1, *put_w = puts
    fetch_x[0]()
    columns, rows_of_down = gather_parts(core)
    half = rows_of_down[0][-1]
    for n in range(g_ref.shape[0]):
        gu_v[(n, core, *place.at)] = jnp.where(core == 0, g_ref[n], u_ref[n])
        d_v[(n, *place.at, EVERY, EVERY, half)] = d_ref[n, :, :, half]
    entered = enter(place, 1)
    fetch_dy[0]()
    plan = [(gu_v.at[0, core], piece) for piece in columns[:-1]]
    plan += [(d_v.at[0], rows_of_down), (gu_v.at[1, core], columns[-1]), (d_v.at[1], rows_of_down)]
    jobs = [Gather(f"ag{n}", place, *what, send.at[n], recv.at[n]) for n, what in enumerate(plan)]
    prelude, *hooks = spread(jobs, GATHERS, FORWARD_STEPS)
    with jax.named_scope("enter"):
        entered()

    def norm_rows(k):
        rows = part(k, MXU)
        a = normed(h_v[rows])
        a_v[rows] = a
        t_v[:, rows] = a.T

    for step in sorted(prelude):
        prelude[step]()
        if step == 0:
            fetch_x[1]()
        if step < 2:
            with jax.named_scope("norm"):
                pl.loop(RING * step, RING * (step + 1))(norm_rows)
    put_t0[0]()

    def gate_up_body(out_gu, out_act):
        step = pl.program_id(0)
        at_step(hooks[0], step)
        w = [gu_v[0, m, :, :, :, :, part(step, MXU)].reshape(D, MXU) for m in BOTH]
        tall = T // RING
        for k in range(RING):
            rows = part(k, tall)
            gate, up = (dot(a_v[rows], w[m]) for m in BOTH)
            for m, val in enumerate((gate, up)):
                out_gu[m, rows] = val
            out_act[rows] = (silu_parts(gate)[0] * up).astype(BF)

    with jax.named_scope("P1"):
        outs = [blocks((2, T, MXU), {2: 0}), blocks((T, MXU), {1: 0})]
        pltpu.emit_pipeline(gate_up_body, grid=(FF // MXU,), out_specs=outs)(gate_up, act1)
    put_t0[1]()

    wide = 512

    def down_body(act, out_h):
        step = pl.program_id(0)
        at_step(hooks[1], step)
        for k in range(wide // MXU):
            rows = part(k, MXU)
            there = part(step * (wide // MXU) + k, MXU)
            out = dot(act[rows], d_v[0].reshape(FF, D)).astype(BF)
            h = (h_v[there].astype(F32) + out.astype(F32)).astype(BF)
            out_h[rows] = h
            a = normed(h)
            a_v[there] = a
            t_v[:, there] = a.T

    with jax.named_scope("P2"):
        pltpu.emit_pipeline(
            down_body, grid=(T // wide,), in_specs=[blocks((wide, FF), {0: 0})], out_specs=[blocks((wide, D), {0: 0})]
        )(act1, h1)
    put_t1[0]()
    fetch_dy[1]()

    for step in sorted(hooks[2]):
        hooks[2][step]()

    for step, put in enumerate(put_w):
        hooks[3][step + 1] = put[0]

    def second_body(out_act, out_dgu):
        col, row = pl.program_id(0), pl.program_id(1)
        at_step(hooks[3], col * (T // wide) + row)
        rows = part(row, wide)
        a, dy = a_v[rows], dy_v[rows]
        wd = d_v[1, pl.ds(2 * col, 2)].reshape(FF // 2 // ROWS, ROWS, D)
        for k in range(FF // 2 // MXU):
            cols = part(k, MXU)
            there = part(col * (FF // 2 // MXU) + k, MXU)
            gate, up = (dot(a, gu_v[1, m, :, :, :, :, there].reshape(D, MXU)) for m in BOTH)
            by_act = dot(dy, wd[part(k, MXU // ROWS)].reshape(MXU, D), 1, 1).astype(BF).astype(F32)
            silu, slope = silu_parts(gate)
            out_act[:, cols] = (silu * up).astype(BF)
            for m, val in enumerate((by_act * up * slope, by_act * silu)):
                out_dgu[m, :, cols] = val.astype(BF)

    with jax.named_scope("P3"):
        outs = [blocks((wide, FF // 2), {0: 1, 1: 0}), blocks((2, wide, FF // 2), {1: 1, 2: 0})]
        pltpu.emit_pipeline(second_body, grid=(2, T // wide), out_specs=outs)(act2, dgu2)
    for put in (put_t1, *put_w):
        put[1]()
    for job in jobs:
        job.finish()


def shaped(*shape, kind=BF):
    return jax.ShapeDtypeStruct(shape, kind)


def calls(kernel, number, ins, outs, scratch):
    return pl.pallas_call(
        kernel,
        out_shape=tuple(shape for shape, _ in outs),
        in_specs=ins,
        out_specs=tuple(spec for _, spec in outs),
        scratch_shapes=scratch,
        compiler_params=pltpu.CompilerParams(collective_id=number, has_side_effects=True, vmem_limit_bytes=VMEM),
        name=kernel.__name__,
    )


def forward(wg, wu, wd, x, dy):
    layers, rows = wg.shape[:-1]
    outs = [
        shaped(layers, 2, *CUBE, rows, FF), shaped(*CUBE, HIGH, ROWS, D), shaped(D, T), shaped(2, T, FF, kind=F32), shaped(T, FF),
        shaped(T, D), shaped(D, T), shaped(T, FF), shaped(2, T, FF),
    ]
    scratch = [(layers, 2, *CUBE, rows, FF), (layers, *CUBE, HIGH, ROWS, D), (T, D), (T, D), (D, T), (T, D)]
    sems = [(7,), (6, 3, 16), (6, 3, 16)]
    scratch = [pltpu.VMEM(t, BF) for t in scratch] + [pltpu.SemaphoreType.DMA(t) for t in sems]
    call = calls(forward_kernel, 0, [VM] * 3 + [ANY] * 2, [(t, ANY) for t in outs], scratch)
    return call(wg, wu, wd.reshape(layers, HIGH, ROWS, D), x, dy)


def down_grad(act, by_out, mine, hooks):
    def body(act_cols):
        k = pl.program_id(0)
        at_step(hooks, k)
        val = dot(act_cols[...], by_out[...], 0, 0)
        tiles = D // LANES
        left = None
        for c in range(tiles):
            col = val[:, part(c, LANES)].reshape(RING**2, HIGH, ROWS, LANES)
            mine[k, :, :, 2 * c : 2 * c + 2] = col[:, : HIGH - 1].reshape(RING, RING, 2, PAIR, LANES).astype(BF)
            last = col[:, HIGH - 1 :]
            if c % 2:
                both = jnp.concatenate([left, last], 1).reshape(RING, RING, PAIR, LANES)
                mine[k, :, :, 2 * tiles + c // 2] = both.astype(BF)
            left = last

    pltpu.emit_pipeline(body, grid=(RING,), in_specs=[blocks((T, FF // RING), {1: 0})])(act)


def gate_up_grads(a_t, dgu, mine, hooks):
    wide = 512
    each = FF // wide

    def body(cols):
        k = pl.program_id(0)
        at_step(hooks, k)
        for n in range(wide // MXU):
            val = dot(a_t[...], cols[:, part(n, MXU)])
            for c in range(MXU // LANES):
                col = val[:, part(c, LANES)].reshape(*CUBE, PAIR, LANES).astype(BF)
                mine[1 + k // each, :, :, :, (k % each) * (wide // LANES) + n * (MXU // LANES) + c] = col

    pltpu.emit_pipeline(body, grid=(2 * each,), in_specs=[pl.BlockSpec((None, T, wide), lambda k: (k // each, 0, k % each))])(dgu)


def state_grad(dgu, w, h, by_out, held, out, keep, hooks):
    steps = T // MXU

    def project(d, k, n):
        cols = part(n, MXU)
        by_gate, by_up = (dot(d[m], w[m, cols], 1, 1).astype(BF).astype(F32) for m in BOTH)
        held[k % 2, :, cols] = (by_gate + by_up).astype(BF)

    def finish(h, outs, k, n):
        rows = part(n, MXU // RING)
        there = part(jnp.maximum(k - 1, 0) * RING + n, MXU // RING)
        by_a = held[(k + 1) % 2, rows].astype(F32)
        wide = h[rows].astype(F32)
        scale = lax.rsqrt(jnp.mean(wide**2, -1, keepdims=True) + 1e-6)
        inner = jnp.mean(by_a * wide, -1, keepdims=True)
        by_norm = (by_a * scale - wide * (inner * scale * scale * scale)).astype(BF)
        total = (by_out[there].astype(F32) + by_norm.astype(F32)).astype(BF)
        if keep is None:
            outs[0][rows] = total
        else:
            keep[there] = total

    def body(d, h, *outs):
        k = pl.program_id(0)
        at_step(hooks, k)

        @pl.when(k < steps)
        def _():
            for n in range(RING):
                finish(h, outs, k, n)
                project(d, k, n)

        @pl.when(k == steps)
        def _():
            for n in range(RING):
                finish(h, outs, k, n)

    behind = pl.BlockSpec((MXU, D), lambda k: (jnp.maximum(k - 1, 0), 0))
    now = lambda k: jnp.minimum(k, steps - 1)
    if len(dgu.shape) > 3:
        each = steps // 2
        source = pl.BlockSpec((2, None, MXU, FF), lambda k: (0, now(k) // each, now(k) % each, 0))
    else:
        source = pl.BlockSpec((2, MXU, FF), lambda k: (0, now(k), 0))
    pltpu.emit_pipeline(
        body,
        grid=(steps + 1,),
        in_specs=[source, behind],
        out_specs=[behind] if keep is None else [],
    )(dgu, h, *([out] if keep is None else []))


def layer_grads(gate_up, by_out, w, a_t, mine, held, out, sem, hooks, fetch):
    steps = FF // MXU
    pairs = steps // 2

    def held_at(k, m):
        return part(2 * (k % pairs) + m, MXU)

    def moves(k):
        for m in BOTH:
            for n in BOTH:
                yield pltpu.make_async_copy(held.at[n, :, held_at(k, m)], out.at[m, n, :, part(k, MXU)], sem.at[k % 2, m, n])

    def act(gu, k, r):
        rows = part(r, T // RING)
        by_act = dot(by_out[rows], w[part(k, MXU)], 1, 1).astype(BF).astype(F32)
        silu, slope = silu_parts(gu[0, rows])
        for m, val in enumerate((by_act * gu[1, rows] * slope, by_act * silu)):
            held[r // 2, part(r % 2, T // RING), held_at(k, m)] = val.astype(BF)

    def weights(k, r):
        m, h = r // 2, r % 2
        val = dot(a_t[part(h, D // 2)], held[:, :, held_at(k, m)].reshape(T, MXU))
        for c in range(MXU // LANES):
            unit = m * (UNITS // 2) + (k % pairs) * (MXU // LANES) + c
            mine[1 + k // pairs, 2 * h : 2 * h + 2, :, :, unit] = val[:, part(c, LANES)].reshape(2, RING, RING, PAIR, LANES).astype(BF)

    def body(gu):
        k = pl.program_id(0)
        at_step(hooks, k)

        @pl.when(k >= 1)
        def _():
            for copy in moves(k - 1):
                copy.start()

        @pl.when(k >= 2)
        def _():
            for copy in moves(k - 2):
                copy.wait()

        @pl.when(k == 0)
        def _():
            for r in range(RING):
                act(gu, k, r)

        @pl.when((k > 0) & (k < steps))
        def _():
            for r in range(RING):
                weights(k - 1, r)
                act(gu, k, r)

        @pl.when(k == steps)
        def _():
            fetch()
            for r in range(RING):
                weights(k - 1, r)

    block = pl.BlockSpec((2, T, MXU), lambda k: (0, 0, jnp.minimum(k, steps - 1)))
    pltpu.emit_pipeline(body, grid=(steps + 1,), in_specs=[block])(gate_up)
    for copy in moves(steps - 1):
        copy.wait()


BACKWARD_STEPS = (4, 10, 9, 4, 11, 9, 6)
SCATTERS = (
    (4, 8, 14, 16, 18, 24),
    (9, 16, 21, 24, 26, 29),
    (16, 24, 29, 30, 33, 35),
    (27, 30, 35, 37, 41, 43),
    (33, 36, 41, 43, 47, 50),
    (38, 42, 48, 49, 51, 52),
)


def backward_kernel(
    act2, dy, aT1, dgu2, gu_w, h1, act1, gate_up, d_w, aT0, x, dx, dgu1, d_out, g_out, u_out, dy_w_v, t_v, dh_v, w_v, held, mine, *more
):
    *bufs, sem, move_sem, send, recv, recv_c = more
    place = Place()
    sems = [sem.at[k] for k in range(sem.shape[0])]

    def load(src, dst):
        at = sems.pop()
        copy = lambda: pltpu.make_async_copy(src, dst, at)
        return lambda: copy().start(), lambda: copy().wait()

    dy_v = dy_w_v.at[:T]
    early, late = slice(0, FF - 2 * MXU), slice(FF - 2 * MXU, FF)
    loads = [(dy, dy_v), (aT1, t_v), (gu_w.at[1], w_v), (aT0, t_v), (d_w, dy_w_v)]
    loads += [(gu_w.at[0, :, :, cols], w_v.at[:, :, cols]) for cols in (early, late)]
    fetch_dy, fetch_t, fetch_w, fetch_t0, fetch_d, *fetch_w0 = (load(*pair) for pair in loads)
    fetch_dy[0]()
    entered = enter(place, 0)
    groups = [bufs[k : k + len(SHARES)] for k in range(0, len(bufs), len(SHARES))]
    jobs = []
    halves = [put_half((g_out.at[0], u_out.at[0]), half) for half in BOTH]
    for puts in ((put_down(d_out.at[1]), put_gate_up(g_out.at[1]), put_gate_up(u_out.at[1])), (put_down(d_out.at[0]), *halves)):
        for k, put in enumerate(puts):
            n = len(jobs)
            jobs.append(Scatter(place, mine.at[k], put, n, groups, send, recv, recv_c))
    hooks = spread(jobs, SCATTERS, BACKWARD_STEPS)
    for phase, step, fetch in ((0, 1, fetch_t), (1, 2, fetch_w), (2, 1, fetch_t0), (3, 0, fetch_d)):
        hooks[phase][step] = fetch[0]
    fetch_dy[1]()
    with jax.named_scope("P4"):
        down_grad(act2, dy_v, mine.at[0], hooks[0])
    entered()
    fetch_t[1]()
    with jax.named_scope("P5"):
        gate_up_grads(t_v, dgu2, mine, hooks[1])
    fetch_w[1]()
    with jax.named_scope("P6"):
        state_grad(dgu2, w_v, h1, dy_v, held, None, dh_v, hooks[2])
    with jax.named_scope("P7"):
        down_grad(act1, dh_v, mine.at[0], hooks[3])
    fetch_d[1]()
    fetch_t0[1]()
    with jax.named_scope("P8"):
        layer_grads(gate_up, dh_v, dy_w_v, t_v, mine, w_v, dgu1, move_sem, hooks[4], fetch_w0[0][0])
    fetch_w0[1][0]()
    begin = hooks[5][0]

    def arrived():
        for fetch in fetch_w0:
            fetch[1]()
        begin()

    hooks[5][0] = arrived
    with jax.named_scope("P10"):
        state_grad(dgu1, w_v, x, dh_v, held, dx, None, hooks[5])
    with jax.named_scope("ending"):
        for step in sorted(hooks[6]):
            hooks[6][step]()


def backward(*args):
    n = 6
    sums = [shaped(2, HIGH * ROWS, D), shaped(2, PAIR, FF), shaped(2, PAIR, FF)]
    outs = [(shaped(T, D), ANY), (shaped(2, 2, T // 2, FF), ANY)] + [(t, VM) for t in sums]
    vmem = [(FF, D), (D, T), (T, D), (2, D, FF), (2, MXU, D), (len(sums), *CUBE, UNITS, PAIR, LANES)]
    scratch = [
        *(pltpu.VMEM(t, BF) for t in vmem),
        *(buf for group in scatter_scratch(n) for buf in group),
        pltpu.SemaphoreType.DMA((n + 1,)),
        pltpu.SemaphoreType.DMA((2, 2, 2)),
        pltpu.SemaphoreType.DMA((2, len(SHARES), Scatter.STARTS[-1])),
        pltpu.SemaphoreType.DMA((2, len(SHARES), Scatter.STARTS[4])),
        pltpu.SemaphoreType.DMA((n, len(SHARES), len(STEPS))),
    ]
    return calls(backward_kernel, 1, [ANY] * len(args), outs, scratch)(*args)


def solution(mesh):
    def step(x, dy, wg, wu, wd):
        x, dy = x[0], dy[0]
        gu, down, aT0, gate_up, act1, h1, aT1, act2, dgu2 = forward(wg, wu, wd, x, dy)
        gu, down = gu.reshape(-1, 2, D, FF), down.reshape(FF, D)
        dx, _, by_d, by_g, by_u = backward(act2, dy, aT1, dgu2, gu, h1, act1, gate_up, down, aT0, x)
        return dx[None], by_g, by_u, by_d

    seq, rows = P(("rep", "dp"), None, None), P(None, "dp", None)
    return jax.shard_map(
        step, mesh=mesh, in_specs=(seq, seq, rows, rows, rows), out_specs=(seq, *[P("rep", "dp", None)] * 3), check_vma=False
    )
```

```python
import jax
import jax.numpy as jnp
from jax import lax
from jax.experimental import pallas as pl
from jax.experimental.pallas import tpu as pltpu
from jax.sharding import PartitionSpec as P

MESH = pl.DeviceIdType.MESH
BF, F32 = jnp.bfloat16, jnp.float32
ANY = pl.BlockSpec(memory_space=pl.ANY)
VM = pl.BlockSpec(memory_space=pltpu.VMEM)
T, D, FF = 2048, 1024, 2560
RING, LANES, ROWS, MXU = 4, 128, 8, 256
PAIR = 2 * ROWS
CUBE = (RING,) * 3
UNITS = 20
HIGH = UNITS * PAIR * LANES // D // ROWS
AXES = range(3)
BOTH = range(2)
STEPS = (1, -1, 2)
SIDES = ((0, 1), (1, -1))
EVERY = slice(None)
VMEM = 67_043_328

GATHER_ORDERS = ((2, 1, 0), (0, 2, 1), (1, 0, 2))
SCATTER_ORDERS = ((0, 1, 2), (1, 2, 0), (2, 0, 1))
SHARES = ((0, 7), (7, 14), (14, 20))


class Place:
    def __init__(self):
        self.core = lax.axis_index("rep")
        me = lax.axis_index("dp")
        self.at = (me // RING**2, (me // RING) % RING, me % RING)
        self.on = {(a, step): (self.at[a] + (step + RING)) % RING for a in AXES for step in STEPS}

    def along(self, axis, step):
        return self.on[axis, step]

    def peer(self, axis, step):
        x, y, z = (self.along(a, step) if a == axis else self.at[a] for a in AXES)
        return {"dp": (x * RING + y) * RING + z}

    def other(self):
        return {"rep": 1 - self.core}


def enter(place, other):
    barrier = pltpu.get_barrier_semaphore()
    for axis in AXES:
        for step in STEPS:
            pl.semaphore_signal(barrier, inc=1, device_id=place.peer(axis, step), device_id_type=MESH)
    if other:
        pl.semaphore_signal(barrier, inc=1, device_id=place.other(), device_id_type=MESH)
    return lambda: pl.semaphore_wait(barrier, len(STEPS) * len(AXES) + other)


def remote(src, dst, send, recv, device):
    return pltpu.make_async_remote_copy(src_ref=src, dst_ref=dst, send_sem=send, recv_sem=recv, device_id=device, device_id_type=MESH)


def normed(h):
    wide = h.astype(F32)
    scale = lax.rsqrt(jnp.mean(wide**2, -1, keepdims=True) + 1e-6)
    return (wide * scale).astype(BF)


def dot(a, b, over_a=1, over_b=0):
    return lax.dot_general(a, b, (((over_a,), (over_b,)), ((), ())), preferred_element_type=F32)


def at_step(hooks, step):
    for number, hook in hooks.items():
        pl.when(step == number)(hook)


class Gather:
    def __init__(self, name, place, full, parts, send, recv):
        self.name, self.p, self.full, self.parts, self.send, self.recv = name, place, full, parts, send, recv

    STARTS = (0, 3, 5, 7, 10, 14, 16)
    CROSS = (9, 12, 13, 14, 15)

    def view(self, color, where):
        at = [where.get(a, self.p.at[a]) for a in AXES]
        return self.full.at[(*at, *self.parts[color])]

    def copy(self, color, slot):
        a, b, c = GATHER_ORDERS[color]
        p = self.p
        sems = self.send.at[color, slot], self.recv.at[color, slot]
        stage = sum(slot >= first for first in self.STARTS) - 1
        k = slot - self.STARTS[stage]
        if stage == 0:
            block = self.view(color, {})
            return remote(block, block, *sems, p.peer(a, STEPS[k]))
        axis, done, split = (b, {a: EVERY}, a) if stage < 3 else (c, {a: EVERY, b: EVERY}, b)
        side = k % 2
        step, half = STEPS[side], slice(2 * side, 2 * side + 2)
        where = dict(done)
        if stage in (2, 4):
            where[axis] = p.along(axis, -step)
            if slot not in self.CROSS:
                where[split] = half
        if stage == 5:
            where.update({axis: p.along(axis, 2), split: half})
        block = self.view(color, where)
        return remote(block, block, *sems, p.other() if slot in self.CROSS else p.peer(axis, step))

    def stage(self, number):
        last = len(self.STARTS) - 1
        for color in AXES:
            if number == last:
                wait = self.CROSS
            else:
                wait = [k for k in range(self.STARTS[number - 1], self.STARTS[number]) if k not in self.CROSS] if number else ()
            for slot in wait:
                self.copy(color, slot).wait_recv()
            for slot in range(self.STARTS[number], self.STARTS[number + 1]) if number < last else ():
                self.copy(color, slot).start()

    def finish(self):
        for color in AXES:
            for slot in range(self.STARTS[-1]):
                self.copy(color, slot).wait_send()


def gather_parts(core):
    pieces = []
    for widths in ((3, 3, 2), (2, 2, 2), (2, 2, 2)):
        pieces.append([])
        for width in widths:
            first = sum(sum(w for _, w in piece) for piece in pieces)
            pieces[-1].append((first, width))
    whole = [(lo, hi - lo) for lo, hi in SHARES]
    columns = [[(EVERY, slice(first * LANES, (first + w) * LANES)) for first, w in piece] for piece in (*pieces, whole)]
    half = part(core, D // 2)
    return columns, [(slice(*cut), EVERY, half) for cut in ((4, 5), (0, 2), (2, 4))]


def slots(*groups):
    def hook():
        for job, stage in groups:
            with jax.named_scope(f"{job.name}_{stage}"):
                job.stage(stage)

    return hook


def spread(jobs, table, sizes):
    plan = {}
    for n, (job, steps) in enumerate(zip(jobs, table, strict=True)):
        for stage, step in enumerate(steps):
            plan.setdefault(step, []).append((-stage, n, job))
    hooks, first = [], 0
    for size in sizes:
        steps = [step for step in sorted(plan) if first <= step < first + size]
        hooks.append({step - first: slots(*((job, -late) for late, _, job in sorted(plan[step], key=lambda t: t[:2]))) for step in steps})
        first += size
    return hooks


class Scatter:
    STARTS = (0, 2, 4, 6, 8, 11)

    def __init__(self, place, mine, put, number, bufs, send, recv, recv_c):
        self.name = f"rs{number}"
        self.p, self.mine, self.put, self.number, self.send, self.recv, self.recv_c = place, mine, put, number, send, recv, recv_c
        self.in_a, self.in_h, self.acc_b, self.send_b, self.in_b, self.in_bh, self.acc_c, self.send_c, self.in_c = bufs

    def term(self, color, where):
        at = dict(zip(SCATTER_ORDERS[color], where))
        return (*(at[axis] for axis in AXES), slice(*SHARES[color]))

    def copy(self, color, slot):
        a, b, c = SCATTER_ORDERS[color]
        p = self.p
        twin = self.number % 2
        stage = sum(slot >= first for first in self.STARTS) - 1
        k = slot - self.STARTS[stage]
        sems = self.send.at[twin, color, slot], self.recv.at[twin, color, slot] if stage < 4 else self.recv_c.at[self.number, color, k]
        step, half = STEPS[k], pl.ds(2 * k, 2)
        if stage == 0:
            src, dst, axis = self.mine.at[self.term(color, (p.along(a, 2), half, EVERY))], self.in_h[color].at[twin, k], a
        elif stage == 1:
            src, dst, axis = self.mine.at[self.term(color, (p.along(a, step), EVERY, EVERY))], self.in_a[color].at[twin, k], a
        elif stage == 2:
            src, dst, axis = self.send_b[color].at[p.along(b, 2), half], self.in_bh[color].at[k], b
        elif stage == 3:
            src, dst, axis = self.send_b[color].at[p.along(b, step)], self.in_b[color].at[k], b
        else:
            src, dst, axis = self.send_c[color].at[p.along(c, step)], self.in_c[color].at[self.number, k], c
        return remote(src, dst, *sems, p.peer(axis, step))

    def stage(self, number):
        last = len(self.STARTS) - 1
        for color, axes in enumerate(SCATTER_ORDERS):
            for slot in range(self.STARTS[number - 1], self.STARTS[number]) if number else ():
                self.copy(color, slot).wait_recv()
            self.sum(number, color, *axes)
            for slot in range(self.STARTS[number], self.STARTS[number + 1]) if number < last else ():
                self.copy(color, slot).start()
            done = {3: self.STARTS[:3:2], 4: self.STARTS[2:5:2], last: self.STARTS[4:]}.get(number)
            for slot in range(*done) if done else ():
                self.copy(color, slot).wait_send()

    def sum(self, number, color, a, b, c):
        p, mine, twin = self.p, self.mine, self.number % 2
        in_a, in_h, acc_b, send_b, in_b, in_bh = (
            t[color] for t in (self.in_a, self.in_h, self.acc_b, self.send_b, self.in_b, self.in_bh)
        )
        acc_c, send_c, in_c = (t[color] for t in (self.acc_c, self.send_c, self.in_c))
        flip = (lambda i, j: (i, j)) if b < c else (lambda i, j: (j, i))
        if number == 1:
            for slot, step in SIDES:

                @pl.loop(0, 2 * RING, unroll=2)
                def _(k):
                    i, j = k // RING, k % RING
                    at = self.term(color, (p.along(a, step), 2 * slot + i, j))
                    mine[at] = (mine[at].astype(F32) + in_h[(twin, slot, *flip(i, j))].astype(F32)).astype(BF)

        if number == 2:

            @pl.loop(0, RING**2, unroll=2)
            def _(k):
                i, j = k // RING, k % RING
                total = mine[self.term(color, (p.at[a], i, j))].astype(F32)
                for slot, _ in SIDES:
                    total = total + in_a[(twin, slot, *flip(i, j))].astype(F32)
                acc_b[i, j] = total
                send_b[i, j] = total.astype(BF)

        if number == 3:
            for slot, step in SIDES:
                i = p.along(b, step)

                @pl.loop(0, 2)
                def _(j):
                    send_b[i, 2 * slot + j] = (acc_b[i, 2 * slot + j] + in_bh[slot, j].astype(F32)).astype(BF)

        if number == 4:

            @pl.loop(0, RING)
            def _(j):
                total = acc_b[p.at[b], j]
                for slot, _ in SIDES:
                    total = total + in_b[slot, j].astype(F32)
                acc_c[j] = total
                send_c[j] = total.astype(BF)

        if number == 5:
            total = acc_c[p.at[c]]
            for slot in AXES:
                total = total + in_c[self.number, slot].astype(F32)
            lo, hi = SHARES[color]
            for k in range(lo, hi):
                self.put(k, total[k - lo])


def scatter_scratch(jobs):
    two, ring = (2,), (RING,)
    groups = []
    for (lo, hi), (a, b, c) in zip(SHARES, SCATTER_ORDERS):
        half = two + ring if b < c else ring + two
        shapes = (
            (two + two + ring + ring, BF), (two + two + half, BF), (ring + ring, F32), (ring + ring, BF), (two + ring, BF), (two + two, BF),
            (ring, F32), (ring, BF), ((jobs, len(STEPS)), BF),
        )
        groups.append([pltpu.VMEM((*shape, hi - lo, PAIR, LANES), kind) for shape, kind in shapes])
    return zip(*groups)


def put_gate_up(out):
    def put(k, unit):
        out[:, part(k, LANES)] = unit.astype(BF)

    return put


def put_half(outs, half):
    def put(k, unit):
        which, col = k // (UNITS // 2), k % (UNITS // 2) + half * (UNITS // 2)
        outs[which][:, part(col, LANES)] = unit.astype(BF)

    return put


def put_down(out):
    def put(k, unit):
        extra = k - D // LANES * 2
        if extra < 0:
            out[part(k % 2, PAIR), part(k // 2, LANES)] = unit.astype(BF)
        else:
            for n in BOTH:
                out[part(HIGH - 1, ROWS), part(2 * extra + n, LANES)] = unit[ROWS * n : ROWS * (n + 1)].astype(BF)

    return put


def part(k, size):
    return slice(k * size, (k + 1) * size) if isinstance(k, int) else pl.ds(pl.multiple_of(k * size, size), size)


def blocks(shape, places, **mode):
    return pl.BlockSpec(shape, lambda *at: tuple(at[places[k]] if k in places else 0 for k in range(len(shape))), **mode)


def silu_parts(gate):
    s = jax.nn.sigmoid(gate)
    silu = gate * s
    return silu, s + silu * (1 - s)


FORWARD_STEPS = (9, FF // MXU, 4, 1, 8)
GATHERS = (
    (0, 1, 2, 3, 5, 7, 8),
    (0, 1, 2, 5, 10, 12, 13),
    (0, 1, 2, 7, 12, 15, 16),
    (0, 4, 6, 11, 15, 18, 19),
    (0, 4, 6, 15, 20, 23, 24),
    (0, 4, 6, 13, 17, 22, 24),
)


def forward_kernel(
    g_ref, u_ref, d_ref, x_ref, dy_ref, gu_out, d_out, aT0, ways, act1, h1, aT1, act2, dgu2, gu_v, d_v, a_v, h_v, t_v, dy_v, sem, send, recv
):
    place = Place()
    core = place.core
    sems = [sem.at[k] for k in range(sem.shape[0])]

    def copy(src, dst):
        at = sems.pop()
        made = lambda: pltpu.make_async_copy(src, dst, at)
        return lambda: made().start(), lambda: made().wait()

    fetch_x, fetch_dy = copy(x_ref, h_v), copy(dy_ref, dy_v)
    puts = [copy(t_v, aT0), copy(t_v, aT1), copy(gu_v.at[0], gu_out.at[0]), copy(gu_v.at[1], gu_out.at[1]), copy(d_v.at[0], d_out)]
    put_t0, put_t1, *put_w = puts
    fetch_x[0]()
    columns, rows_of_down = gather_parts(core)
    half = rows_of_down[0][-1]
    for n in range(g_ref.shape[0]):
        gu_v[(n, core, *place.at)] = jnp.where(core == 0, g_ref[n], u_ref[n])
        d_v[(n, *place.at, EVERY, EVERY, half)] = d_ref[n, :, :, half]
    entered = enter(place, 1)
    fetch_dy[0]()
    plan = [(gu_v.at[0, core], piece) for piece in columns[:-1]]
    plan += [(d_v.at[0], rows_of_down), (gu_v.at[1, core], columns[-1]), (d_v.at[1], rows_of_down)]
    jobs = [Gather(f"ag{n}", place, *what, send.at[n], recv.at[n]) for n, what in enumerate(plan)]
    prelude, *hooks = spread(jobs, GATHERS, FORWARD_STEPS)
    with jax.named_scope("enter"):
        entered()

    def norm_rows(k):
        rows = part(k, MXU)
        a = normed(h_v[rows])
        a_v[rows] = a
        t_v[:, rows] = a.T

    for step in sorted(prelude):
        prelude[step]()
        if step == 0:
            fetch_x[1]()
        if step < 2:
            with jax.named_scope("norm"):
                pl.loop(RING * step, RING * (step + 1))(norm_rows)
    put_t0[0]()

    def gate_up_body(out_ways, out_act):
        step = pl.program_id(0)
        at_step(hooks[0], step)
        w = [gu_v[0, m, :, :, :, :, part(step, MXU)].reshape(D, MXU) for m in BOTH]
        tall = T // RING
        for k in range(RING):
            rows = part(k, tall)
            gate, up = (dot(a_v[rows], w[m]) for m in BOTH)
            silu, slope = silu_parts(gate)
            for m, val in enumerate((up * slope, silu)):
                out_ways[m, rows] = val
            out_act[rows] = (silu * up).astype(BF)

    with jax.named_scope("P1"):
        outs = [blocks((2, T, MXU), {2: 0}), blocks((T, MXU), {1: 0})]
        pltpu.emit_pipeline(gate_up_body, grid=(FF // MXU,), out_specs=outs)(ways, act1)
    put_t0[1]()

    wide = 512

    def down_body(act, out_h):
        step = pl.program_id(0)
        at_step(hooks[1], step)
        for k in range(wide // MXU):
            rows = part(k, MXU)
            there = part(step * (wide // MXU) + k, MXU)
            out = dot(act[rows], d_v[0].reshape(FF, D)).astype(BF)
            h = (h_v[there].astype(F32) + out.astype(F32)).astype(BF)
            out_h[rows] = h
            a = normed(h)
            a_v[there] = a
            t_v[:, there] = a.T

    with jax.named_scope("P2"):
        pltpu.emit_pipeline(
            down_body, grid=(T // wide,), in_specs=[blocks((wide, FF), {0: 0})], out_specs=[blocks((wide, D), {0: 0})]
        )(act1, h1)
    put_t1[0]()
    fetch_dy[1]()

    for step in sorted(hooks[2]):
        hooks[2][step]()

    for step, put in enumerate(put_w):
        hooks[3][step + 1] = put[0]

    def second_body(out_act, out_dgu):
        col, row = pl.program_id(0), pl.program_id(1)
        at_step(hooks[3], col * (T // wide) + row)
        rows = part(row, wide)
        a, dy = a_v[rows], dy_v[rows]
        wd = d_v[1, pl.ds(2 * col, 2)].reshape(FF // 2 // ROWS, ROWS, D)
        for k in range(FF // 2 // MXU):
            cols = part(k, MXU)
            there = part(col * (FF // 2 // MXU) + k, MXU)
            gate, up = (dot(a, gu_v[1, m, :, :, :, :, there].reshape(D, MXU)) for m in BOTH)
            by_act = dot(dy, wd[part(k, MXU // ROWS)].reshape(MXU, D), 1, 1).astype(BF).astype(F32)
            silu, slope = silu_parts(gate)
            out_act[:, cols] = (silu * up).astype(BF)
            for m, val in enumerate((by_act * up * slope, by_act * silu)):
                out_dgu[m, :, cols] = val.astype(BF)

    with jax.named_scope("P3"):
        outs = [blocks((wide, FF // 2), {0: 1, 1: 0}), blocks((2, wide, FF // 2), {1: 1, 2: 0})]
        pltpu.emit_pipeline(second_body, grid=(2, T // wide), out_specs=outs)(act2, dgu2)
    for put in (put_t1, *put_w):
        put[1]()
    for job in jobs:
        job.finish()


def shaped(*shape, kind=BF):
    return jax.ShapeDtypeStruct(shape, kind)


def calls(kernel, number, ins, outs, scratch):
    return pl.pallas_call(
        kernel,
        out_shape=tuple(shape for shape, _ in outs),
        in_specs=ins,
        out_specs=tuple(spec for _, spec in outs),
        scratch_shapes=scratch,
        compiler_params=pltpu.CompilerParams(collective_id=number, has_side_effects=True, vmem_limit_bytes=VMEM),
        name=kernel.__name__,
    )


def forward(wg, wu, wd, x, dy):
    layers, rows = wg.shape[:-1]
    outs = [
        shaped(layers, 2, *CUBE, rows, FF), shaped(*CUBE, HIGH, ROWS, D), shaped(D, T), shaped(2, T, FF, kind=F32), shaped(T, FF),
        shaped(T, D), shaped(D, T), shaped(T, FF), shaped(2, T, FF),
    ]
    scratch = [(layers, 2, *CUBE, rows, FF), (layers, *CUBE, HIGH, ROWS, D), (T, D), (T, D), (D, T), (T, D)]
    sems = [(7,), (6, 3, 16), (6, 3, 16)]
    scratch = [pltpu.VMEM(t, BF) for t in scratch] + [pltpu.SemaphoreType.DMA(t) for t in sems]
    call = calls(forward_kernel, 0, [VM] * 3 + [ANY] * 2, [(t, ANY) for t in outs], scratch)
    return call(wg, wu, wd.reshape(layers, HIGH, ROWS, D), x, dy)


def down_grad(act, by_out, mine, hooks):
    def body(act_cols):
        k = pl.program_id(0)
        at_step(hooks, k)
        val = dot(act_cols[...], by_out[...], 0, 0)
        tiles = D // LANES
        left = None
        for c in range(tiles):
            col = val[:, part(c, LANES)].reshape(RING**2, HIGH, ROWS, LANES)
            mine[k, :, :, 2 * c : 2 * c + 2] = col[:, : HIGH - 1].reshape(RING, RING, 2, PAIR, LANES).astype(BF)
            last = col[:, HIGH - 1 :]
            if c % 2:
                both = jnp.concatenate([left, last], 1).reshape(RING, RING, PAIR, LANES)
                mine[k, :, :, 2 * tiles + c // 2] = both.astype(BF)
            left = last

    pltpu.emit_pipeline(body, grid=(RING,), in_specs=[blocks((T, FF // RING), {1: 0})])(act)


def gate_up_grads(a_t, dgu, mine, hooks):
    wide = 512
    each = FF // wide

    def body(cols):
        k = pl.program_id(0)
        at_step(hooks, k)
        for n in range(wide // MXU):
            val = dot(a_t[...], cols[:, part(n, MXU)])
            for c in range(MXU // LANES):
                col = val[:, part(c, LANES)].reshape(*CUBE, PAIR, LANES).astype(BF)
                mine[1 + k // each, :, :, :, (k % each) * (wide // LANES) + n * (MXU // LANES) + c] = col

    pltpu.emit_pipeline(body, grid=(2 * each,), in_specs=[pl.BlockSpec((None, T, wide), lambda k: (k // each, 0, k % each))])(dgu)


def state_grad(dgu, w, h, by_out, held, out, keep, hooks):
    steps = T // MXU

    def project(d, k, n):
        cols = part(n, MXU)
        by_gate, by_up = (dot(d[m], w[m, cols], 1, 1).astype(BF).astype(F32) for m in BOTH)
        held[k % 2, :, cols] = (by_gate + by_up).astype(BF)

    def finish(h, outs, k, n):
        rows = part(n, MXU // RING)
        there = part(jnp.maximum(k - 1, 0) * RING + n, MXU // RING)
        by_a = held[(k + 1) % 2, rows].astype(F32)
        wide = h[rows].astype(F32)
        scale = lax.rsqrt(jnp.mean(wide**2, -1, keepdims=True) + 1e-6)
        inner = jnp.mean(by_a * wide, -1, keepdims=True)
        by_norm = (by_a * scale - wide * (inner * scale * scale * scale)).astype(BF)
        total = (by_out[there].astype(F32) + by_norm.astype(F32)).astype(BF)
        if keep is None:
            outs[0][rows] = total
        else:
            keep[there] = total

    def body(d, h, *outs):
        k = pl.program_id(0)
        at_step(hooks, k)

        @pl.when(k < steps)
        def _():
            for n in range(RING):
                finish(h, outs, k, n)
                project(d, k, n)

        @pl.when(k == steps)
        def _():
            for n in range(RING):
                finish(h, outs, k, n)

    behind = pl.BlockSpec((MXU, D), lambda k: (jnp.maximum(k - 1, 0), 0))
    now = lambda k: jnp.minimum(k, steps - 1)
    if len(dgu.shape) > 3:
        each = steps // 2
        source = pl.BlockSpec((2, None, MXU, FF), lambda k: (0, now(k) // each, now(k) % each, 0))
    else:
        source = pl.BlockSpec((2, MXU, FF), lambda k: (0, now(k), 0))
    pltpu.emit_pipeline(
        body,
        grid=(steps + 1,),
        in_specs=[source, behind],
        out_specs=[behind] if keep is None else [],
    )(dgu, h, *([out] if keep is None else []))


def layer_grads(ways, by_out, w, a_t, mine, held, out, sem, hooks, fetch):
    steps = FF // MXU
    pairs = steps // 2

    def held_at(k, m):
        return part(2 * (k % pairs) + m, MXU)

    def moves(k):
        for m in BOTH:
            for n in BOTH:
                yield pltpu.make_async_copy(held.at[n, :, held_at(k, m)], out.at[m, n, :, part(k, MXU)], sem.at[k % 2, m, n])

    def act(way, k, r):
        rows = part(r, T // RING)
        by_act = dot(by_out[rows], w[part(k, MXU)], 1, 1).astype(BF).astype(F32)
        for m in BOTH:
            held[r // 2, part(r % 2, T // RING), held_at(k, m)] = (by_act * way[m, rows]).astype(BF)

    def weights(k, r):
        m, h = r // 2, r % 2
        val = dot(a_t[part(h, D // 2)], held[:, :, held_at(k, m)].reshape(T, MXU))
        for c in range(MXU // LANES):
            unit = m * (UNITS // 2) + (k % pairs) * (MXU // LANES) + c
            mine[1 + k // pairs, 2 * h : 2 * h + 2, :, :, unit] = val[:, part(c, LANES)].reshape(2, RING, RING, PAIR, LANES).astype(BF)

    def body(way):
        k = pl.program_id(0)
        at_step(hooks, k)

        @pl.when(k >= 1)
        def _():
            for copy in moves(k - 1):
                copy.start()

        @pl.when(k >= 2)
        def _():
            for copy in moves(k - 2):
                copy.wait()

        @pl.when(k == 0)
        def _():
            for r in range(RING):
                act(way, k, r)

        @pl.when((k > 0) & (k < steps))
        def _():
            for r in range(RING):
                weights(k - 1, r)
                act(way, k, r)

        @pl.when(k == steps)
        def _():
            fetch()
            for r in range(RING):
                weights(k - 1, r)

    block = pl.BlockSpec((2, T, MXU), lambda k: (0, 0, jnp.minimum(k, steps - 1)))
    pltpu.emit_pipeline(body, grid=(steps + 1,), in_specs=[block])(ways)
    for copy in moves(steps - 1):
        copy.wait()


BACKWARD_STEPS = (4, 10, 9, 4, 11, 1, 9, 6)
SCATTERS = (
    (4, 8, 14, 16, 18, 24),
    (9, 16, 21, 24, 26, 29),
    (16, 24, 29, 30, 32, 35),
    (27, 30, 34, 36, 40, 43),
    (33, 35, 40, 42, 45, 48),
    (38, 42, 47, 49, 50, 51),
)


def backward_kernel(
    act2, dy, aT1, dgu2, gu_w, h1, act1, ways, d_w, aT0, x, dx, dgu1, d_out, g_out, u_out, dy_w_v, t_v, dh_v, w_v, held, mine, *more
):
    *bufs, sem, move_sem, send, recv, recv_c = more
    place = Place()
    sems = [sem.at[k] for k in range(sem.shape[0])]

    def load(src, dst):
        at = sems.pop()
        copy = lambda: pltpu.make_async_copy(src, dst, at)
        return lambda: copy().start(), lambda: copy().wait()

    dy_v = dy_w_v.at[:T]
    early, late = slice(0, FF - 2 * MXU), slice(FF - 2 * MXU, FF)
    loads = [(dy, dy_v), (aT1, t_v), (gu_w.at[1], w_v), (aT0, t_v), (d_w, dy_w_v)]
    loads += [(gu_w.at[0, :, :, cols], w_v.at[:, :, cols]) for cols in (early, late)]
    fetch_dy, fetch_t, fetch_w, fetch_t0, fetch_d, *fetch_w0 = (load(*pair) for pair in loads)
    fetch_dy[0]()
    entered = enter(place, 0)
    groups = [bufs[k : k + len(SHARES)] for k in range(0, len(bufs), len(SHARES))]
    jobs = []
    halves = [put_half((g_out.at[0], u_out.at[0]), half) for half in BOTH]
    for puts in ((put_down(d_out.at[1]), put_gate_up(g_out.at[1]), put_gate_up(u_out.at[1])), (put_down(d_out.at[0]), *halves)):
        for k, put in enumerate(puts):
            n = len(jobs)
            jobs.append(Scatter(place, mine.at[k], put, n, groups, send, recv, recv_c))
    hooks = spread(jobs, SCATTERS, BACKWARD_STEPS)
    for phase, step, fetch in ((0, 1, fetch_t), (1, 2, fetch_w), (2, 1, fetch_t0), (3, 0, fetch_d)):
        hooks[phase][step] = fetch[0]
    fetch_dy[1]()
    with jax.named_scope("P4"):
        down_grad(act2, dy_v, mine.at[0], hooks[0])
    entered()
    fetch_t[1]()
    with jax.named_scope("P5"):
        gate_up_grads(t_v, dgu2, mine, hooks[1])
    fetch_w[1]()
    with jax.named_scope("P6"):
        state_grad(dgu2, w_v, h1, dy_v, held, None, dh_v, hooks[2])
    with jax.named_scope("P7"):
        down_grad(act1, dh_v, mine.at[0], hooks[3])
    fetch_d[1]()
    fetch_t0[1]()
    with jax.named_scope("P8"):
        layer_grads(ways, dh_v, dy_w_v, t_v, mine, w_v, dgu1, move_sem, hooks[4], fetch_w0[0][0])
    fetch_w0[1][0]()
    hooks[5][0]()

    def arrived():
        for fetch in fetch_w0:
            fetch[1]()

    hooks[6][0] = arrived
    with jax.named_scope("P10"):
        state_grad(dgu1, w_v, x, dh_v, held, dx, None, hooks[6])
    with jax.named_scope("ending"):
        for step in sorted(hooks[7]):
            hooks[7][step]()


def backward(*args):
    n = 6
    sums = [shaped(2, HIGH * ROWS, D), shaped(2, PAIR, FF), shaped(2, PAIR, FF)]
    outs = [(shaped(T, D), ANY), (shaped(2, 2, T // 2, FF), ANY)] + [(t, VM) for t in sums]
    vmem = [(FF, D), (D, T), (T, D), (2, D, FF), (2, MXU, D), (len(sums), *CUBE, UNITS, PAIR, LANES)]
    scratch = [
        *(pltpu.VMEM(t, BF) for t in vmem),
        *(buf for group in scatter_scratch(n) for buf in group),
        pltpu.SemaphoreType.DMA((n + 1,)),
        pltpu.SemaphoreType.DMA((2, 2, 2)),
        pltpu.SemaphoreType.DMA((2, len(SHARES), Scatter.STARTS[-1])),
        pltpu.SemaphoreType.DMA((2, len(SHARES), Scatter.STARTS[4])),
        pltpu.SemaphoreType.DMA((n, len(SHARES), len(STEPS))),
    ]
    return calls(backward_kernel, 1, [ANY] * len(args), outs, scratch)(*args)


def solution(mesh):
    def step(x, dy, wg, wu, wd):
        x, dy = x[0], dy[0]
        gu, down, aT0, ways, act1, h1, aT1, act2, dgu2 = forward(wg, wu, wd, x, dy)
        gu, down = gu.reshape(-1, 2, D, FF), down.reshape(FF, D)
        dx, _, by_d, by_g, by_u = backward(act2, dy, aT1, dgu2, gu, h1, act1, ways, down, aT0, x)
        return dx[None], by_g, by_u, by_d

    seq, rows = P(("rep", "dp"), None, None), P(None, "dp", None)
    return jax.shard_map(
        step, mesh=mesh, in_specs=(seq, seq, rows, rows, rows), out_specs=(seq, *[P("rep", "dp", None)] * 3), check_vma=False
    )
```

```python
import jax
import jax.numpy as jnp
from jax import lax
from jax.experimental import pallas as pl
from jax.experimental.pallas import tpu as pltpu
from jax.sharding import PartitionSpec as P

MESH = pl.DeviceIdType.MESH
BF, F32 = jnp.bfloat16, jnp.float32
ANY = pl.BlockSpec(memory_space=pl.ANY)
VM = pl.BlockSpec(memory_space=pltpu.VMEM)
T, D, FF = 2048, 1024, 2560
RING, LANES, ROWS, MXU = 4, 128, 8, 256
PAIR = 2 * ROWS
CUBE = (RING,) * 3
UNITS = 20
HIGH = UNITS * PAIR * LANES // D // ROWS
AXES = range(3)
BOTH = range(2)
STEPS = (1, -1, 2)
SIDES = ((0, 1), (1, -1))
EVERY = slice(None)
VMEM = 67_043_328

GATHER_ORDERS = ((2, 1, 0), (0, 2, 1), (1, 0, 2))
SCATTER_ORDERS = ((0, 1, 2), (1, 2, 0), (2, 0, 1))
SHARES = ((0, 7), (7, 14), (14, 20))


class Place:
    def __init__(self):
        self.core = lax.axis_index("rep")
        me = lax.axis_index("dp")
        self.at = (me // RING**2, (me // RING) % RING, me % RING)
        self.on = {(a, step): (self.at[a] + (step + RING)) % RING for a in AXES for step in STEPS}

    def along(self, axis, step):
        return self.on[axis, step]

    def peer(self, axis, step):
        x, y, z = (self.along(a, step) if a == axis else self.at[a] for a in AXES)
        return {"dp": (x * RING + y) * RING + z}

    def other(self):
        return {"rep": 1 - self.core}


def enter(place, other):
    barrier = pltpu.get_barrier_semaphore()
    for axis in AXES:
        for step in STEPS:
            pl.semaphore_signal(barrier, inc=1, device_id=place.peer(axis, step), device_id_type=MESH)
    if other:
        pl.semaphore_signal(barrier, inc=1, device_id=place.other(), device_id_type=MESH)
    return lambda: pl.semaphore_wait(barrier, len(STEPS) * len(AXES) + other)


def remote(src, dst, send, recv, device):
    return pltpu.make_async_remote_copy(src_ref=src, dst_ref=dst, send_sem=send, recv_sem=recv, device_id=device, device_id_type=MESH)


def normed(h):
    wide = h.astype(F32)
    scale = lax.rsqrt(jnp.mean(wide**2, -1, keepdims=True) + 1e-6)
    return (wide * scale).astype(BF)


def dot(a, b, over_a=1, over_b=0):
    return lax.dot_general(a, b, (((over_a,), (over_b,)), ((), ())), preferred_element_type=F32)


def at_step(hooks, step):
    for number, hook in hooks.items():
        pl.when(step == number)(hook)


class Gather:
    def __init__(self, name, place, full, parts, send, recv):
        self.name, self.p, self.full, self.parts, self.send, self.recv = name, place, full, parts, send, recv

    STARTS = (0, 3, 5, 7, 10, 14, 16)
    CROSS = (9, 12, 13, 14, 15)

    def view(self, color, where):
        at = [where.get(a, self.p.at[a]) for a in AXES]
        return self.full.at[(*at, *self.parts[color])]

    def copy(self, color, slot):
        a, b, c = GATHER_ORDERS[color]
        p = self.p
        sems = self.send.at[color, slot], self.recv.at[color, slot]
        stage = sum(slot >= first for first in self.STARTS) - 1
        k = slot - self.STARTS[stage]
        if stage == 0:
            block = self.view(color, {})
            return remote(block, block, *sems, p.peer(a, STEPS[k]))
        axis, done, split = (b, {a: EVERY}, a) if stage < 3 else (c, {a: EVERY, b: EVERY}, b)
        side = k % 2
        step, half = STEPS[side], slice(2 * side, 2 * side + 2)
        where = dict(done)
        if stage in (2, 4):
            where[axis] = p.along(axis, -step)
            if slot not in self.CROSS:
                where[split] = half
        if stage == 5:
            where.update({axis: p.along(axis, 2), split: half})
        block = self.view(color, where)
        return remote(block, block, *sems, p.other() if slot in self.CROSS else p.peer(axis, step))

    def stage(self, number):
        last = len(self.STARTS) - 1
        for color in AXES:
            if number == last:
                wait = self.CROSS
            else:
                wait = [k for k in range(self.STARTS[number - 1], self.STARTS[number]) if k not in self.CROSS] if number else ()
            for slot in wait:
                self.copy(color, slot).wait_recv()
            for slot in range(self.STARTS[number], self.STARTS[number + 1]) if number < last else ():
                self.copy(color, slot).start()
            for slot in wait:
                self.copy(color, slot).wait_send()


def gather_parts(core):
    pieces = []
    for widths in ((3, 3, 2), (2, 2, 2), (2, 2, 2)):
        pieces.append([])
        for width in widths:
            first = sum(sum(w for _, w in piece) for piece in pieces)
            pieces[-1].append((first, width))
    whole = [(lo, hi - lo) for lo, hi in SHARES]
    columns = [[(EVERY, slice(first * LANES, (first + w) * LANES)) for first, w in piece] for piece in (*pieces, whole)]
    half = part(core, D // 2)
    return columns, [(slice(*cut), EVERY, half) for cut in ((4, 5), (0, 2), (2, 4))]


def slots(*groups):
    def hook():
        for job, stage in groups:
            with jax.named_scope(f"{job.name}_{stage}"):
                job.stage(stage)

    return hook


def spread(jobs, table, sizes):
    plan = {}
    for n, (job, steps) in enumerate(zip(jobs, table, strict=True)):
        for stage, step in enumerate(steps):
            plan.setdefault(step, []).append((-stage, n, job))
    hooks, first = [], 0
    for size in sizes:
        steps = [step for step in sorted(plan) if first <= step < first + size]
        hooks.append({step - first: slots(*((job, -late) for late, _, job in sorted(plan[step], key=lambda t: t[:2]))) for step in steps})
        first += size
    return hooks


class Scatter:
    STARTS = (0, 2, 4, 6, 8, 11)

    def __init__(self, place, mine, put, number, bufs, send, recv, recv_c):
        self.name = f"rs{number}"
        self.p, self.mine, self.put, self.number, self.send, self.recv, self.recv_c = place, mine, put, number, send, recv, recv_c
        self.in_a, self.in_h, self.acc_b, self.send_b, self.in_b, self.in_bh, self.acc_c, self.send_c, self.in_c = bufs

    def term(self, color, where):
        at = dict(zip(SCATTER_ORDERS[color], where))
        return (*(at[axis] for axis in AXES), slice(*SHARES[color]))

    def copy(self, color, slot):
        a, b, c = SCATTER_ORDERS[color]
        p = self.p
        twin = self.number % 2
        stage = sum(slot >= first for first in self.STARTS) - 1
        k = slot - self.STARTS[stage]
        sems = self.send.at[twin, color, slot], self.recv.at[twin, color, slot] if stage < 4 else self.recv_c.at[self.number, color, k]
        step, half = STEPS[k], pl.ds(2 * k, 2)
        if stage == 0:
            src, dst, axis = self.mine.at[self.term(color, (p.along(a, 2), half, EVERY))], self.in_h[color].at[twin, k], a
        elif stage == 1:
            src, dst, axis = self.mine.at[self.term(color, (p.along(a, step), EVERY, EVERY))], self.in_a[color].at[twin, k], a
        elif stage == 2:
            src, dst, axis = self.send_b[color].at[p.along(b, 2), half], self.in_bh[color].at[k], b
        elif stage == 3:
            src, dst, axis = self.send_b[color].at[p.along(b, step)], self.in_b[color].at[k], b
        else:
            src, dst, axis = self.send_c[color].at[p.along(c, step)], self.in_c[color].at[self.number, k], c
        return remote(src, dst, *sems, p.peer(axis, step))

    def stage(self, number):
        last = len(self.STARTS) - 1
        for color, axes in enumerate(SCATTER_ORDERS):
            for slot in range(self.STARTS[number - 1], self.STARTS[number]) if number else ():
                self.copy(color, slot).wait_recv()
            self.sum(number, color, *axes)
            for slot in range(self.STARTS[number], self.STARTS[number + 1]) if number < last else ():
                self.copy(color, slot).start()
            done = {3: self.STARTS[:3:2], 4: self.STARTS[2:5:2], last: self.STARTS[4:]}.get(number)
            for slot in range(*done) if done else ():
                self.copy(color, slot).wait_send()

    def sum(self, number, color, a, b, c):
        p, mine, twin = self.p, self.mine, self.number % 2
        in_a, in_h, acc_b, send_b, in_b, in_bh = (
            t[color] for t in (self.in_a, self.in_h, self.acc_b, self.send_b, self.in_b, self.in_bh)
        )
        acc_c, send_c, in_c = (t[color] for t in (self.acc_c, self.send_c, self.in_c))
        flip = (lambda i, j: (i, j)) if b < c else (lambda i, j: (j, i))
        if number == 1:
            for slot, step in SIDES:

                @pl.loop(0, 2 * RING, unroll=2)
                def _(k):
                    i, j = k // RING, k % RING
                    at = self.term(color, (p.along(a, step), 2 * slot + i, j))
                    mine[at] = (mine[at].astype(F32) + in_h[(twin, slot, *flip(i, j))].astype(F32)).astype(BF)

        if number == 2:

            @pl.loop(0, RING**2, unroll=2)
            def _(k):
                i, j = k // RING, k % RING
                total = mine[self.term(color, (p.at[a], i, j))].astype(F32)
                for slot, _ in SIDES:
                    total = total + in_a[(twin, slot, *flip(i, j))].astype(F32)
                acc_b[i, j] = total
                send_b[i, j] = total.astype(BF)

        if number == 3:
            for slot, step in SIDES:
                i = p.along(b, step)

                @pl.loop(0, 2)
                def _(j):
                    send_b[i, 2 * slot + j] = (acc_b[i, 2 * slot + j] + in_bh[slot, j].astype(F32)).astype(BF)

        if number == 4:

            @pl.loop(0, RING)
            def _(j):
                total = acc_b[p.at[b], j]
                for slot, _ in SIDES:
                    total = total + in_b[slot, j].astype(F32)
                acc_c[j] = total
                send_c[j] = total.astype(BF)

        if number == 5:
            total = acc_c[p.at[c]]
            for slot in AXES:
                total = total + in_c[self.number, slot].astype(F32)
            lo, hi = SHARES[color]
            for k in range(lo, hi):
                self.put(k, total[k - lo])


def scatter_scratch(jobs):
    two, ring = (2,), (RING,)
    groups = []
    for (lo, hi), (a, b, c) in zip(SHARES, SCATTER_ORDERS):
        half = two + ring if b < c else ring + two
        shapes = (
            (two + two + ring + ring, BF), (two + two + half, BF), (ring + ring, F32), (ring + ring, BF), (two + ring, BF), (two + two, BF),
            (ring, F32), (ring, BF), ((jobs, len(STEPS)), BF),
        )
        groups.append([pltpu.VMEM((*shape, hi - lo, PAIR, LANES), kind) for shape, kind in shapes])
    return zip(*groups)


def put_gate_up(out):
    def put(k, unit):
        out[:, part(k, LANES)] = unit.astype(BF)

    return put


def put_half(outs, half):
    def put(k, unit):
        which, col = k // (UNITS // 2), k % (UNITS // 2) + half * (UNITS // 2)
        outs[which][:, part(col, LANES)] = unit.astype(BF)

    return put


def put_down(out):
    def put(k, unit):
        extra = k - D // LANES * 2
        if extra < 0:
            out[part(k % 2, PAIR), part(k // 2, LANES)] = unit.astype(BF)
        else:
            for n in BOTH:
                out[part(HIGH - 1, ROWS), part(2 * extra + n, LANES)] = unit[ROWS * n : ROWS * (n + 1)].astype(BF)

    return put


def part(k, size):
    return slice(k * size, (k + 1) * size) if isinstance(k, int) else pl.ds(pl.multiple_of(k * size, size), size)


def blocks(shape, places, **mode):
    return pl.BlockSpec(shape, lambda *at: tuple(at[places[k]] if k in places else 0 for k in range(len(shape))), **mode)


def silu_parts(gate):
    s = jax.nn.sigmoid(gate)
    silu = gate * s
    return silu, s + silu * (1 - s)


FORWARD_STEPS = (9, FF // MXU, 4, 1, 8)
GATHERS = (
    (0, 1, 2, 3, 5, 7, 8),
    (0, 1, 2, 5, 10, 12, 13),
    (0, 1, 2, 7, 12, 15, 16),
    (0, 4, 6, 11, 15, 18, 19),
    (0, 4, 6, 15, 19, 22, 24),
    (0, 4, 6, 13, 17, 22, 24),
)


def forward_kernel(
    g_ref, u_ref, d_ref, x_ref, dy_ref, gu_out, d_out, aT0, ways, act1, h1, aT1, act2, dgu2, gu_v, d_v, a_v, h_v, t_v, dy_v, sem, send, recv
):
    place = Place()
    core = place.core
    sems = [sem.at[k] for k in range(sem.shape[0])]

    def copy(src, dst):
        at = sems.pop()
        made = lambda: pltpu.make_async_copy(src, dst, at)
        return lambda: made().start(), lambda: made().wait()

    fetch_x, fetch_dy = copy(x_ref, h_v), copy(dy_ref, dy_v)
    puts = [copy(t_v, aT0), copy(t_v, aT1), copy(gu_v.at[0], gu_out.at[0]), copy(gu_v.at[1], gu_out.at[1]), copy(d_v.at[0], d_out)]
    put_t0, put_t1, *put_w = puts
    fetch_x[0]()
    columns, rows_of_down = gather_parts(core)
    half = rows_of_down[0][-1]
    for n in range(g_ref.shape[0]):
        gu_v[(n, core, *place.at)] = jnp.where(core == 0, g_ref[n], u_ref[n])
        d_v[(n, *place.at, EVERY, EVERY, half)] = d_ref[n, :, :, half]
    entered = enter(place, 1)
    fetch_dy[0]()
    plan = [(gu_v.at[0, core], piece) for piece in columns[:-1]]
    plan += [(d_v.at[0], rows_of_down), (gu_v.at[1, core], columns[-1]), (d_v.at[1], rows_of_down)]
    jobs = [Gather(f"ag{n}", place, *what, send.at[n], recv.at[n]) for n, what in enumerate(plan)]
    prelude, *hooks = spread(jobs, GATHERS, FORWARD_STEPS)
    with jax.named_scope("enter"):
        entered()

    def norm_rows(k):
        rows = part(k, MXU)
        a = normed(h_v[rows])
        a_v[rows] = a
        t_v[:, rows] = a.T

    for step in sorted(prelude):
        prelude[step]()
        if step == 0:
            fetch_x[1]()
        if step < 2:
            with jax.named_scope("norm"):
                pl.loop(RING * step, RING * (step + 1))(norm_rows)
    put_t0[0]()

    def gate_up_body(out_ways, out_act):
        step = pl.program_id(0)
        at_step(hooks[0], step)
        w = [gu_v[0, m, :, :, :, :, part(step, MXU)].reshape(D, MXU) for m in BOTH]
        tall = T // RING
        for k in range(RING):
            rows = part(k, tall)
            gate, up = (dot(a_v[rows], w[m]) for m in BOTH)
            silu, slope = silu_parts(gate)
            for m, val in enumerate((up * slope, silu)):
                out_ways[m, rows] = val
            out_act[rows] = (silu * up).astype(BF)

    with jax.named_scope("P1"):
        outs = [blocks((2, T, MXU), {2: 0}), blocks((T, MXU), {1: 0})]
        pltpu.emit_pipeline(gate_up_body, grid=(FF // MXU,), out_specs=outs)(ways, act1)
    put_t0[1]()

    wide = 512

    def down_body(act, out_h):
        step = pl.program_id(0)
        at_step(hooks[1], step)
        for k in range(wide // MXU):
            rows = part(k, MXU)
            there = part(step * (wide // MXU) + k, MXU)
            out = dot(act[rows], d_v[0].reshape(FF, D)).astype(BF)
            h = (h_v[there].astype(F32) + out.astype(F32)).astype(BF)
            out_h[rows] = h
            a = normed(h)
            a_v[there] = a
            t_v[:, there] = a.T

    with jax.named_scope("P2"):
        pltpu.emit_pipeline(
            down_body, grid=(T // wide,), in_specs=[blocks((wide, FF), {0: 0})], out_specs=[blocks((wide, D), {0: 0})]
        )(act1, h1)
    put_t1[0]()
    fetch_dy[1]()

    for step in sorted(hooks[2]):
        hooks[2][step]()

    for step, put in enumerate(put_w):
        hooks[3][step + 1] = put[0]

    def second_body(out_act, out_dgu):
        col, row = pl.program_id(0), pl.program_id(1)
        at_step(hooks[3], col * (T // wide) + row)
        rows = part(row, wide)
        a, dy = a_v[rows], dy_v[rows]
        wd = d_v[1, pl.ds(2 * col, 2)].reshape(FF // 2 // ROWS, ROWS, D)
        for k in range(FF // 2 // MXU):
            cols = part(k, MXU)
            there = part(col * (FF // 2 // MXU) + k, MXU)
            gate, up = (dot(a, gu_v[1, m, :, :, :, :, there].reshape(D, MXU)) for m in BOTH)
            by_act = dot(dy, wd[part(k, MXU // ROWS)].reshape(MXU, D), 1, 1).astype(BF).astype(F32)
            silu, slope = silu_parts(gate)
            out_act[:, cols] = (silu * up).astype(BF)
            for m, val in enumerate((by_act * up * slope, by_act * silu)):
                out_dgu[m, :, cols] = val.astype(BF)

    with jax.named_scope("P3"):
        outs = [blocks((wide, FF // 2), {0: 1, 1: 0}), blocks((2, wide, FF // 2), {1: 1, 2: 0})]
        pltpu.emit_pipeline(second_body, grid=(2, T // wide), out_specs=outs)(act2, dgu2)
    for put in (put_t1, *put_w):
        put[1]()


def shaped(*shape, kind=BF):
    return jax.ShapeDtypeStruct(shape, kind)


def calls(kernel, number, ins, outs, scratch):
    return pl.pallas_call(
        kernel,
        out_shape=tuple(shape for shape, _ in outs),
        in_specs=ins,
        out_specs=tuple(spec for _, spec in outs),
        scratch_shapes=scratch,
        compiler_params=pltpu.CompilerParams(collective_id=number, has_side_effects=True, vmem_limit_bytes=VMEM),
        name=kernel.__name__,
    )


def forward(wg, wu, wd, x, dy):
    layers, rows = wg.shape[:-1]
    outs = [
        shaped(layers, 2, *CUBE, rows, FF), shaped(*CUBE, HIGH, ROWS, D), shaped(D, T), shaped(2, T, FF, kind=F32), shaped(T, FF),
        shaped(T, D), shaped(D, T), shaped(T, FF), shaped(2, T, FF),
    ]
    scratch = [(layers, 2, *CUBE, rows, FF), (layers, *CUBE, HIGH, ROWS, D), (T, D), (T, D), (D, T), (T, D)]
    sems = [(7,), (6, 3, 16), (6, 3, 16)]
    scratch = [pltpu.VMEM(t, BF) for t in scratch] + [pltpu.SemaphoreType.DMA(t) for t in sems]
    call = calls(forward_kernel, 0, [VM] * 3 + [ANY] * 2, [(t, ANY) for t in outs], scratch)
    return call(wg, wu, wd.reshape(layers, HIGH, ROWS, D), x, dy)


def down_grad(act, by_out, mine, hooks):
    def body(act_cols):
        k = pl.program_id(0)
        at_step(hooks, k)
        val = dot(act_cols[...], by_out[...], 0, 0)
        tiles = D // LANES
        left = None
        for c in range(tiles):
            col = val[:, part(c, LANES)].reshape(RING**2, HIGH, ROWS, LANES)
            mine[k, :, :, 2 * c : 2 * c + 2] = col[:, : HIGH - 1].reshape(RING, RING, 2, PAIR, LANES).astype(BF)
            last = col[:, HIGH - 1 :]
            if c % 2:
                both = jnp.concatenate([left, last], 1).reshape(RING, RING, PAIR, LANES)
                mine[k, :, :, 2 * tiles + c // 2] = both.astype(BF)
            left = last

    pltpu.emit_pipeline(body, grid=(RING,), in_specs=[blocks((T, FF // RING), {1: 0})])(act)


def gate_up_grads(a_t, dgu, mine, hooks):
    wide = 512
    each = FF // wide

    def body(cols):
        k = pl.program_id(0)
        at_step(hooks, k)
        for n in range(wide // MXU):
            val = dot(a_t[...], cols[:, part(n, MXU)])
            for c in range(MXU // LANES):
                col = val[:, part(c, LANES)].reshape(*CUBE, PAIR, LANES).astype(BF)
                mine[1 + k // each, :, :, :, (k % each) * (wide // LANES) + n * (MXU // LANES) + c] = col

    pltpu.emit_pipeline(body, grid=(2 * each,), in_specs=[pl.BlockSpec((None, T, wide), lambda k: (k // each, 0, k % each))])(dgu)


def state_grad(dgu, w, h, by_out, held, out, keep, hooks):
    steps = T // MXU

    def project(d, k, n):
        cols = part(n, MXU)
        by_gate, by_up = (dot(d[m], w[m, cols], 1, 1).astype(BF).astype(F32) for m in BOTH)
        held[part(k % 2, MXU), cols] = (by_gate + by_up).astype(BF)

    def finish(h, outs, k, n):
        rows = part(n, MXU // RING)
        there = part(jnp.maximum(k - 1, 0) * RING + n, MXU // RING)
        by_a = held[part((k + 1) % 2 * RING + n, MXU // RING), :D].astype(F32)
        wide = h[rows].astype(F32)
        scale = lax.rsqrt(jnp.mean(wide**2, -1, keepdims=True) + 1e-6)
        inner = jnp.mean(by_a * wide, -1, keepdims=True)
        by_norm = (by_a * scale - wide * (inner * scale * scale * scale)).astype(BF)
        total = (by_out[there].astype(F32) + by_norm.astype(F32)).astype(BF)
        if keep is None:
            outs[0][rows] = total
        else:
            keep[there] = total

    def body(d, h, *outs):
        k = pl.program_id(0)
        at_step(hooks, k)

        @pl.when(k < steps)
        def _():
            for n in range(RING):
                finish(h, outs, k, n)
                project(d, k, n)

        @pl.when(k == steps)
        def _():
            for n in range(RING):
                finish(h, outs, k, n)

    behind = pl.BlockSpec((MXU, D), lambda k: (jnp.maximum(k - 1, 0), 0))
    now = lambda k: jnp.minimum(k, steps - 1)
    if len(dgu.shape) > 3:
        each = steps // 2
        source = pl.BlockSpec((2, None, MXU, FF), lambda k: (0, now(k) // each, now(k) % each, 0))
    else:
        source = pl.BlockSpec((2, MXU, FF), lambda k: (0, now(k), 0))
    pltpu.emit_pipeline(
        body,
        grid=(steps + 1,),
        in_specs=[source, behind],
        out_specs=[behind] if keep is None else [],
    )(dgu, h, *([out] if keep is None else []))


def layer_grads(ways, by_out, w, a_t, mine, held, out, sem, hooks, fetch):
    steps = FF // MXU
    pairs = steps // 2

    def held_at(k, m):
        return part(2 * (k % pairs) + m, MXU)

    def moves(k):
        for m in BOTH:
            for n in BOTH:
                yield pltpu.make_async_copy(held.at[n, :, held_at(k, m)], out.at[m, n, :, part(k, MXU)], sem.at[k % 2, m, n])

    tall = T // 2

    def act(way, k, r):
        rows = part(r, tall)
        by_act = dot(by_out[rows], w[part(k, MXU)], 1, 1).astype(BF).astype(F32)
        for m in BOTH:
            held[r, :, held_at(k, m)] = (by_act * way[m, rows]).astype(BF)

    def weights(k, m):
        val = dot(a_t[...], held[:, :, held_at(k, m)].reshape(T, MXU))
        for c in range(MXU // LANES):
            unit = m * (UNITS // 2) + (k % pairs) * (MXU // LANES) + c
            mine[1 + k // pairs, :, :, :, unit] = val[:, part(c, LANES)].reshape(*CUBE, PAIR, LANES).astype(BF)

    def body(way):
        k = pl.program_id(0)
        at_step(hooks, k)

        @pl.when(k >= 1)
        def _():
            for copy in moves(k - 1):
                copy.start()

        @pl.when(k >= 2)
        def _():
            for copy in moves(k - 2):
                copy.wait()

        @pl.when(k == 0)
        def _():
            for r in BOTH:
                act(way, k, r)

        @pl.when((k > 0) & (k < steps))
        def _():
            for r in BOTH:
                weights(k - 1, r)
                act(way, k, r)

        @pl.when(k == steps)
        def _():
            fetch()
            for r in BOTH:
                weights(k - 1, r)

    block = pl.BlockSpec((2, T, MXU), lambda k: (0, 0, jnp.minimum(k, steps - 1)))
    pltpu.emit_pipeline(body, grid=(steps + 1,), in_specs=[block])(ways)
    for copy in moves(steps - 1):
        copy.wait()


BACKWARD_STEPS = (4, 10, 9, 4, 11, 1, 9, 6)
SCATTERS = (
    (4, 8, 14, 16, 18, 24),
    (9, 16, 21, 24, 26, 29),
    (16, 24, 29, 30, 32, 35),
    (27, 30, 34, 36, 40, 43),
    (33, 35, 40, 42, 46, 48),
    (38, 41, 46, 49, 50, 51),
)


def backward_kernel(
    act2, dy, aT1, dgu2, gu_w, h1, act1, ways, d_w, aT0, x, dx, dgu1, d_out, g_out, u_out, dy_w_v, t_v, dh_v, w_v, mine, *more
):
    *bufs, sem, move_sem, send, recv, recv_c = more
    place = Place()
    sems = [sem.at[k] for k in range(sem.shape[0])]

    def load(src, dst):
        at = sems.pop()
        copy = lambda: pltpu.make_async_copy(src, dst, at)
        return lambda: copy().start(), lambda: copy().wait()

    dy_v = dy_w_v.at[:T]
    early, late = slice(0, FF - 2 * MXU), slice(FF - 2 * MXU, FF)
    loads = [(dy, dy_v), (aT1, t_v), (gu_w.at[1], w_v), (aT0, t_v), (d_w, dy_w_v)]
    loads += [(gu_w.at[0, :, :, cols], w_v.at[:, :, cols]) for cols in (early, late)]
    fetch_dy, fetch_t, fetch_w, fetch_t0, fetch_d, *fetch_w0 = (load(*pair) for pair in loads)
    fetch_dy[0]()
    entered = enter(place, 0)
    groups = [bufs[k : k + len(SHARES)] for k in range(0, len(bufs), len(SHARES))]
    jobs = []
    halves = [put_half((g_out.at[0], u_out.at[0]), half) for half in BOTH]
    for puts in ((put_down(d_out.at[1]), put_gate_up(g_out.at[1]), put_gate_up(u_out.at[1])), (put_down(d_out.at[0]), *halves)):
        for k, put in enumerate(puts):
            n = len(jobs)
            jobs.append(Scatter(place, mine.at[k], put, n, groups, send, recv, recv_c))
    hooks = spread(jobs, SCATTERS, BACKWARD_STEPS)
    for phase, step, fetch in ((0, 1, fetch_t), (1, 2, fetch_w), (3, 2, fetch_t0), (3, 0, fetch_d)):
        hooks[phase][step] = fetch[0]
    fetch_dy[1]()
    with jax.named_scope("P4"):
        down_grad(act2, dy_v, mine.at[0], hooks[0])
    entered()
    fetch_t[1]()
    with jax.named_scope("P5"):
        gate_up_grads(t_v, dgu2, mine, hooks[1])
    fetch_w[1]()
    with jax.named_scope("P6"):
        state_grad(dgu2, w_v, h1, dy_v, t_v, None, dh_v, hooks[2])
    with jax.named_scope("P7"):
        down_grad(act1, dh_v, mine.at[0], hooks[3])
    fetch_d[1]()
    fetch_t0[1]()
    with jax.named_scope("P8"):
        layer_grads(ways, dh_v, dy_w_v, t_v, mine, w_v, dgu1, move_sem, hooks[4], fetch_w0[0][0])
    fetch_w0[1][0]()
    hooks[5][0]()

    def arrived():
        for fetch in fetch_w0:
            fetch[1]()

    hooks[6][0] = arrived
    with jax.named_scope("P10"):
        state_grad(dgu1, w_v, x, dh_v, t_v, dx, None, hooks[6])
    with jax.named_scope("ending"):
        for step in sorted(hooks[7]):
            hooks[7][step]()


def backward(*args):
    n = 6
    sums = [shaped(2, HIGH * ROWS, D), shaped(2, PAIR, FF), shaped(2, PAIR, FF)]
    outs = [(shaped(T, D), ANY), (shaped(2, 2, T // 2, FF), ANY)] + [(t, VM) for t in sums]
    vmem = [(FF, D), (D, T), (T, D), (2, D, FF), (len(sums), *CUBE, UNITS, PAIR, LANES)]
    scratch = [
        *(pltpu.VMEM(t, BF) for t in vmem),
        *(buf for group in scatter_scratch(n) for buf in group),
        pltpu.SemaphoreType.DMA((n + 1,)),
        pltpu.SemaphoreType.DMA((2, 2, 2)),
        pltpu.SemaphoreType.DMA((2, len(SHARES), Scatter.STARTS[-1])),
        pltpu.SemaphoreType.DMA((2, len(SHARES), Scatter.STARTS[4])),
        pltpu.SemaphoreType.DMA((n, len(SHARES), len(STEPS))),
    ]
    return calls(backward_kernel, 1, [ANY] * len(args), outs, scratch)(*args)


def solution(mesh):
    def step(x, dy, wg, wu, wd):
        x, dy = x[0], dy[0]
        gu, down, aT0, ways, act1, h1, aT1, act2, dgu2 = forward(wg, wu, wd, x, dy)
        gu, down = gu.reshape(-1, 2, D, FF), down.reshape(FF, D)
        dx, _, by_d, by_g, by_u = backward(act2, dy, aT1, dgu2, gu, h1, act1, ways, down, aT0, x)
        return dx[None], by_g, by_u, by_d

    seq, rows = P(("rep", "dp"), None, None), P(None, "dp", None)
    return jax.shard_map(
        step, mesh=mesh, in_specs=(seq, seq, rows, rows, rows), out_specs=(seq, *[P("rep", "dp", None)] * 3), check_vma=False
    )
```

```python
import jax
import jax.numpy as jnp
from jax import lax
from jax.experimental import pallas as pl
from jax.experimental.pallas import tpu as pltpu
from jax.sharding import PartitionSpec as P

MESH = pl.DeviceIdType.MESH
BF, F32 = jnp.bfloat16, jnp.float32
ANY = pl.BlockSpec(memory_space=pl.ANY)
VM = pl.BlockSpec(memory_space=pltpu.VMEM)
T, D, FF = 2048, 1024, 2560
RING, LANES, ROWS, MXU = 4, 128, 8, 256
PAIR = 2 * ROWS
CUBE = (RING,) * 3
UNITS = 20
HIGH = UNITS * PAIR * LANES // D // ROWS
AXES = range(3)
BOTH = range(2)
STEPS = (1, -1, 2)
SIDES = ((0, 1), (1, -1))
EVERY = slice(None)
VMEM = 67_043_328

GATHER_ORDERS = ((2, 1, 0), (0, 2, 1), (1, 0, 2))
SCATTER_ORDERS = ((0, 1, 2), (1, 2, 0), (2, 0, 1))
SHARES = ((0, 7), (7, 14), (14, 20))


class Place:
    def __init__(self):
        self.core = lax.axis_index("rep")
        me = lax.axis_index("dp")
        self.at = (me // RING**2, (me // RING) % RING, me % RING)
        self.on = {(a, step): (self.at[a] + (step + RING)) % RING for a in AXES for step in STEPS}

    def along(self, axis, step):
        return self.on[axis, step]

    def peer(self, axis, step):
        x, y, z = (self.along(a, step) if a == axis else self.at[a] for a in AXES)
        return {"dp": (x * RING + y) * RING + z}

    def other(self):
        return {"rep": 1 - self.core}


def enter(place, other):
    barrier = pltpu.get_barrier_semaphore()
    for axis in AXES:
        for step in STEPS:
            pl.semaphore_signal(barrier, inc=1, device_id=place.peer(axis, step), device_id_type=MESH)
    if other:
        pl.semaphore_signal(barrier, inc=1, device_id=place.other(), device_id_type=MESH)
    return lambda: pl.semaphore_wait(barrier, len(STEPS) * len(AXES) + other)


def remote(src, dst, send, recv, device):
    return pltpu.make_async_remote_copy(src_ref=src, dst_ref=dst, send_sem=send, recv_sem=recv, device_id=device, device_id_type=MESH)


def row_mean(x):
    return jnp.mean(x, -1, keepdims=True)


def norm_scale(wide):
    return lax.rsqrt(row_mean(wide * wide) + 1e-6)


def normed(h):
    wide = h.astype(F32)
    return (wide * norm_scale(wide)).astype(BF)


def dot(a, b, over_a=1, over_b=0):
    return lax.dot_general(a, b, (((over_a,), (over_b,)), ((), ())), preferred_element_type=F32)


def at_step(hooks, step):
    for number, hook in hooks.items():
        pl.when(step == number)(hook)


class Gather:
    def __init__(self, name, place, full, parts, send, recv):
        self.name, self.p, self.full, self.parts, self.send, self.recv = name, place, full, parts, send, recv

    STARTS = (0, 3, 5, 7, 10, 14, 16)
    CROSS = (9, 12, 13, 14, 15)

    def view(self, color, where):
        at = [where.get(a, self.p.at[a]) for a in AXES]
        return self.full.at[(*at, *self.parts[color])]

    def copy(self, color, slot):
        a, b, c = GATHER_ORDERS[color]
        p = self.p
        sems = self.send.at[color, slot], self.recv.at[color, slot]
        stage = sum(slot >= first for first in self.STARTS) - 1
        k = slot - self.STARTS[stage]
        if stage == 0:
            block = self.view(color, {})
            return remote(block, block, *sems, p.peer(a, STEPS[k]))
        axis, done, split = (b, {a: EVERY}, a) if stage < 3 else (c, {a: EVERY, b: EVERY}, b)
        side = k % 2
        step, half = STEPS[side], slice(2 * side, 2 * side + 2)
        where = dict(done)
        if stage in (2, 4):
            where[axis] = p.along(axis, -step)
            if slot not in self.CROSS:
                where[split] = half
        if stage == 5:
            where.update({axis: p.along(axis, 2), split: half})
        block = self.view(color, where)
        return remote(block, block, *sems, p.other() if slot in self.CROSS else p.peer(axis, step))

    def stage(self, number):
        last = len(self.STARTS) - 1
        for color in AXES:
            if number == last:
                wait = self.CROSS
            else:
                wait = [k for k in range(self.STARTS[number - 1], self.STARTS[number]) if k not in self.CROSS] if number else ()
            for slot in wait:
                self.copy(color, slot).wait_recv()
            for slot in range(self.STARTS[number], self.STARTS[number + 1]) if number < last else ():
                self.copy(color, slot).start()
            for slot in wait if number < last else ():
                self.copy(color, slot).wait_send()

    def finish(self):
        for color in AXES:
            for slot in self.CROSS:
                self.copy(color, slot).wait_send()


def gather_parts(core):
    columns = []
    for layer in (((3, 3, 2), (2, 2, 2), (2, 2, 2)), ((4, 3, 3), (3, 4, 3))):
        first = 0
        columns.append([])
        for widths in layer:
            columns[-1].append([])
            for width in widths:
                columns[-1][-1].append((EVERY, slice(first * LANES, (first + width) * LANES)))
                first += width
    half = part(core, D // 2)
    return columns, [(slice(*cut), EVERY, half) for cut in ((4, 5), (0, 2), (2, 4))]


def slots(*groups):
    def hook():
        for job, stage in groups:
            with jax.named_scope(f"{job.name}_{stage}"):
                job.stage(stage)

    return hook


def spread(jobs, table, sizes):
    plan = {}
    for n, (job, steps) in enumerate(zip(jobs, table, strict=True)):
        for stage, step in enumerate(steps):
            plan.setdefault(step, []).append((-stage, n, job))
    hooks, first = [], 0
    for size in sizes:
        steps = [step for step in sorted(plan) if first <= step < first + size]
        hooks.append({step - first: slots(*((job, -late) for late, _, job in sorted(plan[step], key=lambda t: t[:2]))) for step in steps})
        first += size
    return hooks


class Scatter:
    STARTS = (0, 2, 4, 6, 8, 11)

    def __init__(self, place, mine, put, number, bufs, send, recv, recv_c):
        self.name = f"rs{number}"
        self.p, self.mine, self.put, self.number, self.send, self.recv, self.recv_c = place, mine, put, number, send, recv, recv_c
        self.in_a, self.in_h, self.acc_b, self.send_b, self.in_b, self.in_bh, self.acc_c, self.send_c, self.in_c = bufs

    def term(self, color, where):
        at = dict(zip(SCATTER_ORDERS[color], where))
        return (*(at[axis] for axis in AXES), slice(*SHARES[color]))

    def copy(self, color, slot):
        a, b, c = SCATTER_ORDERS[color]
        p = self.p
        twin = self.number % 2
        stage = sum(slot >= first for first in self.STARTS) - 1
        k = slot - self.STARTS[stage]
        sems = self.send.at[twin, color, slot], self.recv.at[twin, color, slot] if stage < 4 else self.recv_c.at[self.number, color, k]
        step, half = STEPS[k], pl.ds(2 * k, 2)
        if stage == 0:
            src, dst, axis = self.mine.at[self.term(color, (p.along(a, 2), half, EVERY))], self.in_h[color].at[twin, k], a
        elif stage == 1:
            src, dst, axis = self.mine.at[self.term(color, (p.along(a, step), EVERY, EVERY))], self.in_a[color].at[twin, k], a
        elif stage == 2:
            src, dst, axis = self.send_b[color].at[p.along(b, 2), half], self.in_bh[color].at[k], b
        elif stage == 3:
            src, dst, axis = self.send_b[color].at[p.along(b, step)], self.in_b[color].at[k], b
        else:
            src, dst, axis = self.send_c[color].at[p.along(c, step)], self.in_c[color].at[self.number, k], c
        return remote(src, dst, *sems, p.peer(axis, step))

    def stage(self, number):
        last = len(self.STARTS) - 1
        for color, axes in enumerate(SCATTER_ORDERS):
            for slot in range(self.STARTS[number - 1], self.STARTS[number]) if number else ():
                self.copy(color, slot).wait_recv()
            self.sum(number, color, *axes)
            for slot in range(self.STARTS[number], self.STARTS[number + 1]) if number < last else ():
                self.copy(color, slot).start()
            done = {3: self.STARTS[:3:2], 4: self.STARTS[2:5:2], last: self.STARTS[4:]}.get(number)
            for slot in range(*done) if done else ():
                self.copy(color, slot).wait_send()

    def sum(self, number, color, a, b, c):
        p, mine, twin = self.p, self.mine, self.number % 2
        in_a, in_h, acc_b, send_b, in_b, in_bh = (
            t[color] for t in (self.in_a, self.in_h, self.acc_b, self.send_b, self.in_b, self.in_bh)
        )
        acc_c, send_c, in_c = (t[color] for t in (self.acc_c, self.send_c, self.in_c))
        flip = (lambda i, j: (i, j)) if b < c else (lambda i, j: (j, i))
        if number == 1:
            for slot, step in SIDES:

                @pl.loop(0, 2 * RING, unroll=2)
                def _(k):
                    i, j = k // RING, k % RING
                    at = self.term(color, (p.along(a, step), 2 * slot + i, j))
                    mine[at] = (mine[at].astype(F32) + in_h[(twin, slot, *flip(i, j))].astype(F32)).astype(BF)

        if number == 2:

            @pl.loop(0, RING**2, unroll=2)
            def _(k):
                i, j = k // RING, k % RING
                total = mine[self.term(color, (p.at[a], i, j))].astype(F32)
                for slot, _ in SIDES:
                    total = total + in_a[(twin, slot, *flip(i, j))].astype(F32)
                acc_b[i, j] = total
                send_b[i, j] = total.astype(BF)

        if number == 3:
            for slot, step in SIDES:
                i = p.along(b, step)

                @pl.loop(0, 2)
                def _(j):
                    send_b[i, 2 * slot + j] = (acc_b[i, 2 * slot + j] + in_bh[slot, j].astype(F32)).astype(BF)

        if number == 4:

            @pl.loop(0, RING)
            def _(j):
                total = acc_b[p.at[b], j]
                for slot, _ in SIDES:
                    total = total + in_b[slot, j].astype(F32)
                acc_c[j] = total
                send_c[j] = total.astype(BF)

        if number == 5:
            total = acc_c[p.at[c]]
            for slot in AXES:
                total = total + in_c[self.number, slot].astype(F32)
            lo, hi = SHARES[color]
            for k in range(lo, hi):
                self.put(k, total[k - lo])


def scatter_scratch(jobs):
    two, ring = (2,), (RING,)
    groups = []
    for (lo, hi), (a, b, c) in zip(SHARES, SCATTER_ORDERS):
        half = two + ring if b < c else ring + two
        shapes = (
            (two + two + ring + ring, BF), (two + two + half, BF), (ring + ring, F32), (ring + ring, BF), (two + ring, BF), (two + two, BF),
            (ring, F32), (ring, BF), ((jobs, len(STEPS)), BF),
        )
        groups.append([pltpu.VMEM((*shape, hi - lo, PAIR, LANES), kind) for shape, kind in shapes])
    return zip(*groups)


def put_gate_up(out):
    def put(k, unit):
        out[:, part(k, LANES)] = unit.astype(BF)

    return put


def put_half(outs, half):
    def put(k, unit):
        which, col = k // (UNITS // 2), k % (UNITS // 2) + half * (UNITS // 2)
        outs[which][:, part(col, LANES)] = unit.astype(BF)

    return put


def put_down(out):
    def put(k, unit):
        extra = k - D // LANES * 2
        if extra < 0:
            out[part(k % 2, PAIR), part(k // 2, LANES)] = unit.astype(BF)
        else:
            for n in BOTH:
                out[part(HIGH - 1, ROWS), part(2 * extra + n, LANES)] = unit[ROWS * n : ROWS * (n + 1)].astype(BF)

    return put


def part(k, size):
    return slice(k * size, (k + 1) * size) if isinstance(k, int) else pl.ds(pl.multiple_of(k * size, size), size)


def blocks(shape, places, **mode):
    return pl.BlockSpec(shape, lambda *at: tuple(at[places[k]] if k in places else 0 for k in range(len(shape))), **mode)


def silu_parts(gate):
    s = jax.nn.sigmoid(gate)
    silu = gate * s
    return silu, s + silu * (1 - s)


FORWARD_STEPS = (9, FF // MXU, 4, 8)
GATHERS = (
    (0, 1, 2, 3, 5, 7, 8),
    (0, 1, 2, 5, 10, 12, 13),
    (0, 1, 2, 7, 12, 15, 16),
    (0, 4, 6, 11, 15, 18, 19),
    (0, 4, 6, 15, 19, 21, 23),
    (0, 4, 6, 13, 17, 20, 23),
    (0, 4, 6, 18, 21, 23, 25),
)


def forward_kernel(
    g_ref, u_ref, d_ref, x_ref, dy_ref, gu_out, d_out, aT0, ways, act1, h1, aT1, act2, dgu2, gu_v, d_v, a_v, h_v, t_v, dy_v, sem, send, recv
):
    place = Place()
    core = place.core
    sems = [sem.at[k] for k in range(sem.shape[0])]

    def copy(src, dst):
        at = sems.pop()
        made = lambda: pltpu.make_async_copy(src, dst, at)
        return lambda: made().start(), lambda: made().wait()

    fetch_x, fetch_dy = copy(x_ref, h_v), copy(dy_ref, dy_v)
    puts = [copy(t_v, aT0), copy(t_v, aT1), copy(gu_v.at[0], gu_out.at[0]), copy(gu_v.at[1], gu_out.at[1]), copy(d_v.at[0], d_out)]
    put_t0, put_t1, *put_w = puts
    fetch_x[0]()
    columns, rows_of_down = gather_parts(core)
    half = rows_of_down[0][-1]
    for n in range(g_ref.shape[0]):
        gu_v[(n, core, *place.at)] = jnp.where(core == 0, g_ref[n], u_ref[n])
        d_v[(n, *place.at, EVERY, EVERY, half)] = d_ref[n, :, :, half]
    entered = enter(place, 1)
    fetch_dy[0]()
    plan = [(gu_v.at[0, core], piece) for piece in columns[0]]
    early, late = columns[1]
    plan += [(d_v.at[0], rows_of_down), (gu_v.at[1, core], early), (d_v.at[1], rows_of_down), (gu_v.at[1, core], late)]
    jobs = [Gather(f"ag{n}", place, *what, send.at[n], recv.at[n]) for n, what in enumerate(plan)]
    prelude, *hooks = spread(jobs, GATHERS, FORWARD_STEPS)
    with jax.named_scope("enter"):
        entered()

    def norm_rows(k):
        rows = part(k, MXU)
        a = normed(h_v[rows])
        a_v[rows] = a
        t_v[:, rows] = a.T

    for step in sorted(prelude):
        prelude[step]()
        if step == 0:
            fetch_x[1]()
        if step < 2:
            with jax.named_scope("norm"):
                pl.loop(RING * step, RING * (step + 1))(norm_rows)
    put_t0[0]()

    def gate_up_body(out_ways, out_act):
        step = pl.program_id(0)
        at_step(hooks[0], step)
        w = [gu_v[0, m, :, :, :, :, part(step, MXU)].reshape(D, MXU) for m in BOTH]
        tall = T // RING
        for k in range(RING):
            rows = part(k, tall)
            gate, up = (dot(a_v[rows], w[m]) for m in BOTH)
            silu, slope = silu_parts(gate)
            for m, val in enumerate((up * slope, silu)):
                out_ways[m, rows] = val
            out_act[rows] = (silu * up).astype(BF)

    with jax.named_scope("P1"):
        outs = [blocks((2, T, MXU), {2: 0}), blocks((T, MXU), {1: 0})]
        pltpu.emit_pipeline(gate_up_body, grid=(FF // MXU,), out_specs=outs)(ways, act1)
    put_t0[1]()

    wide = 512

    def down_body(act, out_h):
        step = pl.program_id(0)
        at_step(hooks[1], step)
        for k in range(wide // MXU):
            rows = part(k, MXU)
            there = part(step * (wide // MXU) + k, MXU)
            out = dot(act[rows], d_v[0].reshape(FF, D)).astype(BF)
            h = (h_v[there].astype(F32) + out.astype(F32)).astype(BF)
            out_h[rows] = h
            a = normed(h)
            a_v[there] = a
            t_v[:, there] = a.T

    with jax.named_scope("P2"):
        pltpu.emit_pipeline(
            down_body, grid=(T // wide,), in_specs=[blocks((wide, FF), {0: 0})], out_specs=[blocks((wide, D), {0: 0})]
        )(act1, h1)
    put_t1[0]()
    fetch_dy[1]()

    def finish():
        for job in jobs:
            job.finish()

    last = hooks[2]
    for step, start in enumerate((*(put[0] for put in put_w), finish), 3):
        last[step] = start

    def second_body(out_act, out_dgu):
        col, row = pl.program_id(0), pl.program_id(1)
        at_step(last, col * (T // wide) + row)
        rows = part(row, wide)
        a, dy = a_v[rows], dy_v[rows]
        wd = d_v[1, pl.ds(2 * col, 2)].reshape(FF // 2 // ROWS, ROWS, D)
        for k in range(FF // 2 // MXU):
            cols = part(k, MXU)
            there = part(col * (FF // 2 // MXU) + k, MXU)
            gate, up = (dot(a, gu_v[1, m, :, :, :, :, there].reshape(D, MXU)) for m in BOTH)
            by_act = dot(dy, wd[part(k, MXU // ROWS)].reshape(MXU, D), 1, 1).astype(BF).astype(F32)
            silu, slope = silu_parts(gate)
            out_act[:, cols] = (silu * up).astype(BF)
            for m, val in enumerate((by_act * up * slope, by_act * silu)):
                out_dgu[m, :, cols] = val.astype(BF)

    with jax.named_scope("P3"):
        outs = [blocks((wide, FF // 2), {0: 1, 1: 0}), blocks((2, wide, FF // 2), {1: 1, 2: 0})]
        pltpu.emit_pipeline(second_body, grid=(2, T // wide), out_specs=outs)(act2, dgu2)
    with jax.named_scope("puts"):
        for put in (put_t1, *put_w):
            put[1]()


def shaped(*shape, kind=BF):
    return jax.ShapeDtypeStruct(shape, kind)


def calls(kernel, number, ins, outs, scratch):
    return pl.pallas_call(
        kernel,
        out_shape=tuple(shape for shape, _ in outs),
        in_specs=ins,
        out_specs=tuple(spec for _, spec in outs),
        scratch_shapes=scratch,
        compiler_params=pltpu.CompilerParams(collective_id=number, has_side_effects=True, vmem_limit_bytes=VMEM),
        name=kernel.__name__,
    )


def forward(wg, wu, wd, x, dy):
    layers, rows = wg.shape[:-1]
    outs = [
        shaped(layers, 2, *CUBE, rows, FF), shaped(*CUBE, HIGH, ROWS, D), shaped(D, T), shaped(2, T, FF, kind=F32), shaped(T, FF),
        shaped(T, D), shaped(D, T), shaped(T, FF), shaped(2, T, FF),
    ]
    scratch = [(layers, 2, *CUBE, rows, FF), (layers, *CUBE, HIGH, ROWS, D), (T, D), (T, D), (D, T), (T, D)]
    sems = [(7,), (7, 3, 16), (7, 3, 16)]
    scratch = [pltpu.VMEM(t, BF) for t in scratch] + [pltpu.SemaphoreType.DMA(t) for t in sems]
    call = calls(forward_kernel, 0, [VM] * 3 + [ANY] * 2, [(t, ANY) for t in outs], scratch)
    return call(wg, wu, wd.reshape(layers, HIGH, ROWS, D), x, dy)


def down_grad(act, by_out, mine, hooks):
    def body(act_cols):
        k = pl.program_id(0)
        at_step(hooks, k)
        val = dot(act_cols[...], by_out[...], 0, 0)
        tiles = D // LANES
        left = None
        for c in range(tiles):
            col = val[:, part(c, LANES)].reshape(RING**2, HIGH, ROWS, LANES)
            mine[k, :, :, 2 * c : 2 * c + 2] = col[:, : HIGH - 1].reshape(RING, RING, 2, PAIR, LANES).astype(BF)
            last = col[:, HIGH - 1 :]
            if c % 2:
                both = jnp.concatenate([left, last], 1).reshape(RING, RING, PAIR, LANES)
                mine[k, :, :, 2 * tiles + c // 2] = both.astype(BF)
            left = last

    pltpu.emit_pipeline(body, grid=(RING,), in_specs=[blocks((T, FF // RING), {1: 0})])(act)


def gate_up_grads(a_t, dgu, mine, hooks):
    wide = 512
    each = FF // wide

    def body(cols):
        k = pl.program_id(0)
        at_step(hooks, k)
        for n in range(wide // MXU):
            val = dot(a_t[...], cols[:, part(n, MXU)])
            for c in range(MXU // LANES):
                col = val[:, part(c, LANES)].reshape(*CUBE, PAIR, LANES).astype(BF)
                mine[1 + k // each, :, :, :, (k % each) * (wide // LANES) + n * (MXU // LANES) + c] = col

    pltpu.emit_pipeline(body, grid=(2 * each,), in_specs=[pl.BlockSpec((None, T, wide), lambda k: (k // each, 0, k % each))])(dgu)


def state_grad(dgu, w, h, by_out, held, out, keep, hooks):
    steps = T // MXU

    def project(d, k, n):
        cols = part(n, MXU)
        by_gate, by_up = (dot(d[m], w[m, cols], 1, 1).astype(BF).astype(F32) for m in BOTH)
        held[part(k % 2, MXU), cols] = (by_gate + by_up).astype(BF)

    def finish(h, outs, k, n):
        rows = part(n, MXU // RING)
        there = part(jnp.maximum(k - 1, 0) * RING + n, MXU // RING)
        by_a = held[part((k + 1) % 2 * RING + n, MXU // RING), :D].astype(F32)
        wide = h[rows].astype(F32)
        scale = norm_scale(wide)
        inner = row_mean(by_a * wide)
        by_norm = (by_a * scale - wide * (inner * scale * scale * scale)).astype(BF)
        total = (by_out[there].astype(F32) + by_norm.astype(F32)).astype(BF)
        if keep is None:
            outs[0][rows] = total
        else:
            keep[there] = total

    def body(d, h, *outs):
        k = pl.program_id(0)
        at_step(hooks, k)

        @pl.when(k < steps)
        def _():
            for n in range(RING):
                finish(h, outs, k, n)
                project(d, k, n)

        @pl.when(k == steps)
        def _():
            for n in range(RING):
                finish(h, outs, k, n)

    behind = pl.BlockSpec((MXU, D), lambda k: (jnp.maximum(k - 1, 0), 0))
    now = lambda k: jnp.minimum(k, steps - 1)
    if len(dgu.shape) > 3:
        each = steps // 2
        source = pl.BlockSpec((2, None, MXU, FF), lambda k: (0, now(k) // each, now(k) % each, 0))
    else:
        source = pl.BlockSpec((2, MXU, FF), lambda k: (0, now(k), 0))
    pltpu.emit_pipeline(
        body,
        grid=(steps + 1,),
        in_specs=[source, behind],
        out_specs=[behind] if keep is None else [],
    )(dgu, h, *([out] if keep is None else []))


def layer_grads(ways, by_out, w, a_t, mine, held, out, sem, hooks, fetch):
    steps = FF // MXU
    pairs = steps // 2

    def held_at(k, m):
        return part(2 * (k % pairs) + m, MXU)

    def moves(k):
        for m in BOTH:
            for n in BOTH:
                yield pltpu.make_async_copy(held.at[n, :, held_at(k, m)], out.at[m, n, :, part(k, MXU)], sem.at[k % 2, m, n])

    tall = T // 2

    def act(way, k, r):
        rows = part(r, tall)
        by_act = dot(by_out[rows], w[part(k, MXU)], 1, 1).astype(BF).astype(F32)
        for m in BOTH:
            held[r, :, held_at(k, m)] = (by_act * way[m, rows]).astype(BF)

    def weights(k, m):
        val = dot(a_t[...], held[:, :, held_at(k, m)].reshape(T, MXU))
        for c in range(MXU // LANES):
            unit = m * (UNITS // 2) + (k % pairs) * (MXU // LANES) + c
            mine[1 + k // pairs, :, :, :, unit] = val[:, part(c, LANES)].reshape(*CUBE, PAIR, LANES).astype(BF)

    def body(way):
        k = pl.program_id(0)
        at_step(hooks, k)

        @pl.when(k >= 1)
        def _():
            for copy in moves(k - 1):
                copy.start()

        @pl.when(k >= 2)
        def _():
            for copy in moves(k - 2):
                copy.wait()

        @pl.when(k == 0)
        def _():
            for r in BOTH:
                act(way, k, r)

        @pl.when((k > 0) & (k < steps))
        def _():
            for r in BOTH:
                weights(k - 1, r)
                act(way, k, r)

        @pl.when(k == steps)
        def _():
            fetch()
            for r in BOTH:
                weights(k - 1, r)

    block = pl.BlockSpec((2, T, MXU), lambda k: (0, 0, jnp.minimum(k, steps - 1)))
    pltpu.emit_pipeline(body, grid=(steps + 1,), in_specs=[block])(ways)
    for copy in moves(steps - 1):
        copy.wait()


BACKWARD_STEPS = (4, 10, 9, 4, 11, 1, 9, 6)
SCATTERS = (
    (4, 8, 14, 16, 18, 24),
    (9, 16, 21, 24, 26, 29),
    (16, 24, 29, 30, 32, 35),
    (27, 30, 34, 36, 40, 43),
    (33, 35, 40, 42, 46, 48),
    (38, 41, 46, 49, 50, 51),
)


def backward_kernel(
    act2, dy, aT1, dgu2, gu_w, h1, act1, ways, d_w, aT0, x, dx, dgu1, d_out, g_out, u_out, dy_w_v, t_v, dh_v, w_v, mine, *more
):
    *bufs, sem, move_sem, send, recv, recv_c = more
    place = Place()
    sems = [sem.at[k] for k in range(sem.shape[0])]

    def load(src, dst):
        at = sems.pop()
        copy = lambda: pltpu.make_async_copy(src, dst, at)
        return lambda: copy().start(), lambda: copy().wait()

    dy_v = dy_w_v.at[:T]
    early, late = slice(0, FF - 2 * MXU), slice(FF - 2 * MXU, FF)
    loads = [(dy, dy_v), (aT1, t_v), (gu_w.at[1], w_v), (aT0, t_v), (d_w, dy_w_v)]
    loads += [(gu_w.at[0, :, :, cols], w_v.at[:, :, cols]) for cols in (early, late)]
    fetch_dy, fetch_t, fetch_w, fetch_t0, fetch_d, *fetch_w0 = (load(*pair) for pair in loads)
    fetch_dy[0]()
    entered = enter(place, 0)
    groups = [bufs[k : k + len(SHARES)] for k in range(0, len(bufs), len(SHARES))]
    jobs = []
    halves = [put_half((g_out.at[0], u_out.at[0]), half) for half in BOTH]
    for puts in ((put_down(d_out.at[1]), put_gate_up(g_out.at[1]), put_gate_up(u_out.at[1])), (put_down(d_out.at[0]), *halves)):
        for k, put in enumerate(puts):
            n = len(jobs)
            jobs.append(Scatter(place, mine.at[k], put, n, groups, send, recv, recv_c))
    hooks = spread(jobs, SCATTERS, BACKWARD_STEPS)
    for phase, step, fetch in ((0, 1, fetch_t), (1, 2, fetch_w), (3, 2, fetch_t0), (3, 0, fetch_d)):
        hooks[phase][step] = fetch[0]
    fetch_dy[1]()
    with jax.named_scope("P4"):
        down_grad(act2, dy_v, mine.at[0], hooks[0])
    entered()
    fetch_t[1]()
    with jax.named_scope("P5"):
        gate_up_grads(t_v, dgu2, mine, hooks[1])
    fetch_w[1]()
    with jax.named_scope("P6"):
        state_grad(dgu2, w_v, h1, dy_v, t_v, None, dh_v, hooks[2])
    with jax.named_scope("P7"):
        down_grad(act1, dh_v, mine.at[0], hooks[3])
    fetch_d[1]()
    fetch_t0[1]()
    with jax.named_scope("P8"):
        layer_grads(ways, dh_v, dy_w_v, t_v, mine, w_v, dgu1, move_sem, hooks[4], fetch_w0[0][0])
    fetch_w0[1][0]()
    hooks[5][0]()

    def arrived():
        for fetch in fetch_w0:
            fetch[1]()

    hooks[6][0] = arrived
    with jax.named_scope("P10"):
        state_grad(dgu1, w_v, x, dh_v, t_v, dx, None, hooks[6])
    with jax.named_scope("ending"):
        for step in sorted(hooks[7]):
            hooks[7][step]()


def backward(*args):
    n = 6
    sums = [shaped(2, HIGH * ROWS, D), shaped(2, PAIR, FF), shaped(2, PAIR, FF)]
    outs = [(shaped(T, D), ANY), (shaped(2, 2, T // 2, FF), ANY)] + [(t, VM) for t in sums]
    vmem = [(FF, D), (D, T), (T, D), (2, D, FF), (len(sums), *CUBE, UNITS, PAIR, LANES)]
    scratch = [
        *(pltpu.VMEM(t, BF) for t in vmem),
        *(buf for group in scatter_scratch(n) for buf in group),
        pltpu.SemaphoreType.DMA((n + 1,)),
        pltpu.SemaphoreType.DMA((2, 2, 2)),
        pltpu.SemaphoreType.DMA((2, len(SHARES), Scatter.STARTS[-1])),
        pltpu.SemaphoreType.DMA((2, len(SHARES), Scatter.STARTS[4])),
        pltpu.SemaphoreType.DMA((n, len(SHARES), len(STEPS))),
    ]
    return calls(backward_kernel, 1, [ANY] * len(args), outs, scratch)(*args)


def solution(mesh):
    def step(x, dy, wg, wu, wd):
        x, dy = x[0], dy[0]
        gu, down, aT0, ways, act1, h1, aT1, act2, dgu2 = forward(wg, wu, wd, x, dy)
        gu, down = gu.reshape(-1, 2, D, FF), down.reshape(FF, D)
        dx, _, by_d, by_g, by_u = backward(act2, dy, aT1, dgu2, gu, h1, act1, ways, down, aT0, x)
        return dx[None], by_g, by_u, by_d

    seq, rows = P(("rep", "dp"), None, None), P(None, "dp", None)
    return jax.shard_map(
        step, mesh=mesh, in_specs=(seq, seq, rows, rows, rows), out_specs=(seq, *[P("rep", "dp", None)] * 3), check_vma=False
    )
```

```python
import jax
import jax.numpy as jnp
from jax import lax
from jax.experimental import pallas as pl
from jax.experimental.pallas import tpu as pltpu
from jax.sharding import PartitionSpec as P

MESH = pl.DeviceIdType.MESH
BF, F32 = jnp.bfloat16, jnp.float32
ANY = pl.BlockSpec(memory_space=pl.ANY)
VM = pl.BlockSpec(memory_space=pltpu.VMEM)
T, D, FF = 2048, 1024, 2560
RING, LANES, ROWS, MXU = 4, 128, 8, 256
PAIR = 2 * ROWS
CUBE = (RING,) * 3
UNITS = 20
HIGH = UNITS * PAIR * LANES // D // ROWS
AXES = range(3)
BOTH = range(2)
STEPS = (1, -1, 2)
SIDES = ((0, 1), (1, -1))
EVERY = slice(None)
TWO = slice(0, 2)
VMEM = 67_043_328

GATHER_ORDERS = ((2, 1, 0), (0, 2, 1), (1, 0, 2))
SCATTER_ORDERS = ((0, 1, 2), (1, 2, 0), (2, 0, 1))
SHARES = ((0, 7), (7, 14), (14, 20))


class Place:
    def __init__(self):
        self.core = lax.axis_index("rep")
        me = lax.axis_index("dp")
        self.at = (me // RING**2, (me // RING) % RING, me % RING)
        self.on = {(a, step): (self.at[a] + (step + RING)) % RING for a in AXES for step in STEPS}

    def along(self, axis, step):
        return self.on[axis, step]

    def peer(self, axis, step):
        x, y, z = (self.along(a, step) if a == axis else self.at[a] for a in AXES)
        return {"dp": (x * RING + y) * RING + z}

    def other(self):
        return {"rep": 1 - self.core}


def enter(place, other):
    barrier = pltpu.get_barrier_semaphore()
    for axis in AXES:
        for step in STEPS:
            pl.semaphore_signal(barrier, inc=1, device_id=place.peer(axis, step), device_id_type=MESH)
    if other:
        pl.semaphore_signal(barrier, inc=1, device_id=place.other(), device_id_type=MESH)
    return lambda: pl.semaphore_wait(barrier, len(STEPS) * len(AXES) + other)


def remote(src, dst, send, recv, device):
    return pltpu.make_async_remote_copy(src_ref=src, dst_ref=dst, send_sem=send, recv_sem=recv, device_id=device, device_id_type=MESH)


def wait_for(what, sem):
    pltpu.make_async_copy(what, what, sem).wait()


def row_mean(x):
    return jnp.mean(x, -1, keepdims=True)


def norm_scale(wide):
    return lax.rsqrt(row_mean(wide * wide) + 1e-6)


def normed(h):
    wide = h.astype(F32)
    return (wide * norm_scale(wide)).astype(BF)


def dot(a, b, over_a=1, over_b=0):
    return lax.dot_general(a, b, (((over_a,), (over_b,)), ((), ())), preferred_element_type=F32)


def at_step(hooks, step):
    for number, hook in hooks.items():
        pl.when(step == number)(hook)


class Gather:
    def __init__(self, name, place, full, parts, send, recv):
        self.name, self.p, self.full, self.parts, self.send, self.recv = name, place, full, parts, send, recv

    STARTS = (0, 3, 5, 7, 10, 14, 16)
    CROSS = (9, 12, 13, 14, 15)

    def view(self, color, where):
        at = [where.get(a, self.p.at[a]) for a in AXES]
        return self.full.at[(*at, *self.parts[color])]

    def copy(self, color, slot):
        a, b, c = GATHER_ORDERS[color]
        p = self.p
        stage = sum(slot >= first for first in self.STARTS) - 1
        group = len(self.CROSS) if slot in self.CROSS else stage
        sems = self.send.at[color, group], self.recv.at[color, group]
        k = slot - self.STARTS[stage]
        if stage == 0:
            block = self.view(color, {})
            return remote(block, block, *sems, p.peer(a, STEPS[k]))
        axis, done, split = (b, {a: EVERY}, a) if stage < 3 else (c, {a: EVERY, b: EVERY}, b)
        side = k % 2
        step, half = STEPS[side], slice(2 * side, 2 * side + 2)
        where = dict(done)
        if stage in (2, 4):
            where[axis] = p.along(axis, -step)
            if slot not in self.CROSS:
                where[split] = half
        if stage == 5:
            where.update({axis: p.along(axis, 2), split: half})
        block = self.view(color, where)
        return remote(block, block, *sems, p.other() if slot in self.CROSS else p.peer(axis, step))

    def wait(self, color, group, sems):
        a, b, c = GATHER_ORDERS[color]
        ab = {a: EVERY, b: EVERY}
        where = {a: slice(len(STEPS))}, {a: EVERY, b: TWO}, {a: EVERY}, {**ab, c: TWO}, ab, {**ab, c: EVERY}
        wait_for(self.view(color, where[group]), sems.at[color, group])

    def stage(self, number):
        last = len(self.STARTS) - 1
        for color in AXES:
            if number:
                self.wait(color, number - 1, self.recv)
            for slot in range(self.STARTS[number], self.STARTS[number + 1]) if number < last else ():
                self.copy(color, slot).start()
            if 0 < number < last:
                self.wait(color, number - 1, self.send)

    def finish(self):
        for color in AXES:
            self.wait(color, len(self.CROSS), self.send)


def gather_parts(core):
    columns = []
    for layer in (((3, 3, 2), (2, 2, 2), (2, 2, 2)), ((4, 3, 3), (3, 4, 3))):
        first = 0
        columns.append([])
        for widths in layer:
            columns[-1].append([])
            for width in widths:
                columns[-1][-1].append((EVERY, slice(first * LANES, (first + width) * LANES)))
                first += width
    half = part(core, D // 2)
    return columns, [(slice(*cut), EVERY, half) for cut in ((4, 5), (0, 2), (2, 4))]


def slots(*groups):
    def hook():
        for job, stage in groups:
            with jax.named_scope(f"{job.name}_{stage}"):
                job.stage(stage)

    return hook


def spread(jobs, table, sizes):
    plan = {}
    for n, (job, steps) in enumerate(zip(jobs, table, strict=True)):
        for stage, step in enumerate(steps):
            plan.setdefault(step, []).append((-stage, n, job))
    hooks, first = [], 0
    for size in sizes:
        steps = [step for step in sorted(plan) if first <= step < first + size]
        hooks.append({step - first: slots(*((job, -late) for late, _, job in sorted(plan[step], key=lambda t: t[:2]))) for step in steps})
        first += size
    return hooks


class Scatter:
    STARTS = (0, 2, 4, 6, 8, 11)

    def __init__(self, place, mine, put, number, bufs, send, recv, recv_c):
        self.name = f"rs{number}"
        self.p, self.mine, self.put, self.number, self.send, self.recv, self.recv_c = place, mine, put, number, send, recv, recv_c
        self.in_a, self.in_h, self.acc_b, self.send_b, self.in_b, self.in_bh, self.acc_c, self.send_c, self.in_c = bufs

    def sems(self, color, stage):
        twin = self.number % 2
        return self.send.at[twin, color, stage], self.recv.at[twin, color, stage] if stage < 4 else self.recv_c.at[self.number, color]

    def arrived(self, color, stage):
        twin = self.number % 2
        what = (self.in_h[color].at[twin], self.in_a[color].at[twin], self.in_bh[color], self.in_b[color], self.in_c[color].at[self.number])
        wait_for(what[stage], self.sems(color, stage)[1])

    def sent(self, color, stage):
        mine = lambda where: self.mine.at[self.term(color, (where, EVERY, EVERY))]
        send_b = self.send_b[color]
        what = (mine(0), mine(TWO), send_b.at[0], send_b.at[TWO], self.send_c[color].at[slice(len(STEPS))])
        wait_for(what[stage], self.sems(color, stage)[0])

    def term(self, color, where):
        at = dict(zip(SCATTER_ORDERS[color], where))
        return (*(at[axis] for axis in AXES), slice(*SHARES[color]))

    def copy(self, color, slot):
        a, b, c = SCATTER_ORDERS[color]
        p = self.p
        twin = self.number % 2
        stage = sum(slot >= first for first in self.STARTS) - 1
        k = slot - self.STARTS[stage]
        sems = self.sems(color, stage)
        step, half = STEPS[k], pl.ds(2 * k, 2)
        if stage == 0:
            src, dst, axis = self.mine.at[self.term(color, (p.along(a, 2), half, EVERY))], self.in_h[color].at[twin, k], a
        elif stage == 1:
            src, dst, axis = self.mine.at[self.term(color, (p.along(a, step), EVERY, EVERY))], self.in_a[color].at[twin, k], a
        elif stage == 2:
            src, dst, axis = self.send_b[color].at[p.along(b, 2), half], self.in_bh[color].at[k], b
        elif stage == 3:
            src, dst, axis = self.send_b[color].at[p.along(b, step)], self.in_b[color].at[k], b
        else:
            src, dst, axis = self.send_c[color].at[p.along(c, step)], self.in_c[color].at[self.number, k], c
        return remote(src, dst, *sems, p.peer(axis, step))

    def stage(self, number):
        last = len(self.STARTS) - 1
        for color, axes in enumerate(SCATTER_ORDERS):
            if number:
                self.arrived(color, number - 1)
            self.sum(number, color, *axes)
            for slot in range(self.STARTS[number], self.STARTS[number + 1]) if number < last else ():
                self.copy(color, slot).start()
            for stage in range(2 * (number - 3), min(2 * number - 4, last)) if number > 2 else ():
                self.sent(color, stage)

    def sum(self, number, color, a, b, c):
        p, mine, twin = self.p, self.mine, self.number % 2
        in_a, in_h, acc_b, send_b, in_b, in_bh = (
            t[color] for t in (self.in_a, self.in_h, self.acc_b, self.send_b, self.in_b, self.in_bh)
        )
        acc_c, send_c, in_c = (t[color] for t in (self.acc_c, self.send_c, self.in_c))
        flip = (lambda i, j: (i, j)) if b < c else (lambda i, j: (j, i))
        if number == 1:
            for slot, step in SIDES:

                @pl.loop(0, 2 * RING, unroll=2)
                def _(k):
                    i, j = k // RING, k % RING
                    at = self.term(color, (p.along(a, step), 2 * slot + i, j))
                    mine[at] = (mine[at].astype(F32) + in_h[(twin, slot, *flip(i, j))].astype(F32)).astype(BF)

        if number == 2:

            @pl.loop(0, RING**2, unroll=2)
            def _(k):
                i, j = k // RING, k % RING
                total = mine[self.term(color, (p.at[a], i, j))].astype(F32)
                for slot, _ in SIDES:
                    total = total + in_a[(twin, slot, *flip(i, j))].astype(F32)
                acc_b[i, j] = total
                send_b[i, j] = total.astype(BF)

        if number == 3:
            for slot, step in SIDES:
                i = p.along(b, step)

                @pl.loop(0, 2)
                def _(j):
                    send_b[i, 2 * slot + j] = (acc_b[i, 2 * slot + j] + in_bh[slot, j].astype(F32)).astype(BF)

        if number == 4:

            @pl.loop(0, RING)
            def _(j):
                total = acc_b[p.at[b], j]
                for slot, _ in SIDES:
                    total = total + in_b[slot, j].astype(F32)
                acc_c[j] = total
                send_c[j] = total.astype(BF)

        if number == 5:
            total = acc_c[p.at[c]]
            for slot in AXES:
                total = total + in_c[self.number, slot].astype(F32)
            lo, hi = SHARES[color]
            for k in range(lo, hi):
                self.put(k, total[k - lo])


def scatter_scratch(jobs):
    two, ring = (2,), (RING,)
    groups = []
    for (lo, hi), (a, b, c) in zip(SHARES, SCATTER_ORDERS):
        half = two + ring if b < c else ring + two
        shapes = (
            (two + two + ring + ring, BF), (two + two + half, BF), (ring + ring, F32), (ring + ring, BF), (two + ring, BF), (two + two, BF),
            (ring, F32), (ring, BF), ((jobs, len(STEPS)), BF),
        )
        groups.append([pltpu.VMEM((*shape, hi - lo, PAIR, LANES), kind) for shape, kind in shapes])
    return zip(*groups)


def put_gate_up(out):
    def put(k, unit):
        out[:, part(k, LANES)] = unit.astype(BF)

    return put


def put_half(outs, half):
    def put(k, unit):
        which, col = k // (UNITS // 2), k % (UNITS // 2) + half * (UNITS // 2)
        outs[which][:, part(col, LANES)] = unit.astype(BF)

    return put


def put_down(out):
    def put(k, unit):
        extra = k - D // LANES * 2
        if extra < 0:
            out[part(k % 2, PAIR), part(k // 2, LANES)] = unit.astype(BF)
        else:
            for n in BOTH:
                out[part(HIGH - 1, ROWS), part(2 * extra + n, LANES)] = unit[ROWS * n : ROWS * (n + 1)].astype(BF)

    return put


def part(k, size):
    return slice(k * size, (k + 1) * size) if isinstance(k, int) else pl.ds(pl.multiple_of(k * size, size), size)


def blocks(shape, places, **mode):
    return pl.BlockSpec(shape, lambda *at: tuple(at[places[k]] if k in places else 0 for k in range(len(shape))), **mode)


def silu_parts(gate):
    s = jax.nn.sigmoid(gate)
    silu = gate * s
    return silu, s + silu * (1 - s)


FORWARD_STEPS = (9, FF // MXU, 4, 8)
GATHERS = (
    (0, 1, 2, 3, 5, 7, 8),
    (0, 1, 2, 5, 10, 12, 13),
    (0, 1, 2, 7, 12, 15, 16),
    (0, 4, 6, 11, 15, 18, 19),
    (0, 4, 6, 15, 19, 21, 23),
    (0, 4, 6, 13, 17, 20, 23),
    (0, 4, 6, 18, 21, 23, 25),
)


def forward_kernel(
    g_ref, u_ref, d_ref, x_ref, dy_ref, gu_out, d_out, aT0, ways, act1, h1, aT1, act2, dgu2, gu_v, d_v, a_v, h_v, t_v, dy_v, sem, send, recv
):
    place = Place()
    core = place.core
    sems = [sem.at[k] for k in range(sem.shape[0])]

    def copy(src, dst):
        at = sems.pop()
        made = lambda: pltpu.make_async_copy(src, dst, at)
        return lambda: made().start(), lambda: made().wait()

    fetch_x, fetch_dy = copy(x_ref, h_v), copy(dy_ref, dy_v)
    puts = [copy(t_v, aT0), copy(t_v, aT1), copy(gu_v.at[0], gu_out.at[0]), copy(gu_v.at[1], gu_out.at[1]), copy(d_v.at[0], d_out)]
    put_t0, put_t1, *put_w = puts
    fetch_x[0]()
    columns, rows_of_down = gather_parts(core)
    half = rows_of_down[0][-1]
    for n in range(g_ref.shape[0]):
        gu_v[(n, core, *place.at)] = jnp.where(core == 0, g_ref[n], u_ref[n])
        d_v[(n, *place.at, EVERY, EVERY, half)] = d_ref[n, :, :, half]
    entered = enter(place, 1)
    fetch_dy[0]()
    plan = [(gu_v.at[0, core], piece) for piece in columns[0]]
    early, late = columns[1]
    plan += [(d_v.at[0], rows_of_down), (gu_v.at[1, core], early), (d_v.at[1], rows_of_down), (gu_v.at[1, core], late)]
    jobs = [Gather(f"ag{n}", place, *what, send.at[n], recv.at[n]) for n, what in enumerate(plan)]
    prelude, *hooks = spread(jobs, GATHERS, FORWARD_STEPS)
    with jax.named_scope("enter"):
        entered()

    def norm_rows(k):
        rows = part(k, MXU)
        a = normed(h_v[rows])
        a_v[rows] = a
        t_v[:, rows] = a.T

    for step in sorted(prelude):
        prelude[step]()
        if step == 0:
            fetch_x[1]()
        if step < 2:
            with jax.named_scope("norm"):
                pl.loop(RING * step, RING * (step + 1))(norm_rows)
    put_t0[0]()

    def gate_up_body(out_ways, out_act):
        step = pl.program_id(0)
        at_step(hooks[0], step)
        w = [gu_v[0, m, :, :, :, :, part(step, MXU)].reshape(D, MXU) for m in BOTH]
        tall = T // RING
        for k in range(RING):
            rows = part(k, tall)
            gate, up = (dot(a_v[rows], w[m]) for m in BOTH)
            silu, slope = silu_parts(gate)
            for m, val in enumerate((up * slope, silu)):
                out_ways[m, rows] = val
            out_act[rows] = (silu * up).astype(BF)

    with jax.named_scope("P1"):
        outs = [blocks((2, T, MXU), {2: 0}), blocks((T, MXU), {1: 0})]
        pltpu.emit_pipeline(gate_up_body, grid=(FF // MXU,), out_specs=outs)(ways, act1)
    put_t0[1]()

    wide = 512

    def down_body(act, out_h):
        step = pl.program_id(0)
        at_step(hooks[1], step)
        for k in range(wide // MXU):
            rows = part(k, MXU)
            there = part(step * (wide // MXU) + k, MXU)
            out = dot(act[rows], d_v[0].reshape(FF, D)).astype(BF)
            h = (h_v[there].astype(F32) + out.astype(F32)).astype(BF)
            out_h[rows] = h
            a = normed(h)
            a_v[there] = a
            t_v[:, there] = a.T

    with jax.named_scope("P2"):
        pltpu.emit_pipeline(
            down_body, grid=(T // wide,), in_specs=[blocks((wide, FF), {0: 0})], out_specs=[blocks((wide, D), {0: 0})]
        )(act1, h1)
    put_t1[0]()
    fetch_dy[1]()

    def finish():
        for job in jobs:
            job.finish()

    last = hooks[2]
    for step, start in enumerate((*(put[0] for put in put_w), finish), 3):
        last[step] = start

    def second_body(out_act, out_dgu):
        col, row = pl.program_id(0), pl.program_id(1)
        at_step(last, col * (T // wide) + row)
        rows = part(row, wide)
        a, dy = a_v[rows], dy_v[rows]
        wd = d_v[1, pl.ds(2 * col, 2)].reshape(FF // 2 // ROWS, ROWS, D)
        for k in range(FF // 2 // MXU):
            cols = part(k, MXU)
            there = part(col * (FF // 2 // MXU) + k, MXU)
            gate, up = (dot(a, gu_v[1, m, :, :, :, :, there].reshape(D, MXU)) for m in BOTH)
            by_act = dot(dy, wd[part(k, MXU // ROWS)].reshape(MXU, D), 1, 1).astype(BF).astype(F32)
            silu, slope = silu_parts(gate)
            out_act[:, cols] = (silu * up).astype(BF)
            for m, val in enumerate((by_act * up * slope, by_act * silu)):
                out_dgu[m, :, cols] = val.astype(BF)

    with jax.named_scope("P3"):
        outs = [blocks((wide, FF // 2), {0: 1, 1: 0}), blocks((2, wide, FF // 2), {1: 1, 2: 0})]
        pltpu.emit_pipeline(second_body, grid=(2, T // wide), out_specs=outs)(act2, dgu2)
    with jax.named_scope("puts"):
        for put in (put_t1, *put_w):
            put[1]()


def shaped(*shape, kind=BF):
    return jax.ShapeDtypeStruct(shape, kind)


def calls(kernel, number, ins, outs, scratch):
    return pl.pallas_call(
        kernel,
        out_shape=tuple(shape for shape, _ in outs),
        in_specs=ins,
        out_specs=tuple(spec for _, spec in outs),
        scratch_shapes=scratch,
        compiler_params=pltpu.CompilerParams(collective_id=number, has_side_effects=True, vmem_limit_bytes=VMEM),
        name=kernel.__name__,
    )


def forward(wg, wu, wd, x, dy):
    layers, rows = wg.shape[:-1]
    outs = [
        shaped(layers, 2, *CUBE, rows, FF), shaped(*CUBE, HIGH, ROWS, D), shaped(D, T), shaped(2, T, FF, kind=F32), shaped(T, FF),
        shaped(T, D), shaped(D, T), shaped(T, FF), shaped(2, T, FF),
    ]
    scratch = [(layers, 2, *CUBE, rows, FF), (layers, *CUBE, HIGH, ROWS, D), (T, D), (T, D), (D, T), (T, D)]
    sems = [(len(GATHERS),)] + [(len(GATHERS), len(SHARES), 6)] * 2
    scratch = [pltpu.VMEM(t, BF) for t in scratch] + [pltpu.SemaphoreType.DMA(t) for t in sems]
    call = calls(forward_kernel, 0, [VM] * 3 + [ANY] * 2, [(t, ANY) for t in outs], scratch)
    return call(wg, wu, wd.reshape(layers, HIGH, ROWS, D), x, dy)


def down_grad(act, by_out, mine, hooks):
    def body(act_cols):
        k = pl.program_id(0)
        at_step(hooks, k)
        val = dot(act_cols[...], by_out[...], 0, 0)
        tiles = D // LANES
        left = None
        for c in range(tiles):
            col = val[:, part(c, LANES)].reshape(RING**2, HIGH, ROWS, LANES)
            mine[k, :, :, 2 * c : 2 * c + 2] = col[:, : HIGH - 1].reshape(RING, RING, 2, PAIR, LANES).astype(BF)
            last = col[:, HIGH - 1 :]
            if c % 2:
                both = jnp.concatenate([left, last], 1).reshape(RING, RING, PAIR, LANES)
                mine[k, :, :, 2 * tiles + c // 2] = both.astype(BF)
            left = last

    pltpu.emit_pipeline(body, grid=(RING,), in_specs=[blocks((T, FF // RING), {1: 0})])(act)


def gate_up_grads(a_t, dgu, mine, hooks):
    wide = 512
    each = FF // wide

    def body(cols):
        k = pl.program_id(0)
        at_step(hooks, k)
        for n in range(wide // MXU):
            val = dot(a_t[...], cols[:, part(n, MXU)])
            for c in range(MXU // LANES):
                col = val[:, part(c, LANES)].reshape(*CUBE, PAIR, LANES).astype(BF)
                mine[1 + k // each, :, :, :, (k % each) * (wide // LANES) + n * (MXU // LANES) + c] = col

    pltpu.emit_pipeline(body, grid=(2 * each,), in_specs=[pl.BlockSpec((None, T, wide), lambda k: (k // each, 0, k % each))])(dgu)


def state_grad(dgu, w, h, by_out, held, out, keep, hooks):
    steps = T // MXU

    def project(d, k, n):
        cols = part(n, MXU)
        by_gate, by_up = (dot(d[m], w[m, cols], 1, 1).astype(BF).astype(F32) for m in BOTH)
        held[part(k % 2, MXU), cols] = (by_gate + by_up).astype(BF)

    def finish(h, outs, k, n):
        rows = part(n, MXU // RING)
        there = part(jnp.maximum(k - 1, 0) * RING + n, MXU // RING)
        by_a = held[part((k + 1) % 2 * RING + n, MXU // RING), :D].astype(F32)
        wide = h[rows].astype(F32)
        scale = norm_scale(wide)
        inner = row_mean(by_a * wide)
        by_norm = (by_a * scale - wide * (inner * scale * scale * scale)).astype(BF)
        total = (by_out[there].astype(F32) + by_norm.astype(F32)).astype(BF)
        if keep is None:
            outs[0][rows] = total
        else:
            keep[there] = total

    def body(d, h, *outs):
        k = pl.program_id(0)
        at_step(hooks, k)

        @pl.when(k < steps)
        def _():
            for n in range(RING):
                finish(h, outs, k, n)
                project(d, k, n)

        @pl.when(k == steps)
        def _():
            for n in range(RING):
                finish(h, outs, k, n)

    behind = pl.BlockSpec((MXU, D), lambda k: (jnp.maximum(k - 1, 0), 0))
    now = lambda k: jnp.minimum(k, steps - 1)
    if len(dgu.shape) > 3:
        each = steps // 2
        source = pl.BlockSpec((2, None, MXU, FF), lambda k: (0, now(k) // each, now(k) % each, 0))
    else:
        source = pl.BlockSpec((2, MXU, FF), lambda k: (0, now(k), 0))
    pltpu.emit_pipeline(
        body,
        grid=(steps + 1,),
        in_specs=[source, behind],
        out_specs=[behind] if keep is None else [],
    )(dgu, h, *([out] if keep is None else []))


def layer_grads(ways, by_out, w, a_t, mine, held, out, sem, hooks, fetch):
    steps = FF // MXU
    pairs = steps // 2

    def held_at(k, m):
        return part(2 * (k % pairs) + m, MXU)

    def moves(k):
        for m in BOTH:
            for n in BOTH:
                yield pltpu.make_async_copy(held.at[n, :, held_at(k, m)], out.at[m, n, :, part(k, MXU)], sem.at[k % 2, m, n])

    tall = T // 2

    def act(way, k, r):
        rows = part(r, tall)
        by_act = dot(by_out[rows], w[part(k, MXU)], 1, 1).astype(BF).astype(F32)
        for m in BOTH:
            held[r, :, held_at(k, m)] = (by_act * way[m, rows]).astype(BF)

    def weights(k, m):
        val = dot(a_t[...], held[:, :, held_at(k, m)].reshape(T, MXU))
        for c in range(MXU // LANES):
            unit = m * (UNITS // 2) + (k % pairs) * (MXU // LANES) + c
            mine[1 + k // pairs, :, :, :, unit] = val[:, part(c, LANES)].reshape(*CUBE, PAIR, LANES).astype(BF)

    def body(way):
        k = pl.program_id(0)
        at_step(hooks, k)

        @pl.when(k >= 1)
        def _():
            for copy in moves(k - 1):
                copy.start()

        @pl.when(k >= 2)
        def _():
            for copy in moves(k - 2):
                copy.wait()

        @pl.when(k == 0)
        def _():
            for r in BOTH:
                act(way, k, r)

        @pl.when((k > 0) & (k < steps))
        def _():
            for r in BOTH:
                weights(k - 1, r)
                act(way, k, r)

        @pl.when(k == steps)
        def _():
            fetch()
            for r in BOTH:
                weights(k - 1, r)

    block = pl.BlockSpec((2, T, MXU), lambda k: (0, 0, jnp.minimum(k, steps - 1)))
    pltpu.emit_pipeline(body, grid=(steps + 1,), in_specs=[block])(ways)
    for copy in moves(steps - 1):
        copy.wait()


BACKWARD_STEPS = (4, 10, 9, 4, 11, 1, 9, 6)
SCATTERS = (
    (4, 8, 14, 16, 18, 24),
    (9, 16, 21, 24, 26, 29),
    (16, 24, 29, 30, 32, 35),
    (27, 30, 34, 36, 40, 43),
    (33, 35, 40, 42, 46, 48),
    (38, 41, 46, 49, 50, 51),
)


def backward_kernel(
    act2, dy, aT1, dgu2, gu_w, h1, act1, ways, d_w, aT0, x, dx, dgu1, d_out, g_out, u_out, dy_w_v, t_v, dh_v, w_v, mine, *more
):
    *bufs, sem, move_sem, send, recv, recv_c = more
    place = Place()
    sems = [sem.at[k] for k in range(sem.shape[0])]

    def load(src, dst):
        at = sems.pop()
        copy = lambda: pltpu.make_async_copy(src, dst, at)
        return lambda: copy().start(), lambda: copy().wait()

    dy_v = dy_w_v.at[:T]
    early, late = slice(0, FF - 2 * MXU), slice(FF - 2 * MXU, FF)
    loads = [(dy, dy_v), (aT1, t_v), (gu_w.at[1], w_v), (aT0, t_v), (d_w, dy_w_v)]
    loads += [(gu_w.at[0, :, :, cols], w_v.at[:, :, cols]) for cols in (early, late)]
    fetch_dy, fetch_t, fetch_w, fetch_t0, fetch_d, *fetch_w0 = (load(*pair) for pair in loads)
    fetch_dy[0]()
    entered = enter(place, 0)
    groups = [bufs[k : k + len(SHARES)] for k in range(0, len(bufs), len(SHARES))]
    jobs = []
    halves = [put_half((g_out.at[0], u_out.at[0]), half) for half in BOTH]
    for puts in ((put_down(d_out.at[1]), put_gate_up(g_out.at[1]), put_gate_up(u_out.at[1])), (put_down(d_out.at[0]), *halves)):
        for k, put in enumerate(puts):
            n = len(jobs)
            jobs.append(Scatter(place, mine.at[k], put, n, groups, send, recv, recv_c))
    hooks = spread(jobs, SCATTERS, BACKWARD_STEPS)
    for phase, step, fetch in ((0, 1, fetch_t), (1, 2, fetch_w), (3, 2, fetch_t0), (3, 0, fetch_d)):
        hooks[phase][step] = fetch[0]
    fetch_dy[1]()
    with jax.named_scope("P4"):
        down_grad(act2, dy_v, mine.at[0], hooks[0])
    entered()
    fetch_t[1]()
    with jax.named_scope("P5"):
        gate_up_grads(t_v, dgu2, mine, hooks[1])
    fetch_w[1]()
    with jax.named_scope("P6"):
        state_grad(dgu2, w_v, h1, dy_v, t_v, None, dh_v, hooks[2])
    with jax.named_scope("P7"):
        down_grad(act1, dh_v, mine.at[0], hooks[3])
    fetch_d[1]()
    fetch_t0[1]()
    with jax.named_scope("P8"):
        layer_grads(ways, dh_v, dy_w_v, t_v, mine, w_v, dgu1, move_sem, hooks[4], fetch_w0[0][0])
    fetch_w0[1][0]()
    hooks[5][0]()

    def arrived():
        for fetch in fetch_w0:
            fetch[1]()

    hooks[6][0] = arrived
    with jax.named_scope("P10"):
        state_grad(dgu1, w_v, x, dh_v, t_v, dx, None, hooks[6])
    with jax.named_scope("ending"):
        for step in sorted(hooks[7]):
            hooks[7][step]()


def backward(*args):
    n = len(SCATTERS)
    twins = (2, len(SHARES))
    sums = [shaped(2, HIGH * ROWS, D), shaped(2, PAIR, FF), shaped(2, PAIR, FF)]
    outs = [(shaped(T, D), ANY), (shaped(2, 2, T // 2, FF), ANY)] + [(t, VM) for t in sums]
    vmem = [(FF, D), (D, T), (T, D), (2, D, FF), (len(sums), *CUBE, UNITS, PAIR, LANES)]
    scratch = [
        *(pltpu.VMEM(t, BF) for t in vmem),
        *(buf for group in scatter_scratch(n) for buf in group),
        pltpu.SemaphoreType.DMA((n + 1,)),
        pltpu.SemaphoreType.DMA((2, 2, 2)),
        *(pltpu.SemaphoreType.DMA(t) for t in ((*twins, 5), (*twins, 4), (n, len(SHARES)))),
    ]
    return calls(backward_kernel, 1, [ANY] * len(args), outs, scratch)(*args)


def solution(mesh):
    def step(x, dy, wg, wu, wd):
        x, dy = x[0], dy[0]
        gu, down, aT0, ways, act1, h1, aT1, act2, dgu2 = forward(wg, wu, wd, x, dy)
        gu, down = gu.reshape(-1, 2, D, FF), down.reshape(FF, D)
        dx, _, by_d, by_g, by_u = backward(act2, dy, aT1, dgu2, gu, h1, act1, ways, down, aT0, x)
        return dx[None], by_g, by_u, by_d

    seq, rows = P(("rep", "dp"), None, None), P(None, "dp", None)
    return jax.shard_map(
        step, mesh=mesh, in_specs=(seq, seq, rows, rows, rows), out_specs=(seq, *[P("rep", "dp", None)] * 3), check_vma=False
    )
```

```python
import jax
import jax.numpy as jnp
from jax import lax
from jax.experimental import pallas as pl
from jax.experimental.pallas import tpu as pltpu
from jax.sharding import PartitionSpec as P

MESH = pl.DeviceIdType.MESH
BF, F32 = jnp.bfloat16, jnp.float32
ANY = pl.BlockSpec(memory_space=pl.ANY)
VM = pl.BlockSpec(memory_space=pltpu.VMEM)
T, D, FF = 2048, 1024, 2560
RING, LANES, ROWS, MXU = 4, 128, 8, 256
PAIR = 2 * ROWS
CUBE = (RING,) * 3
UNITS = 20
HIGH = UNITS * PAIR * LANES // D // ROWS
AXES = range(3)
BOTH = range(2)
STEPS = (1, -1, 2)
SIDES = ((0, 1), (1, -1))
EVERY = slice(None)
TWO = slice(0, 2)
VMEM = 67_043_328

GATHER_ORDERS = ((2, 1, 0), (0, 2, 1), (1, 0, 2))
SCATTER_ORDERS = ((0, 1, 2), (1, 2, 0), (2, 0, 1))
SHARES = ((0, 7), (7, 14), (14, 20))


class Place:
    def __init__(self):
        self.core = lax.axis_index("rep")
        me = lax.axis_index("dp")
        self.at = (me // RING**2, (me // RING) % RING, me % RING)
        self.on = {(a, step): (self.at[a] + (step + RING)) % RING for a in AXES for step in STEPS}

    def along(self, axis, step):
        return self.on[axis, step]

    def peer(self, axis, step):
        x, y, z = (self.along(a, step) if a == axis else self.at[a] for a in AXES)
        return {"dp": (x * RING + y) * RING + z}

    def other(self):
        return {"rep": 1 - self.core}


def enter(place, other):
    barrier = pltpu.get_barrier_semaphore()
    for axis in AXES:
        for step in STEPS:
            pl.semaphore_signal(barrier, inc=1, device_id=place.peer(axis, step), device_id_type=MESH)
    if other:
        pl.semaphore_signal(barrier, inc=1, device_id=place.other(), device_id_type=MESH)
    return lambda: pl.semaphore_wait(barrier, len(STEPS) * len(AXES) + other)


def remote(src, dst, send, recv, device):
    return pltpu.make_async_remote_copy(src_ref=src, dst_ref=dst, send_sem=send, recv_sem=recv, device_id=device, device_id_type=MESH)


def wait_for(what, sem):
    pltpu.make_async_copy(what, what, sem).wait()


def row_mean(x):
    return jnp.mean(x, -1, keepdims=True)


def norm_scale(wide):
    return lax.rsqrt(row_mean(wide * wide) + 1e-6)


def normed(h):
    wide = h.astype(F32)
    return (wide * norm_scale(wide)).astype(BF)


def dot(a, b, over_a=1, over_b=0):
    return lax.dot_general(a, b, (((over_a,), (over_b,)), ((), ())), preferred_element_type=F32)


def at_step(hooks, step):
    for number, hook in hooks.items():
        pl.when(step == number)(hook)


class Gather:
    def __init__(self, name, place, full, parts, send, recv):
        self.name, self.p, self.full, self.parts, self.send, self.recv = name, place, full, parts, send, recv

    STARTS = (0, 3, 5, 7, 10, 14, 16)
    CROSS = (9, 12, 13, 14, 15)

    def view(self, color, where):
        at = [where.get(a, self.p.at[a]) for a in AXES]
        return self.full.at[(*at, *self.parts[color])]

    def copy(self, color, slot):
        a, b, c = GATHER_ORDERS[color]
        p = self.p
        stage = sum(slot >= first for first in self.STARTS) - 1
        group = len(self.CROSS) if slot in self.CROSS else stage
        sems = self.send.at[color, group], self.recv.at[color, group]
        k = slot - self.STARTS[stage]
        if stage == 0:
            block = self.view(color, {})
            return remote(block, block, *sems, p.peer(a, STEPS[k]))
        axis, done, split = (b, {a: EVERY}, a) if stage < 3 else (c, {a: EVERY, b: EVERY}, b)
        side = k % 2
        step, half = STEPS[side], slice(2 * side, 2 * side + 2)
        where = dict(done)
        if stage in (2, 4):
            where[axis] = p.along(axis, -step)
            if slot not in self.CROSS:
                where[split] = half
        if stage == 5:
            where.update({axis: p.along(axis, 2), split: half})
        block = self.view(color, where)
        return remote(block, block, *sems, p.other() if slot in self.CROSS else p.peer(axis, step))

    def wait(self, color, group, sems):
        a, b, c = GATHER_ORDERS[color]
        ab = {a: EVERY, b: EVERY}
        where = {a: slice(len(STEPS))}, {a: EVERY, b: TWO}, {a: EVERY}, {**ab, c: TWO}, ab, {**ab, c: EVERY}
        wait_for(self.view(color, where[group]), sems.at[color, group])

    def stage(self, number):
        last = len(self.STARTS) - 1
        for color in AXES:
            if number:
                self.wait(color, number - 1, self.recv)
            for slot in range(self.STARTS[number], self.STARTS[number + 1]) if number < last else ():
                self.copy(color, slot).start()
            if 0 < number < last:
                self.wait(color, number - 1, self.send)

    def finish(self):
        for color in AXES:
            self.wait(color, len(self.CROSS), self.send)


def gather_parts(core):
    columns = []
    for layer in (((3, 3, 2), (2, 2, 2), (2, 2, 2)), ((4, 3, 3), (3, 4, 3))):
        first = 0
        columns.append([])
        for widths in layer:
            columns[-1].append([])
            for width in widths:
                columns[-1][-1].append((EVERY, slice(first * LANES, (first + width) * LANES)))
                first += width
    half = part(core, D // 2)
    return columns, [(slice(*cut), EVERY, half) for cut in ((4, 5), (0, 2), (2, 4))]


def slots(*groups):
    def hook():
        for job, stage in groups:
            with jax.named_scope(f"{job.name}_{stage}"):
                job.stage(stage)

    return hook


def spread(jobs, table, sizes):
    plan = {}
    for n, (job, steps) in enumerate(zip(jobs, table, strict=True)):
        for stage, step in enumerate(steps):
            plan.setdefault(step, []).append((-stage, n, job))
    hooks, first = [], 0
    for size in sizes:
        steps = [step for step in sorted(plan) if first <= step < first + size]
        hooks.append({step - first: slots(*((job, -late) for late, _, job in sorted(plan[step], key=lambda t: t[:2]))) for step in steps})
        first += size
    return hooks


class Scatter:
    STARTS = (0, 2, 4, 6, 8, 11)

    def __init__(self, place, mine, put, number, bufs, send, recv, recv_c):
        self.name = f"rs{number}"
        self.p, self.mine, self.put, self.number, self.send, self.recv, self.recv_c = place, mine, put, number, send, recv, recv_c
        self.in_a, self.in_h, self.acc_b, self.send_b, self.in_b, self.in_bh, self.acc_c, self.send_c, self.in_c = bufs

    def sems(self, color, stage):
        twin = self.number % 2
        return self.send.at[twin, color, stage], self.recv.at[twin, color, stage] if stage < 4 else self.recv_c.at[self.number, color]

    def arrived(self, color, stage):
        twin = self.number % 2
        what = (self.in_h[color].at[twin], self.in_a[color].at[twin], self.in_bh[color], self.in_b[color], self.in_c[color].at[self.number])
        wait_for(what[stage], self.sems(color, stage)[1])

    def sent(self, color, stage):
        mine = lambda where: self.mine.at[self.term(color, (where, EVERY, EVERY))]
        send_b = self.send_b[color]
        what = (mine(0), mine(TWO), send_b.at[0], send_b.at[TWO], self.send_c[color].at[slice(len(STEPS))])
        wait_for(what[stage], self.sems(color, stage)[0])

    def term(self, color, where):
        at = dict(zip(SCATTER_ORDERS[color], where))
        return (*(at[axis] for axis in AXES), slice(*SHARES[color]))

    def copy(self, color, slot):
        a, b, c = SCATTER_ORDERS[color]
        p = self.p
        twin = self.number % 2
        stage = sum(slot >= first for first in self.STARTS) - 1
        k = slot - self.STARTS[stage]
        sems = self.sems(color, stage)
        step, half = STEPS[k], pl.ds(2 * k, 2)
        if stage == 0:
            src, dst, axis = self.mine.at[self.term(color, (p.along(a, 2), half, EVERY))], self.in_h[color].at[twin, k], a
        elif stage == 1:
            src, dst, axis = self.mine.at[self.term(color, (p.along(a, step), EVERY, EVERY))], self.in_a[color].at[twin, k], a
        elif stage == 2:
            src, dst, axis = self.send_b[color].at[p.along(b, 2), half], self.in_bh[color].at[k], b
        elif stage == 3:
            src, dst, axis = self.send_b[color].at[p.along(b, step)], self.in_b[color].at[k], b
        else:
            src, dst, axis = self.send_c[color].at[p.along(c, step)], self.in_c[color].at[self.number, k], c
        return remote(src, dst, *sems, p.peer(axis, step))

    def stage(self, number):
        last = len(self.STARTS) - 1
        for color, axes in enumerate(SCATTER_ORDERS):
            if number:
                self.arrived(color, number - 1)
            self.sum(number, color, *axes)
            for slot in range(self.STARTS[number], self.STARTS[number + 1]) if number < last else ():
                self.copy(color, slot).start()
            for stage in range(2 * (number - 3), min(2 * number - 4, last)) if number > 2 else ():
                self.sent(color, stage)

    def sum(self, number, color, a, b, c):
        p, mine, twin = self.p, self.mine, self.number % 2
        in_a, in_h, acc_b, send_b, in_b, in_bh = (
            t[color] for t in (self.in_a, self.in_h, self.acc_b, self.send_b, self.in_b, self.in_bh)
        )
        acc_c, send_c, in_c = (t[color] for t in (self.acc_c, self.send_c, self.in_c))
        flip = (lambda i, j: (i, j)) if b < c else (lambda i, j: (j, i))
        if number == 1:
            for slot, step in SIDES:

                @pl.loop(0, 2 * RING, unroll=2)
                def _(k):
                    i, j = k // RING, k % RING
                    at = self.term(color, (p.along(a, step), 2 * slot + i, j))
                    mine[at] = (mine[at].astype(F32) + in_h[(twin, slot, *flip(i, j))].astype(F32)).astype(BF)

        if number == 2:

            @pl.loop(0, RING**2, unroll=2)
            def _(k):
                i, j = k // RING, k % RING
                total = mine[self.term(color, (p.at[a], i, j))].astype(F32)
                for slot, _ in SIDES:
                    total = total + in_a[(twin, slot, *flip(i, j))].astype(F32)
                acc_b[i, j] = total
                send_b[i, j] = total.astype(BF)

        if number == 3:
            for slot, step in SIDES:
                i = p.along(b, step)

                @pl.loop(0, 2)
                def _(j):
                    send_b[i, 2 * slot + j] = (acc_b[i, 2 * slot + j] + in_bh[slot, j].astype(F32)).astype(BF)

        if number == 4:

            @pl.loop(0, RING)
            def _(j):
                total = acc_b[p.at[b], j]
                for slot, _ in SIDES:
                    total = total + in_b[slot, j].astype(F32)
                acc_c[j] = total
                send_c[j] = total.astype(BF)

        if number == 5:
            total = acc_c[p.at[c]]
            for slot in AXES:
                total = total + in_c[self.number, slot].astype(F32)
            lo, hi = SHARES[color]
            for k in range(lo, hi):
                self.put(k, total[k - lo])


def scatter_scratch(jobs):
    two, ring = (2,), (RING,)
    groups = []
    for (lo, hi), (a, b, c) in zip(SHARES, SCATTER_ORDERS):
        half = two + ring if b < c else ring + two
        shapes = (
            (two + two + ring + ring, BF), (two + two + half, BF), (ring + ring, F32), (ring + ring, BF), (two + ring, BF), (two + two, BF),
            (ring, F32), (ring, BF), ((jobs, len(STEPS)), BF),
        )
        groups.append([pltpu.VMEM((*shape, hi - lo, PAIR, LANES), kind) for shape, kind in shapes])
    return zip(*groups)


def put_gate_up(out):
    def put(k, unit):
        out[:, part(k, LANES)] = unit.astype(BF)

    return put


def put_half(outs, half):
    def put(k, unit):
        which, col = k // (UNITS // 2), k % (UNITS // 2) + half * (UNITS // 2)
        outs[which][:, part(col, LANES)] = unit.astype(BF)

    return put


def put_down(out):
    def put(k, unit):
        extra = k - D // LANES * 2
        if extra < 0:
            out[part(k % 2, PAIR), part(k // 2, LANES)] = unit.astype(BF)
        else:
            for n in BOTH:
                out[part(HIGH - 1, ROWS), part(2 * extra + n, LANES)] = unit[ROWS * n : ROWS * (n + 1)].astype(BF)

    return put


def part(k, size):
    return slice(k * size, (k + 1) * size) if isinstance(k, int) else pl.ds(pl.multiple_of(k * size, size), size)


def blocks(shape, places, **mode):
    return pl.BlockSpec(shape, lambda *at: tuple(at[places[k]] if k in places else 0 for k in range(len(shape))), **mode)


def silu_parts(gate):
    s = jax.nn.sigmoid(gate)
    silu = gate * s
    return silu, s + silu * (1 - s)


FORWARD_STEPS = (9, FF // MXU, 4, 8)
GATHERS = (
    (0, 1, 2, 3, 5, 7, 8),
    (0, 1, 2, 5, 10, 12, 13),
    (0, 1, 2, 7, 12, 15, 16),
    (0, 4, 6, 11, 15, 18, 19),
    (0, 4, 6, 15, 19, 21, 23),
    (0, 4, 6, 13, 17, 20, 23),
    (0, 4, 6, 18, 21, 23, 25),
)


def forward_kernel(
    g_ref, u_ref, d_ref, x_ref, dy_ref, gu_out, d_out, aT0, ways, act1, h1, aT1, act2, dgu2, gu_v, d_v, a_v, h_v, t_v, dy_v, sem, send, recv
):
    place = Place()
    core = place.core
    sems = [sem.at[k] for k in range(sem.shape[0])]

    def copy(src, dst):
        at = sems.pop()
        made = lambda: pltpu.make_async_copy(src, dst, at)
        return lambda: made().start(), lambda: made().wait()

    fetch_x, fetch_dy = copy(x_ref, h_v), copy(dy_ref, dy_v)
    puts = [copy(t_v, aT0), copy(t_v, aT1), copy(gu_v.at[0], gu_out.at[0]), copy(gu_v.at[1], gu_out.at[1]), copy(d_v.at[0], d_out)]
    put_t0, put_t1, *put_w = puts
    entered = enter(place, 1)
    columns, rows_of_down = gather_parts(core)
    half = rows_of_down[0][-1]
    own = []
    for n in BOTH:
        of_down = (EVERY, EVERY, half)
        own.append(pltpu.make_async_copy(d_ref.at[(n, *of_down)], d_v.at[(n, *place.at, *of_down)], sems.pop()))
        own[-1].start()
        at = sems.pop()
        of_mine = [pltpu.make_async_copy(ref.at[n], gu_v.at[(n, core, *place.at)], at) for ref in (g_ref, u_ref)]
        for m, fetch in enumerate(of_mine):
            pl.when(core == m)(fetch.start)
        own.append(of_mine[0])
    fetch_x[0]()
    fetch_dy[0]()
    plan = [(gu_v.at[0, core], piece) for piece in columns[0]]
    early, late = columns[1]
    plan += [(d_v.at[0], rows_of_down), (gu_v.at[1, core], early), (d_v.at[1], rows_of_down), (gu_v.at[1, core], late)]
    jobs = [Gather(f"ag{n}", place, *what, send.at[n], recv.at[n]) for n, what in enumerate(plan)]
    prelude, *hooks = spread(jobs, GATHERS, FORWARD_STEPS)
    with jax.named_scope("enter"):
        for fetch in own:
            fetch.wait()
        entered()

    def norm_rows(k):
        rows = part(k, MXU)
        a = normed(h_v[rows])
        a_v[rows] = a
        t_v[:, rows] = a.T

    for step in sorted(prelude):
        prelude[step]()
        if step == 0:
            fetch_x[1]()
        if step < 2:
            with jax.named_scope("norm"):
                pl.loop(RING * step, RING * (step + 1))(norm_rows)
    put_t0[0]()

    def gate_up_body(out_ways, out_act):
        step = pl.program_id(0)
        at_step(hooks[0], step)
        w = [gu_v[0, m, :, :, :, :, part(step, MXU)].reshape(D, MXU) for m in BOTH]
        tall = T // RING
        for k in range(RING):
            rows = part(k, tall)
            gate, up = (dot(a_v[rows], w[m]) for m in BOTH)
            silu, slope = silu_parts(gate)
            for m, val in enumerate((up * slope, silu)):
                out_ways[m, rows] = val
            out_act[rows] = (silu * up).astype(BF)

    with jax.named_scope("P1"):
        outs = [blocks((2, T, MXU), {2: 0}), blocks((T, MXU), {1: 0})]
        pltpu.emit_pipeline(gate_up_body, grid=(FF // MXU,), out_specs=outs)(ways, act1)
    put_t0[1]()

    wide = 512

    def down_body(act, out_h):
        step = pl.program_id(0)
        at_step(hooks[1], step)
        for k in range(wide // MXU):
            rows = part(k, MXU)
            there = part(step * (wide // MXU) + k, MXU)
            out = dot(act[rows], d_v[0].reshape(FF, D)).astype(BF)
            h = (h_v[there].astype(F32) + out.astype(F32)).astype(BF)
            out_h[rows] = h
            a = normed(h)
            a_v[there] = a
            t_v[:, there] = a.T

    with jax.named_scope("P2"):
        pltpu.emit_pipeline(
            down_body, grid=(T // wide,), in_specs=[blocks((wide, FF), {0: 0})], out_specs=[blocks((wide, D), {0: 0})]
        )(act1, h1)
    put_t1[0]()
    fetch_dy[1]()

    def finish():
        for job in jobs:
            job.finish()

    last = hooks[2]
    for step, start in enumerate((*(put[0] for put in put_w), finish), 3):
        last[step] = start

    def second_body(out_act, out_dgu):
        col, row = pl.program_id(0), pl.program_id(1)
        at_step(last, col * (T // wide) + row)
        rows = part(row, wide)
        a, dy = a_v[rows], dy_v[rows]
        wd = d_v[1, pl.ds(2 * col, 2)].reshape(FF // 2 // ROWS, ROWS, D)
        for k in range(FF // 2 // MXU):
            cols = part(k, MXU)
            there = part(col * (FF // 2 // MXU) + k, MXU)
            gate, up = (dot(a, gu_v[1, m, :, :, :, :, there].reshape(D, MXU)) for m in BOTH)
            by_act = dot(dy, wd[part(k, MXU // ROWS)].reshape(MXU, D), 1, 1).astype(BF).astype(F32)
            silu, slope = silu_parts(gate)
            out_act[:, cols] = (silu * up).astype(BF)
            for m, val in enumerate((by_act * up * slope, by_act * silu)):
                out_dgu[m, :, cols] = val.astype(BF)

    with jax.named_scope("P3"):
        outs = [blocks((wide, FF // 2), {0: 1, 1: 0}), blocks((2, wide, FF // 2), {1: 1, 2: 0})]
        pltpu.emit_pipeline(second_body, grid=(2, T // wide), out_specs=outs)(act2, dgu2)
    with jax.named_scope("puts"):
        for put in (put_t1, *put_w):
            put[1]()


def shaped(*shape, kind=BF):
    return jax.ShapeDtypeStruct(shape, kind)


def calls(kernel, number, ins, outs, scratch):
    return pl.pallas_call(
        kernel,
        out_shape=tuple(shape for shape, _ in outs),
        in_specs=ins,
        out_specs=tuple(spec for _, spec in outs),
        scratch_shapes=scratch,
        compiler_params=pltpu.CompilerParams(collective_id=number, has_side_effects=True, vmem_limit_bytes=VMEM),
        name=kernel.__name__,
    )


def forward(wg, wu, wd, x, dy):
    layers, rows = wg.shape[:-1]
    outs = [
        shaped(layers, 2, *CUBE, rows, FF), shaped(*CUBE, HIGH, ROWS, D), shaped(D, T), shaped(2, T, FF, kind=F32), shaped(T, FF),
        shaped(T, D), shaped(D, T), shaped(T, FF), shaped(2, T, FF),
    ]
    scratch = [(layers, 2, *CUBE, rows, FF), (layers, *CUBE, HIGH, ROWS, D), (T, D), (T, D), (D, T), (T, D)]
    sems = [(11,)] + [(len(GATHERS), len(SHARES), 6)] * 2
    scratch = [pltpu.VMEM(t, BF) for t in scratch] + [pltpu.SemaphoreType.DMA(t) for t in sems]
    call = calls(forward_kernel, 0, [ANY] * 5, [(t, ANY) for t in outs], scratch)
    return call(wg, wu, wd.reshape(layers, HIGH, ROWS, D), x, dy)


def down_grad(act, by_out, mine, hooks):
    def body(act_cols):
        k = pl.program_id(0)
        at_step(hooks, k)
        val = dot(act_cols[...], by_out[...], 0, 0)
        tiles = D // LANES
        left = None
        for c in range(tiles):
            col = val[:, part(c, LANES)].reshape(RING**2, HIGH, ROWS, LANES)
            mine[k, :, :, 2 * c : 2 * c + 2] = col[:, : HIGH - 1].reshape(RING, RING, 2, PAIR, LANES).astype(BF)
            last = col[:, HIGH - 1 :]
            if c % 2:
                both = jnp.concatenate([left, last], 1).reshape(RING, RING, PAIR, LANES)
                mine[k, :, :, 2 * tiles + c // 2] = both.astype(BF)
            left = last

    pltpu.emit_pipeline(body, grid=(RING,), in_specs=[blocks((T, FF // RING), {1: 0})])(act)


def gate_up_grads(a_t, dgu, mine, hooks):
    wide = 512
    each = FF // wide

    def body(cols):
        k = pl.program_id(0)
        at_step(hooks, k)
        for n in range(wide // MXU):
            val = dot(a_t[...], cols[:, part(n, MXU)])
            for c in range(MXU // LANES):
                col = val[:, part(c, LANES)].reshape(*CUBE, PAIR, LANES).astype(BF)
                mine[1 + k // each, :, :, :, (k % each) * (wide // LANES) + n * (MXU // LANES) + c] = col

    pltpu.emit_pipeline(body, grid=(2 * each,), in_specs=[pl.BlockSpec((None, T, wide), lambda k: (k // each, 0, k % each))])(dgu)


def state_grad(dgu, w, h, by_out, held, out, keep, hooks):
    steps = T // MXU

    def project(d, k, n):
        cols = part(n, MXU)
        by_gate, by_up = (dot(d[m], w[m, cols], 1, 1).astype(BF).astype(F32) for m in BOTH)
        held[part(k % 2, MXU), cols] = (by_gate + by_up).astype(BF)

    def finish(h, outs, k, n):
        rows = part(n, MXU // RING)
        there = part(jnp.maximum(k - 1, 0) * RING + n, MXU // RING)
        by_a = held[part((k + 1) % 2 * RING + n, MXU // RING), :D].astype(F32)
        wide = h[rows].astype(F32)
        scale = norm_scale(wide)
        inner = row_mean(by_a * wide)
        by_norm = (by_a * scale - wide * (inner * scale * scale * scale)).astype(BF)
        total = (by_out[there].astype(F32) + by_norm.astype(F32)).astype(BF)
        if keep is None:
            outs[0][rows] = total
        else:
            keep[there] = total

    def body(d, h, *outs):
        k = pl.program_id(0)
        at_step(hooks, k)

        @pl.when(k < steps)
        def _():
            for n in range(RING):
                finish(h, outs, k, n)
                project(d, k, n)

        @pl.when(k == steps)
        def _():
            for n in range(RING):
                finish(h, outs, k, n)

    behind = pl.BlockSpec((MXU, D), lambda k: (jnp.maximum(k - 1, 0), 0))
    now = lambda k: jnp.minimum(k, steps - 1)
    if len(dgu.shape) > 3:
        each = steps // 2
        source = pl.BlockSpec((2, None, MXU, FF), lambda k: (0, now(k) // each, now(k) % each, 0))
    else:
        source = pl.BlockSpec((2, MXU, FF), lambda k: (0, now(k), 0))
    pltpu.emit_pipeline(
        body,
        grid=(steps + 1,),
        in_specs=[source, behind],
        out_specs=[behind] if keep is None else [],
    )(dgu, h, *([out] if keep is None else []))


def layer_grads(ways, by_out, w, a_t, mine, held, out, sem, hooks, fetch):
    steps = FF // MXU
    pairs = steps // 2

    def held_at(k, m):
        return part(2 * (k % pairs) + m, MXU)

    def moves(k):
        for m in BOTH:
            for n in BOTH:
                yield pltpu.make_async_copy(held.at[n, :, held_at(k, m)], out.at[m, n, :, part(k, MXU)], sem.at[k % 2, m, n])

    tall = T // 2

    def act(way, k, r):
        rows = part(r, tall)
        by_act = dot(by_out[rows], w[part(k, MXU)], 1, 1).astype(BF).astype(F32)
        for m in BOTH:
            held[r, :, held_at(k, m)] = (by_act * way[m, rows]).astype(BF)

    def weights(k, m):
        val = dot(a_t[...], held[:, :, held_at(k, m)].reshape(T, MXU))
        for c in range(MXU // LANES):
            unit = m * (UNITS // 2) + (k % pairs) * (MXU // LANES) + c
            mine[1 + k // pairs, :, :, :, unit] = val[:, part(c, LANES)].reshape(*CUBE, PAIR, LANES).astype(BF)

    def body(way):
        k = pl.program_id(0)
        at_step(hooks, k)

        @pl.when(k >= 1)
        def _():
            for copy in moves(k - 1):
                copy.start()

        @pl.when(k >= 2)
        def _():
            for copy in moves(k - 2):
                copy.wait()

        @pl.when(k == 0)
        def _():
            for r in BOTH:
                act(way, k, r)

        @pl.when((k > 0) & (k < steps))
        def _():
            for r in BOTH:
                weights(k - 1, r)
                act(way, k, r)

        @pl.when(k == steps)
        def _():
            fetch()
            for r in BOTH:
                weights(k - 1, r)

    block = pl.BlockSpec((2, T, MXU), lambda k: (0, 0, jnp.minimum(k, steps - 1)))
    pltpu.emit_pipeline(body, grid=(steps + 1,), in_specs=[block])(ways)
    for copy in moves(steps - 1):
        copy.wait()


BACKWARD_STEPS = (4, 10, 9, 4, 11, 1, 9, 6)
SCATTERS = (
    (4, 8, 14, 16, 18, 24),
    (9, 16, 21, 24, 26, 29),
    (16, 24, 29, 30, 32, 35),
    (27, 30, 34, 36, 40, 43),
    (33, 35, 40, 42, 46, 48),
    (38, 41, 46, 49, 50, 51),
)


def backward_kernel(
    act2, dy, aT1, dgu2, gu_w, h1, act1, ways, d_w, aT0, x, dx, dgu1, d_out, g_out, u_out, dy_w_v, t_v, dh_v, w_v, mine, *more
):
    *bufs, sem, move_sem, send, recv, recv_c = more
    place = Place()
    sems = [sem.at[k] for k in range(sem.shape[0])]

    def load(src, dst):
        at = sems.pop()
        copy = lambda: pltpu.make_async_copy(src, dst, at)
        return lambda: copy().start(), lambda: copy().wait()

    dy_v = dy_w_v.at[:T]
    early, late = slice(0, FF - 2 * MXU), slice(FF - 2 * MXU, FF)
    loads = [(dy, dy_v), (aT1, t_v), (gu_w.at[1], w_v), (aT0, t_v), (d_w, dy_w_v)]
    loads += [(gu_w.at[0, :, :, cols], w_v.at[:, :, cols]) for cols in (early, late)]
    fetch_dy, fetch_t, fetch_w, fetch_t0, fetch_d, *fetch_w0 = (load(*pair) for pair in loads)
    fetch_dy[0]()
    entered = enter(place, 0)
    groups = [bufs[k : k + len(SHARES)] for k in range(0, len(bufs), len(SHARES))]
    jobs = []
    halves = [put_half((g_out.at[0], u_out.at[0]), half) for half in BOTH]
    for puts in ((put_down(d_out.at[1]), put_gate_up(g_out.at[1]), put_gate_up(u_out.at[1])), (put_down(d_out.at[0]), *halves)):
        for k, put in enumerate(puts):
            n = len(jobs)
            jobs.append(Scatter(place, mine.at[k], put, n, groups, send, recv, recv_c))
    hooks = spread(jobs, SCATTERS, BACKWARD_STEPS)
    for phase, step, fetch in ((0, 1, fetch_t), (0, 2, fetch_w), (3, 2, fetch_t0), (3, 0, fetch_d)):
        hooks[phase][step] = fetch[0]
    hooks[0][0] = fetch_dy[1]
    with jax.named_scope("P4"):
        down_grad(act2, dy_v, mine.at[0], hooks[0])
    entered()
    fetch_t[1]()
    with jax.named_scope("P5"):
        gate_up_grads(t_v, dgu2, mine, hooks[1])
    fetch_w[1]()
    with jax.named_scope("P6"):
        state_grad(dgu2, w_v, h1, dy_v, t_v, None, dh_v, hooks[2])
    with jax.named_scope("P7"):
        down_grad(act1, dh_v, mine.at[0], hooks[3])
    fetch_d[1]()
    fetch_t0[1]()
    with jax.named_scope("P8"):
        layer_grads(ways, dh_v, dy_w_v, t_v, mine, w_v, dgu1, move_sem, hooks[4], fetch_w0[0][0])
    fetch_w0[1][0]()
    hooks[5][0]()

    def arrived():
        for fetch in fetch_w0:
            fetch[1]()

    hooks[6][0] = arrived
    with jax.named_scope("P10"):
        state_grad(dgu1, w_v, x, dh_v, t_v, dx, None, hooks[6])
    with jax.named_scope("ending"):
        for step in sorted(hooks[7]):
            hooks[7][step]()


def backward(*args):
    n = len(SCATTERS)
    twins = (2, len(SHARES))
    sums = [shaped(2, HIGH * ROWS, D), shaped(2, PAIR, FF), shaped(2, PAIR, FF)]
    outs = [(shaped(T, D), ANY), (shaped(2, 2, T // 2, FF), ANY)] + [(t, VM) for t in sums]
    vmem = [(FF, D), (D, T), (T, D), (2, D, FF), (len(sums), *CUBE, UNITS, PAIR, LANES)]
    scratch = [
        *(pltpu.VMEM(t, BF) for t in vmem),
        *(buf for group in scatter_scratch(n) for buf in group),
        pltpu.SemaphoreType.DMA((n + 1,)),
        pltpu.SemaphoreType.DMA((2, 2, 2)),
        *(pltpu.SemaphoreType.DMA(t) for t in ((*twins, 5), (*twins, 4), (n, len(SHARES)))),
    ]
    return calls(backward_kernel, 1, [ANY] * len(args), outs, scratch)(*args)


def solution(mesh):
    def step(x, dy, wg, wu, wd):
        x, dy = x[0], dy[0]
        gu, down, aT0, ways, act1, h1, aT1, act2, dgu2 = forward(wg, wu, wd, x, dy)
        gu, down = gu.reshape(-1, 2, D, FF), down.reshape(FF, D)
        dx, _, by_d, by_g, by_u = backward(act2, dy, aT1, dgu2, gu, h1, act1, ways, down, aT0, x)
        return dx[None], by_g, by_u, by_d

    seq, rows = P(("rep", "dp"), None, None), P(None, "dp", None)
    return jax.shard_map(
        step, mesh=mesh, in_specs=(seq, seq, rows, rows, rows), out_specs=(seq, *[P("rep", "dp", None)] * 3), check_vma=False
    )
```
